128 devices in a mesh: lat: 4 (over y), lon: 16 (over z, x), mem: 2 (over core).
Axes of the slice: x: 4, y: 4, z: 4, core: 2. Of those that a mesh axis runs over, the one named last changes fastest.
Arguments:
- anomalies: bfloat16 [24, 16, 1440, 512], P('mem', None, 'lon', 'lat'), may hold values from -6 to 6
- taper: float32 [16, 1440, 512], P('lon', 'lat'), may hold values from 0.5 to 8
- obs_row: int32 [256, 2048], P('lat', 'lon'), may hold values from 0 to 511, as said below
- obs_col: int32 [256, 2048], P('lat', 'lon'), may hold values from 0 to 1439, as said below
- obs_level: int32 [256, 2048], P('lat', 'lon'), may hold values from 0 to 15
- obs_value: float32 [256, 2048], P('lat', 'lon'), may hold values from -18 to 18
Outputs:
- increment: float32 [16, 1440, 512], P(None, 'lon', 'lat')
The draws below stay inside these ranges and needn't reach their ends.
Inputs may be any that keep to these rules, and one draw needn't show every extreme that they name: `obs_row`: the entry in row i lies in latitude rows (i // 64) * 128 to (i // 64 + 1) * 128 - 1, drawn evenly there. `obs_col`: the entry in column j lies in longitude columns (j // 128) * 90 to (j // 128 + 1) * 90 - 1, drawn evenly there.
All inputs are finite; a program needn't handle non-finite values.
Results may differ from the reference program's by a relative error of at most 0.0066.
Values may be sent and summed in bfloat16 or wider, within the bound.
No kernel may reach another device: no remote copies, remote signals or barrier semaphores. Data moves between devices by JAX's collectives and lax.ppermute only.
A program may use at most 128 MiB of HBM per device.

```python
import math
import jax
import jax.numpy as jnp
from jax import lax

NLAT = 512
NLON = 1440
OBS_BLK = 64
L = 16
M = 24
ROWS_DEV = 128
COLS_DEV = 90
OBS_LAT = 256
OBS_LON = 2048


def draw_obs_row(key, part):
    blocks = jnp.arange(OBS_LAT, dtype=jnp.int32)[:, None] // OBS_BLK
    offsets = jax.random.randint(jax.random.fold_in(key, 11), (OBS_LAT, OBS_LON), 0, ROWS_DEV, dtype=jnp.int32)
    return (blocks * ROWS_DEV + offsets).astype(jnp.int32)


def draw_obs_col(key, part):
    blocks = jnp.arange(OBS_LON, dtype=jnp.int32)[None, :] // 128
    offsets = jax.random.randint(jax.random.fold_in(key, 23), (OBS_LAT, OBS_LON), 0, COLS_DEV, dtype=jnp.int32)
    return (blocks * COLS_DEV + offsets).astype(jnp.int32)


def touch_ends(array, own_key, smallest, high):
    longest = array.shape.index(max(array.shape))
    spots = []
    for shift in (0, 1):
        where = [jax.random.randint(jax.random.fold_in(own_key, axis), (), 0, length) for axis, length in enumerate(array.shape)]
        where[longest] = (where[longest] + shift) % array.shape[longest]
        spots.append(tuple(where))
    return array.at[spots[0]].set(smallest).at[spots[1]].set(high)


def shard_levels(rng, extent, cuts, least, top_value):
    def one(dim, parts):
        heights = jax.random.uniform(jax.random.fold_in(jax.random.fold_in(rng, 6), dim), (parts,), jnp.float32, least / len(cuts), top_value / len(cuts))
        return jnp.repeat(jnp.exp(heights), extent[dim] // parts).reshape((-1,) + (1,) * (len(extent) - dim - 1))

    level = one(*cuts[0])
    for cut in cuts[1:]:
        level = level * one(*cut)
    return level


def centred(key, shape, spread, most, shards=(), held_as=jnp.bfloat16):
    level = shard_levels(key, shape, shards, -0.22, 0.18) if shards else 1.0
    entries = jax.random.normal(key, shape, jnp.float32) * spread * level
    return jnp.minimum(jnp.maximum(entries, -most), most).astype(held_as)


def setup_inputs(seed: int = 0) -> dict:
    streams_of = jax.random.split(jax.random.key(seed), 7)
    return {
        "anomalies": centred(streams_of[0], (M, L, NLON, NLAT), 1.0, 6.0, ((0, 2), (2, 16), (3, 4))),
        "taper": jnp.clip(jnp.exp(math.log(8.0) - 2.7725887 * jax.random.uniform(streams_of[1], (L, NLON, NLAT), jnp.float32) ** shard_levels(streams_of[1], (L, NLON, NLAT), ((0, 16), (1, 4)), -0.2, 0.2)), 0.5, 8.0),
        "obs_row": draw_obs_row(jax.random.fold_in(streams_of[6], 71), 0),
        "obs_col": draw_obs_col(jax.random.fold_in(streams_of[6], 71), 0),
        "obs_level": touch_ends(jax.random.randint(streams_of[4], (OBS_LAT, OBS_LON), 0, L), jax.random.fold_in(streams_of[4], 1), 0, L - 1).astype(jnp.int32),
        "obs_value": centred(streams_of[5], (OBS_LAT, OBS_LON), 3.0, 18.0, ((0, 4), (1, 16)), jnp.float32),
    }


def lon_basis(length):
    grid_idx = jnp.arange(length, dtype=jnp.int32)[:, None]
    coef_idx = jnp.arange(length, dtype=jnp.int32)[None, :]
    nyquist = length // 2
    wavenum = jnp.where(coef_idx <= nyquist, coef_idx, coef_idx - nyquist)
    phase_idx = grid_idx * wavenum % length
    angles = phase_idx.astype(jnp.float32) * (2.0 * math.pi / length)
    scales = jnp.where((coef_idx == 0) | (coef_idx == nyquist), 1.0 / math.sqrt(length), math.sqrt(2.0 / length))
    basis = jnp.where(coef_idx <= nyquist, jnp.cos(angles), jnp.sin(angles)) * scales
    return basis.astype(jnp.bfloat16)

def lat_basis(length):
    grid_idx = jnp.arange(length, dtype=jnp.int32)[:, None]
    mode_idx = jnp.arange(length, dtype=jnp.int32)[None, :]
    phase_idx = mode_idx * (2 * grid_idx + 1) % (4 * length)
    angles = phase_idx.astype(jnp.float32) * (math.pi / (2.0 * length))
    scales = jnp.where(mode_idx == 0, 1.0 / math.sqrt(length), math.sqrt(2.0 / length))
    return (jnp.cos(angles) * scales).astype(jnp.bfloat16)

def rounded(value):
    return lax.optimization_barrier(value.astype(jnp.bfloat16)).astype(jnp.float32)

def reference(anomalies, taper, obs_row, obs_col, obs_level, obs_value):
    innovation = jnp.zeros((L, NLON, NLAT), jnp.float32).at[obs_level, obs_col, obs_row].add(obs_value)
    innov_wide = rounded(innovation)
    lon_table = lon_basis(NLON).astype(jnp.float32)
    lat_table = lat_basis(NLAT).astype(jnp.float32)

    def accumulate(summed, member):
        member_wide = member.astype(jnp.float32)
        weighted = rounded(member_wide * innov_wide)
        zonal_coef = rounded(jnp.einsum('lxy,xk->lky', weighted, lon_table))
        spectrum = jnp.einsum('lky,yn->lkn', zonal_coef, lat_table)
        tapered = rounded(spectrum * taper)
        inverse = rounded(jnp.einsum('lkn,yn->lky', tapered, lat_table))
        localized = jnp.einsum('lky,xk->lxy', inverse, lon_table)
        return (summed + member_wide * localized, None)
    summed, _ = lax.scan(accumulate, jnp.zeros((L, NLON, NLAT), jnp.float32), anomalies)
    return summed / (M - 1)
```

```python
import math

import jax
import jax.numpy as jnp
from jax import lax
from jax.experimental import pallas as pl
from jax.experimental.pallas import tpu as pltpu
from jax.sharding import PartitionSpec as P

BF = jnp.bfloat16
F32 = jnp.float32
LL = ("lat", "lon")
SWAP = [(0, 1), (1, 0)]


def vspec():
    return pl.BlockSpec(memory_space=pltpu.VMEM)


def sspec():
    return pl.BlockSpec(memory_space=pltpu.SMEM)


def params(mib):
    return pltpu.CompilerParams(vmem_limit_bytes=mib * 1024 * 1024)


def over_all(x):
    return lax.all_to_all(x, LL, split_axis=0, concat_axis=0, tiled=True)


def spread_kernel(place, row_ref, col_ref, level_ref, value_ref, out_ref, acc, *, half, levels, copies):
    mem = place[0]
    slots = levels * half
    acc[...] = jnp.zeros_like(acc)
    slot_ids = lax.broadcasted_iota(jnp.int32, (slots, 128), 0)
    row_ids = lax.broadcasted_iota(jnp.int32, (128, 128), 0)

    def add_group(g, carry):
        rows = pl.ds(pl.multiple_of(g * 8, 8), 8)
        within = col_ref[rows, :] - place[2] - mem * half
        inside = (within >= 0) & (within < half)
        keys = jnp.where(inside, level_ref[rows, :] * half + within, -1)
        lat_row = row_ref[rows, :] - place[1]
        value = value_ref[rows, :]
        high = value.astype(BF).astype(F32)
        middle = value - high
        left = []
        right = []
        for r in range(8):
            hit = slot_ids == keys[r : r + 1, :]
            left.append(jnp.where(hit, 1.0, 0.0).astype(BF))
            row_hit = row_ids == lat_row[r : r + 1, :]
            top = jnp.where(row_hit, high[r : r + 1, :], 0.0)
            low = jnp.where(row_hit, middle[r : r + 1, :], 0.0)
            right.append(jnp.concatenate([top, low], axis=0).astype(BF))
        acc[...] += lax.dot_general(
            jnp.concatenate(left, axis=1),
            jnp.concatenate(right, axis=1),
            (((1,), (1,)), ((), ())),
            preferred_element_type=F32,
        )
        return carry

    lax.fori_loop(0, row_ref.shape[0] // 8, add_group, 0)
    summed = (acc[:, :128] + acc[:, 128:]).astype(BF).reshape(levels, half, 128)
    for copy in range(copies):
        out_ref[copy] = summed


def spread(place, obs_row, obs_col, obs_level, obs_value, half, levels, copies):
    return pl.pallas_call(
        lambda *refs: spread_kernel(*refs, half=half, levels=levels, copies=copies),
        out_shape=jax.ShapeDtypeStruct((copies, levels, half, 128), BF),
        in_specs=[sspec()] + [vspec()] * 4,
        out_specs=vspec(),
        scratch_shapes=[pltpu.VMEM((levels * half, 256), F32)],
        compiler_params=params(24),
        name="spread",
    )(place, obs_row, obs_col, obs_level, obs_value)


def basis_kernel(lon_ref, lon_t_ref, lat_ref, lat_t_ref, *, cols, blocks, padded):
    total = cols * blocks
    half = total // 2
    tiles = lon_ref.shape[1] // 128
    lanes = lax.broadcasted_iota(jnp.int32, (padded, 128), 1)

    def angles(product):
        turns = (product.astype(F32) * (1.0 / total)).astype(jnp.int32)
        return (product - turns * total).astype(F32) * (2.0 * math.pi / total)

    def lon_rows(j, carry):
        within = lax.broadcasted_iota(jnp.int32, (padded, 128), 0)
        x = within + cols * j
        fine = angles(x * lanes)
        coarse = angles(x * lax.rem(lanes * 128, total))
        fine_cos = jnp.cos(fine)
        fine_sin = jnp.sin(fine)
        scale = jnp.where(within < cols, math.sqrt(2.0 / total), 0.0)
        coarse_cos = jnp.cos(coarse) * scale
        coarse_sin = jnp.sin(coarse) * scale
        sign = jnp.where((x & 1) == 0, 1.0, -1.0)
        rows = pl.ds(pl.multiple_of(j * padded, padded), padded)
        for t in range(tiles):
            c = lanes + 128 * t
            cos_t = coarse_cos[:, t : t + 1]
            sin_t = coarse_sin[:, t : t + 1]
            parts = []
            if 128 * t <= half:
                parts.append(fine_cos * cos_t - fine_sin * sin_t)
            if 128 * t + 127 > half:
                parts.append((fine_sin * cos_t + fine_cos * sin_t) * sign)
            value = parts[0] if len(parts) == 1 else jnp.where(c <= half, parts[0], parts[1])
            if t == 0 or 128 * t <= half < 128 * t + 128:
                value = jnp.where((c == 0) | (c == half), value * math.sqrt(0.5), value)
            if 128 * t + 127 >= total:
                value = jnp.where(c < total, value, 0.0)
            lon_ref[rows, 128 * t : 128 * t + 128] = value.astype(BF)
        return carry

    lax.fori_loop(0, blocks, lon_rows, 0)
    for t in range(tiles):
        strip = lon_ref[:, 128 * t : 128 * t + 128].astype(F32)
        lon_t_ref[128 * t : 128 * t + 128, :] = strip.T.astype(BF)

    length = lat_ref.shape[0]
    step = 64

    def lat_rows(i, carry):
        shape = (step, length)
        down = lax.broadcasted_iota(jnp.int32, shape, 0) + step * i
        across = lax.broadcasted_iota(jnp.int32, shape, 1)
        rows = pl.ds(pl.multiple_of(i * step, step), step)
        for grid, mode, ref in ((down, across, lat_ref), (across, down, lat_t_ref)):
            phase = (mode * (2 * grid + 1)) & (4 * length - 1)
            angle = phase.astype(F32) * (math.pi / (2.0 * length))
            scale = jnp.where(mode == 0, 1.0 / math.sqrt(length), math.sqrt(2.0 / length))
            ref[rows, :] = (jnp.cos(angle) * scale).astype(BF)
        return carry

    lax.fori_loop(0, length // step, lat_rows, 0)


def bases(cols, blocks, padded, lat_total):
    wide = padded * blocks
    return pl.pallas_call(
        lambda *refs: basis_kernel(*refs, cols=cols, blocks=blocks, padded=padded),
        out_shape=(
            jax.ShapeDtypeStruct((wide, wide), BF),
            jax.ShapeDtypeStruct((wide, wide), BF),
            jax.ShapeDtypeStruct((lat_total, lat_total), BF),
            jax.ShapeDtypeStruct((lat_total, lat_total), BF),
        ),
        out_specs=(vspec(),) * 4,
        compiler_params=params(40),
        name="bases",
    )()


def member_kernel(*refs, first, final, cols, blocks, bands, padded, coefs):
    place, field, innov_own, innov_other, taper_own, taper_other = refs[:6]
    lon_ref, lon_t_ref, lat_ref, lat_t_ref = refs[6:10]
    rest = list(refs[10:])
    so_far = None if first else rest.pop(0)
    if final:
        own_out, other_out = rest[:2]
        rest = rest[2:]
        innov, taper, weighted, inverse, acc = rest
    else:
        acc = rest.pop(0)
        innov, taper, weighted, inverse = rest
    mem = place[0]
    half = padded // 2
    wide = padded * blocks
    own_rows = pl.ds(pl.multiple_of(mem * half, half), half)
    other_rows = pl.ds(pl.multiple_of((1 - mem) * half, half), half)
    innov[:, own_rows, :] = innov_own[...]
    innov[:, other_rows, :] = innov_other[...]
    taper[mem] = taper_own[...]
    taper[1 - mem] = taper_other[...]
    weighted[...] = jnp.zeros_like(weighted)
    inverse[coefs:, :] = jnp.zeros((wide - coefs, inverse.shape[1]), BF)

    def weigh(j, carry):
        rows = pl.ds(pl.multiple_of(j * padded, padded), cols)
        for a in range(bands):
            product = field[a * blocks + j] * innov[a * blocks + j, :cols, :]
            weighted[rows, 128 * a : 128 * a + 128] = product
        return carry

    lax.fori_loop(0, blocks, weigh, 0)
    step = coefs // 3

    def spectral(i, carry):
        rows = pl.ds(pl.multiple_of(i * step, 16), step)
        zonal = jnp.dot(lon_t_ref[rows, :], weighted[...], preferred_element_type=F32).astype(BF)
        spectrum = jnp.dot(zonal, lat_ref[...], preferred_element_type=F32)
        weights = jnp.concatenate([taper[0, rows, :], taper[1, rows, :]], axis=1).astype(F32)
        tapered = (spectrum * weights).astype(BF)
        inverse[rows, :] = jnp.dot(tapered, lat_t_ref[...], preferred_element_type=F32).astype(BF)
        return carry

    lax.fori_loop(0, 3, spectral, 0)
    group = 4

    def gridded(i, carry):
        rows = pl.ds(pl.multiple_of(i * group * padded, padded), group * padded)
        localized = jnp.dot(lon_ref[rows, :], inverse[...], preferred_element_type=F32)
        for g in range(group):
            j = i * group + g
            for a in range(bands):
                spot = a * blocks + j
                piece = localized[g * padded : g * padded + cols, 128 * a : 128 * a + 128]
                piece = piece * field[spot].astype(F32)
                if not first:
                    piece = piece + so_far[spot, :cols, :]
                acc[spot, :cols, :] = piece
        return carry

    lax.fori_loop(0, blocks // group, gridded, 0)
    if final:
        own_out[...] = acc[:, own_rows, :]
        other_out[...] = acc[:, other_rows, :].astype(BF)


def member(place, field, innov, taper, tables, so_far, final, dims):
    cols, blocks, bands, padded, coefs, lat_total = dims
    spots = bands * blocks
    half = padded // 2
    wide = padded * blocks
    first = so_far is None
    operands = [place, field, *innov, *taper, *tables] + ([] if first else [so_far])
    scratch = [
        pltpu.VMEM((spots, padded, 128), BF),
        pltpu.VMEM((2, coefs, lat_total // 2), BF),
        pltpu.VMEM((wide, lat_total), BF),
        pltpu.VMEM((wide, lat_total), BF),
    ]
    if final:
        out_shape = (
            jax.ShapeDtypeStruct((spots, half, 128), F32),
            jax.ShapeDtypeStruct((spots, half, 128), BF),
        )
        out_specs = (vspec(), vspec())
        scratch.append(pltpu.VMEM((spots, padded, 128), F32))
    else:
        out_shape = jax.ShapeDtypeStruct((spots, padded, 128), F32)
        out_specs = vspec()
    return pl.pallas_call(
        lambda *refs: member_kernel(
            *refs, first=first, final=final, cols=cols, blocks=blocks, bands=bands, padded=padded, coefs=coefs
        ),
        out_shape=out_shape,
        in_specs=[sspec()] + [vspec()] * (len(operands) - 1),
        out_specs=out_specs,
        scratch_shapes=scratch,
        compiler_params=params(48),
        name="member",
    )(*operands)


def local(anomalies, taper, obs_row, obs_col, obs_level, obs_value):
    members, levels, cols, lat_rows = anomalies.shape
    bands = lax.axis_size("lat")
    blocks = lax.axis_size("lon")
    mem = lax.axis_index("mem")
    coefs = cols * blocks
    lat_total = lat_rows * bands
    padded = -(-cols // 32) * 32
    half = padded // 2
    ensemble = members * lax.axis_size("mem")
    place = jnp.stack([mem, lax.axis_index("lat") * lat_rows, lax.axis_index("lon") * cols]).astype(jnp.int32)

    chunks = [
        over_all(anomalies[i : i + bands].reshape(bands * levels, cols, lat_rows))
        for i in range(0, members, bands)
    ]

    innovation = spread(place, obs_row, obs_col, obs_level, obs_value, half, levels, bands)
    innov_own = over_all(innovation.reshape(bands * levels, half, lat_rows))
    innov_other = lax.ppermute(innov_own, "mem", SWAP)

    n_half = lat_total // 2
    taper_own = lax.dynamic_slice_in_dim(taper[0], mem * n_half, n_half, axis=1).astype(BF)
    taper_own = lax.all_gather(taper_own, "lat", axis=0, tiled=True)
    taper_other = lax.ppermute(taper_own, "mem", SWAP)

    tables = bases(cols, blocks, padded, lat_total)
    dims = (cols, blocks, bands, padded, coefs, lat_total)
    summed = None
    for i, field in enumerate(chunks):
        summed = member(
            place, field, (innov_own, innov_other), (taper_own, taper_other), tables, summed,
            i == len(chunks) - 1, dims,
        )
    own, other = summed
    arrived = lax.ppermute(other, "mem", SWAP)
    merged = (own + arrived.astype(F32)).astype(BF)
    pieces = over_all(merged).reshape(bands, levels, half, lat_rows)
    total = jnp.sum(pieces.astype(F32), axis=0) / (ensemble - 1)
    both = lax.all_gather(total, "mem", axis=0)
    return jnp.concatenate([both[0], both[1][:, : cols - half, :]], axis=1)


def solution(mesh):
    in_specs = (
        P("mem", None, "lon", "lat"),
        P("lon", "lat", None),
        P("lat", "lon"),
        P("lat", "lon"),
        P("lat", "lon"),
        P("lat", "lon"),
    )
    out_specs = P(None, "lon", "lat")
    return jax.shard_map(local, mesh=mesh, in_specs=in_specs, out_specs=out_specs, check_vma=False)
```

```python
import math

import jax
import jax.numpy as jnp
from jax import lax
from jax.experimental import pallas as pl
from jax.experimental.pallas import tpu as pltpu
from jax.sharding import PartitionSpec as P


BF = jnp.bfloat16
F32 = jnp.float32
LL = ("lat", "lon")
SWAP = [(0, 1), (1, 0)]
RING = 4


def vspec():
    return pl.BlockSpec(memory_space=pltpu.VMEM)


def sspec():
    return pl.BlockSpec(memory_space=pltpu.SMEM)


def params(mib, **more):
    return pltpu.CompilerParams(vmem_limit_bytes=mib * 1024 * 1024, **more)


def cost(flops):
    return pl.CostEstimate(flops=int(flops), bytes_accessed=1 << 20, transcendentals=0)


def over_all(x):
    return lax.all_to_all(x, LL, split_axis=0, concat_axis=0, tiled=True)


def shift_lat(x, s):
    return lax.ppermute(x, "lat", [(i, (i + s) % RING) for i in range(RING)])


def shift_z(x, s):
    return lax.ppermute(
        x, "lon", [(z * RING + i, (z + s) % RING * RING + i) for z in range(RING) for i in range(RING)]
    )


def shift_x(x, s):
    return lax.ppermute(
        x, "lon", [(z * RING + i, z * RING + (i + s) % RING) for z in range(RING) for i in range(RING)]
    )


def swap(x):
    return lax.ppermute(x, "mem", SWAP)


def relayout_kernel(in_ref, out_ref, *, split, cols, levels, padded):
    size = 16 * levels
    to = lax.broadcasted_iota(jnp.int32, (size, size), 0)
    frm = lax.broadcasted_iota(jnp.int32, (size, size), 1)
    turn = jnp.where(frm == (to & 15) * levels + (to >> 4), 1.0, 0.0).astype(BF)
    for start in range(0, padded, 16):
        have = min(16, cols - start)
        parts = []
        for p in range(2):
            block = in_ref[(p, 0) if split else (0, p)][start : start + have]
            parts.append(block.reshape(have * levels, 128))
        both = jnp.concatenate(parts, axis=1)
        if have < 16:
            both = jnp.concatenate([both, jnp.zeros(((16 - have) * levels, 256), BF)], axis=0)
        turned = jnp.dot(turn, both, preferred_element_type=F32).astype(BF)
        for l in range(levels):
            for p in range(2):
                piece = turned[16 * l : 16 * l + 16, 128 * p : 128 * p + 128]
                if split:
                    out_ref[l, p, start : start + 16, :] = piece
                else:
                    out_ref[p * levels + l, 0, start : start + 16, :] = piece


def relayout(fields, pair, padded):
    rounds, bands, cols, levels, lanes = fields.shape
    kernel = lambda i, o: relayout_kernel(i, o, split=pair, cols=cols, levels=levels, padded=padded)
    if pair:
        return pl.pallas_call(
            kernel,
            grid=(bands,),
            in_specs=[pl.BlockSpec((2, 1, cols, levels, lanes), lambda g: (0, g, 0, 0, 0))],
            out_specs=pl.BlockSpec((levels, 2, padded, lanes), lambda g: (g, 0, 0, 0)),
            out_shape=jax.ShapeDtypeStruct((bands * levels, 2, padded, lanes), BF),
            compiler_params=params(12),
            name="relayout_pair",
        )(fields)
    return pl.pallas_call(
        kernel,
        grid=(bands // 2,),
        in_specs=[pl.BlockSpec((1, 2, cols, levels, lanes), lambda g: (rounds - 1, g, 0, 0, 0))],
        out_specs=pl.BlockSpec((2 * levels, 1, padded, lanes), lambda g: (g, 0, 0, 0)),
        out_shape=jax.ShapeDtypeStruct((bands * levels, 1, padded, lanes), BF),
        compiler_params=params(12),
        name="relayout_last",
    )(fields)


def spread_kernel(place, row_ref, col_ref, level_ref, value_ref, out_ref, acc, *, half, levels, cols):
    mem, lat, z, x = place[0], place[1], place[2], place[3]
    slots = levels * half
    col_start = (z * RING + x) * cols + mem * half
    acc[...] = jnp.zeros_like(acc)
    slot_ids = lax.broadcasted_iota(jnp.int32, (slots, 128), 0)
    row_ids = lax.broadcasted_iota(jnp.int32, (128, 128), 0)

    def add_group(g, carry):
        rows = pl.ds(pl.multiple_of(g * 8, 8), 8)
        within = col_ref[rows, :] - col_start
        inside = (within >= 0) & (within < half)
        keys = jnp.where(inside, level_ref[rows, :] * half + within, -1)
        lat_row = row_ref[rows, :] - lat * 128
        value = value_ref[rows, :]
        high = value.astype(BF).astype(F32)
        middle = value - high
        left = []
        right = []
        for r in range(8):
            hit = slot_ids == keys[r : r + 1, :]
            left.append(jnp.where(hit, 1.0, 0.0).astype(BF))
            row_hit = row_ids == lat_row[r : r + 1, :]
            top = jnp.where(row_hit, high[r : r + 1, :], 0.0)
            low = jnp.where(row_hit, middle[r : r + 1, :], 0.0)
            right.append(jnp.concatenate([top, low], axis=0).astype(BF))
        acc[...] += lax.dot_general(
            jnp.concatenate(left, axis=1),
            jnp.concatenate(right, axis=1),
            (((1,), (1,)), ((), ())),
            preferred_element_type=F32,
        )
        return carry

    lax.fori_loop(0, row_ref.shape[0] // 8, add_group, 0)
    for s in range(RING):
        for t in range(RING):
            level = lax.rem(z + s, RING) * RING + lax.rem(x + t, RING)
            rows = pl.ds(pl.multiple_of(level * half, 8), half)
            out_ref[s, t] = (acc[rows, :128] + acc[rows, 128:]).astype(BF)


def spread(place, obs_row, obs_col, obs_level, obs_value, half, levels, cols):
    return pl.pallas_call(
        lambda *refs: spread_kernel(*refs, half=half, levels=levels, cols=cols),
        out_shape=jax.ShapeDtypeStruct((RING, RING, half, 128), BF),
        in_specs=[sspec()] + [vspec()] * 4,
        out_specs=vspec(),
        scratch_shapes=[pltpu.VMEM((levels * half, 256), F32)],
        compiler_params=params(14),
        cost_estimate=cost(6e9),
        name="spread",
    )(place, obs_row, obs_col, obs_level, obs_value)


def turn_cos(turns):
    near = 0.25 - jnp.abs(turns - jnp.floor(turns + 0.5))
    square = near * near
    value = jnp.full_like(square, -15.094642576822990)
    for factor in (42.058693944897653, -76.705859753061386, 81.605249276075055, -41.341702240399755):
        value = value * square + factor
    return near * (value * square + 6.283185307179586)


def basis_kernel(lon_ref, lon_t_ref, lat_ref, lat_t_ref, *, cols, blocks, padded):
    total = cols * blocks
    half = total // 2
    tiles = lon_ref.shape[1] // 128
    lanes = lax.broadcasted_iota(jnp.int32, (padded, 128), 1)

    def turns_of(product):
        whole = (product.astype(F32) * (1.0 / total)).astype(jnp.int32)
        return (product - whole * total).astype(F32) * (1.0 / total)

    def lon_rows(j, carry):
        within = lax.broadcasted_iota(jnp.int32, (padded, 128), 0)
        x = within + cols * j
        fine = turns_of(x * lanes)
        coarse = turns_of(x * (lanes * 128))
        fine_cos = turn_cos(fine)
        fine_sin = turn_cos(fine - 0.25)
        scale = jnp.where(within < cols, math.sqrt(2.0 / total), 0.0)
        coarse_cos = turn_cos(coarse) * scale
        coarse_sin = turn_cos(coarse - 0.25) * scale
        sign = jnp.where((x & 1) == 0, 1.0, -1.0)
        rows = pl.ds(pl.multiple_of(j * padded, padded), padded)
        for t in range(tiles):
            c = lanes + 128 * t
            cos_t = coarse_cos[:, t : t + 1]
            sin_t = coarse_sin[:, t : t + 1]
            parts = []
            if 128 * t <= half:
                parts.append(fine_cos * cos_t - fine_sin * sin_t)
            if 128 * t + 127 > half:
                parts.append((fine_sin * cos_t + fine_cos * sin_t) * sign)
            value = parts[0] if len(parts) == 1 else jnp.where(c <= half, parts[0], parts[1])
            if t == 0 or 128 * t <= half < 128 * t + 128:
                value = jnp.where((c == 0) | (c == half), value * math.sqrt(0.5), value)
            if 128 * t + 127 >= total:
                value = jnp.where(c < total, value, 0.0)
            lon_ref[rows, 128 * t : 128 * t + 128] = value.astype(BF)
        return carry

    lax.fori_loop(0, blocks, lon_rows, 0)
    for t in range(tiles):
        strip = lon_ref[:, 128 * t : 128 * t + 128].astype(F32)
        lon_t_ref[128 * t : 128 * t + 128, :] = strip.T.astype(BF)

    length = lat_ref.shape[0]
    step = 64

    def lat_rows(i, carry):
        shape = (step, length)
        down = lax.broadcasted_iota(jnp.int32, shape, 0) + step * i
        across = lax.broadcasted_iota(jnp.int32, shape, 1)
        rows = pl.ds(pl.multiple_of(i * step, step), step)
        for grid, mode, ref in ((down, across, lat_ref), (across, down, lat_t_ref)):
            phase = (mode * (2 * grid + 1)) & (4 * length - 1)
            scale = jnp.where(mode == 0, 1.0 / math.sqrt(length), math.sqrt(2.0 / length))
            ref[rows, :] = (turn_cos(phase.astype(F32) * (0.25 / length)) * scale).astype(BF)
        return carry

    lax.fori_loop(0, length // step, lat_rows, 0)


def bases(cols, blocks, padded, lat_total):
    wide = padded * blocks
    return pl.pallas_call(
        lambda *refs: basis_kernel(*refs, cols=cols, blocks=blocks, padded=padded),
        out_shape=(
            jax.ShapeDtypeStruct((wide, wide), BF),
            jax.ShapeDtypeStruct((wide, wide), BF),
            jax.ShapeDtypeStruct((lat_total, lat_total), BF),
            jax.ShapeDtypeStruct((lat_total, lat_total), BF),
        ),
        out_specs=(vspec(),) * 4,
        compiler_params=params(20),
        cost_estimate=cost(12e9),
        name="bases",
    )()


def arrange_kernel(place, own, other, innov, taper, *, half, blocks, rows_each):
    mem, lat, z, x = place[0], place[1], place[2], place[3]
    packed = blocks * half
    for ref, side in ((own, mem), (other, 1 - mem)):
        rows = pl.ds(pl.multiple_of(side * half, 16), half)
        for u in range(RING):
            band = lax.rem(lat + RING - u, RING)
            for t in range(RING):
                for s in range(RING):
                    j = lax.rem(z + RING - s, RING) * RING + lax.rem(x + RING - t, RING)
                    start = (t * RING + s) * half
                    innov[band * blocks + j, rows, :] = ref[u, start : start + half, :]
            into = pl.ds(pl.multiple_of(band * rows_each, 8), rows_each)
            for q in range(2):
                start = packed + q * rows_each
                taper[2 * side + q, into, :] = ref[u, start : start + rows_each, :]


def arrange(place, own, other, half, blocks, padded, rows_each):
    return pl.pallas_call(
        lambda *refs: arrange_kernel(*refs, half=half, blocks=blocks, rows_each=rows_each),
        out_shape=(
            jax.ShapeDtypeStruct((RING * blocks, padded, 128), BF),
            jax.ShapeDtypeStruct((4, RING * rows_each, 128), BF),
        ),
        in_specs=[sspec(), vspec(), vspec()],
        out_specs=(vspec(), vspec()),
        compiler_params=params(12),
        cost_estimate=cost(1e9),
        name="arrange",
    )(place, own, other)


def member_kernel(*refs, first, final, blocks, bands, padded, coefs):
    place, field, innov_hbm, taper_hbm, lon_hbm, lon_t_hbm, lat_hbm, lat_t_hbm = refs[:8]
    rest = list(refs[8:])
    so_far_hbm = None if first else rest.pop(0)
    if final:
        own_out, other_out, acc = rest[0], rest[1], rest.pop()
        rest = rest[2:]
    else:
        acc = rest.pop(0)
    weighted, inverse, innov, taper, lon_ref, lon_t_ref, lat_ref, lat_t_ref, sems = rest
    wide = padded * blocks
    step = coefs // 3
    group = 4
    tall = group * padded
    count = iter(range(16))

    def fetch(source, target):
        copy = pltpu.make_async_copy(source, target, sems.at[next(count)])
        copy.start()
        return copy

    innov_copy = fetch(innov_hbm, innov)
    lon_t_copies = [fetch(lon_t_hbm.at[pl.ds(0, step)], lon_t_ref.at[pl.ds(0, step)])]
    lat_copies = [fetch(lat_hbm, lat_ref), fetch(taper_hbm, taper), fetch(lat_t_hbm, lat_t_ref)]
    lon_t_copies += [
        fetch(lon_t_hbm.at[pl.ds(r * step, step)], lon_t_ref.at[pl.ds(r * step, step)]) for r in (1, 2)
    ]
    lon_copies = [
        fetch(lon_hbm.at[pl.ds(b * tall, tall)], lon_ref.at[pl.ds(b * tall, tall)]) for b in range(blocks // group)
    ]
    if not first:
        lon_copies.append(fetch(so_far_hbm, acc))
    inverse[coefs:, :] = jnp.zeros((wide - coefs, inverse.shape[1]), BF)
    innov_copy.wait()

    def weigh(i):
        def body(j, carry):
            rows = pl.ds(pl.multiple_of(j * padded, padded), padded)
            for a in range(bands):
                spot = a * blocks + j
                weighted[rows, 128 * a : 128 * a + 128] = field[spot, i] * innov[spot]
            return carry

        lax.fori_loop(0, blocks, body, 0)

    def spectral(r, carry):
        rows = pl.ds(pl.multiple_of(r * step, 16), step)
        zonal = jnp.dot(lon_t_ref[rows, :], weighted[...], preferred_element_type=F32).astype(BF)
        spectrum = jnp.dot(zonal, lat_ref[...], preferred_element_type=F32)
        weights = jnp.concatenate([taper[q, rows, :] for q in range(4)], axis=1).astype(F32)
        tapered = (spectrum * weights).astype(BF)
        inverse[rows, :] = jnp.dot(tapered, lat_t_ref[...], preferred_element_type=F32).astype(BF)
        return carry

    def gridded(i):
        def body(b, carry):
            rows = pl.ds(pl.multiple_of(b * tall, tall), tall)
            localized = jnp.dot(lon_ref[rows, :], inverse[...], preferred_element_type=F32)
            for g in range(group):
                for a in range(bands):
                    spot = a * blocks + b * group + g
                    piece = localized[g * padded : (g + 1) * padded, 128 * a : 128 * a + 128]
                    piece = piece * field[spot, i].astype(F32)
                    acc[spot] = piece if first and i == 0 else piece + acc[spot]
            return carry

        lax.fori_loop(0, blocks // group, body, 0)

    for i in range(field.shape[1]):
        weigh(i)
        if i == 0:
            for copy in [lon_t_copies[0], *lat_copies]:
                copy.wait()
            for copy in lon_t_copies[1:]:
                copy.wait()
        lax.fori_loop(0, coefs // step, spectral, 0)
        if i == 0:
            for copy in lon_copies:
                copy.wait()
        gridded(i)
    if final:
        half = padded // 2
        mem = place[0]
        own_out[...] = acc[:, pl.ds(pl.multiple_of(mem * half, half), half), :]
        other_out[...] = acc[:, pl.ds(pl.multiple_of((1 - mem) * half, half), half), :].astype(BF)


def member(place, field, innov, taper, tables, so_far, final, dims):
    _, blocks, bands, padded, coefs, lat_total = dims
    spots = bands * blocks
    half = padded // 2
    wide = padded * blocks
    first = so_far is None
    far = [innov, taper, *tables] + ([] if first else [so_far])
    scratch = [pltpu.VMEM((wide, lat_total), BF), pltpu.VMEM((wide, lat_total), BF)]
    scratch += [pltpu.VMEM(array.shape, array.dtype) for array in (innov, taper, *tables)]
    scratch.append(pltpu.SemaphoreType.DMA((16,)))
    if final:
        out_shape = (
            jax.ShapeDtypeStruct((spots, half, 128), F32),
            jax.ShapeDtypeStruct((spots, half, 128), BF),
        )
        out_specs = (vspec(), vspec())
        scratch.append(pltpu.VMEM((spots, padded, 128), F32))
    else:
        out_shape = jax.ShapeDtypeStruct((spots, padded, 128), F32)
        out_specs = vspec()
    return pl.pallas_call(
        lambda *refs: member_kernel(
            *refs, first=first, final=final, blocks=blocks, bands=bands, padded=padded, coefs=coefs
        ),
        out_shape=out_shape,
        in_specs=[sspec(), vspec()] + [pl.BlockSpec(memory_space=pltpu.HBM)] * len(far),
        out_specs=out_specs,
        scratch_shapes=scratch,
        compiler_params=params(44),
        cost_estimate=cost(field.shape[1] * 6e9),
        name="member_last" if final else "member_pair",
    )(place, field, *far)


def finish_kernel(place, own, other, out, *, levels, cols, half, scale):
    mem = place[0]
    bands = own.shape[0] // levels
    for side in range(2):
        rows = min(half, cols - side * half)
        for l in range(levels):
            mine = sum(own[a * levels + l].astype(F32) for a in range(bands))
            theirs = sum(other[a * levels + l].astype(F32) for a in range(bands))
            total = jnp.where(mem == side, mine, theirs) * scale
            out[side * half : side * half + rows, l, :] = total[:rows]


def finish(place, own, other, levels, cols, half, scale):
    return pl.pallas_call(
        lambda *refs: finish_kernel(*refs, levels=levels, cols=cols, half=half, scale=scale),
        out_shape=jax.ShapeDtypeStruct((cols, levels, 128), F32),
        in_specs=[sspec(), vspec(), vspec()],
        out_specs=vspec(),
        compiler_params=params(12),
        name="finish",
    )(place, own, other)


def local(anomalies, taper, obs_row, obs_col, obs_level, obs_value):
    members, levels, cols, lat_rows = anomalies.shape
    bands = lax.axis_size("lat")
    blocks = lax.axis_size("lon")
    mem, lat, lon = lax.axis_index("mem"), lax.axis_index("lat"), lax.axis_index("lon")
    coefs = cols * blocks
    lat_total = lat_rows * bands
    padded = -(-cols // 32) * 32
    half = padded // 2
    ensemble = members * lax.axis_size("mem")
    place = jnp.stack([mem, lat, lon // RING, lon % RING]).astype(jnp.int32)

    by_round = jnp.transpose(anomalies, (0, 2, 1, 3)).reshape(members // bands, bands, cols, levels, lat_rows)
    pair_out, early = lax.optimization_barrier((relayout(by_round, True, padded), place))
    pair = over_all(pair_out)
    last = over_all(relayout(by_round, False, padded))

    blocks_out = spread(early, obs_row, obs_col, obs_level, obs_value, half, levels, cols)
    by_z = [blocks_out[0]] + [shift_z(blocks_out[s], s) for s in range(1, RING)]
    by_x = []
    for t in range(RING):
        column = jnp.concatenate([piece[t] for piece in by_z], axis=0)
        by_x.append(column if t == 0 else shift_x(column, t))

    n_half = lat_total // 2
    coef_rows = taper.shape[1]
    taper_own = lax.dynamic_slice_in_dim(taper[0], mem * n_half, n_half, axis=1).astype(BF)
    payload = jnp.concatenate(by_x + [taper_own[:, :128], taper_own[:, 128:]], axis=0)
    own = jnp.stack([payload] + [shift_lat(payload, u) for u in range(1, RING)])
    other = swap(own)
    innov, weights = arrange(place, own, other, half, blocks, padded, coef_rows)

    tables = bases(cols, blocks, padded, lat_total)
    dims = (cols, blocks, bands, padded, coefs, lat_total)
    summed = member(place, pair, innov, weights, tables, None, False, dims)
    mine, theirs = member(place, last, innov, weights, tables, summed, True, dims)
    merged = (mine + swap(theirs).astype(F32)).astype(BF)
    pieces = over_all(merged)
    out = finish(place, pieces, swap(pieces), levels, cols, half, 1.0 / (ensemble - 1))
    return jnp.transpose(out, (1, 0, 2))


def solution(mesh):
    in_specs = (
        P("mem", None, "lon", "lat"),
        P("lon", "lat", None),
        P("lat", "lon"),
        P("lat", "lon"),
        P("lat", "lon"),
        P("lat", "lon"),
    )
    out_specs = P(None, "lon", "lat")

    return jax.shard_map(local, mesh=mesh, in_specs=in_specs, out_specs=out_specs, check_vma=False)
```

```python
import math

import jax
import jax.numpy as jnp
from jax import lax
from jax.experimental import pallas as pl
from jax.experimental.pallas import tpu as pltpu
from jax.sharding import PartitionSpec as P


BF = jnp.bfloat16
F32 = jnp.float32
LL = ("lat", "lon")
SWAP = [(0, 1), (1, 0)]
RING = 4


def vspec():
    return pl.BlockSpec(memory_space=pltpu.VMEM)


def sspec():
    return pl.BlockSpec(memory_space=pltpu.SMEM)


def params(mib, **more):
    return pltpu.CompilerParams(vmem_limit_bytes=mib * 1024 * 1024, **more)


def cost(flops):
    return pl.CostEstimate(flops=int(flops), bytes_accessed=1 << 20, transcendentals=0)


def over_all(x):
    return lax.all_to_all(x, LL, split_axis=0, concat_axis=0, tiled=True)


def shift_lat(x, s):
    return lax.ppermute(x, "lat", [(i, (i + s) % RING) for i in range(RING)])


def swap(x):
    return lax.ppermute(x, "mem", SWAP)


def relayout_kernel(in_ref, extra, out_ref, *, cols, levels, padded):
    split = extra is not None
    size = 16 * levels
    to = lax.broadcasted_iota(jnp.int32, (size, size), 0)
    frm = lax.broadcasted_iota(jnp.int32, (size, size), 1)
    turn = jnp.where(frm == (to & 15) * levels + (to >> 4), 1.0, 0.0).astype(BF)
    for start in range(0, padded, 16):
        have = min(16, cols - start)
        parts = []
        for p in range(2):
            block = in_ref[(p, 0) if split else (0, p)][start : start + have]
            parts.append(block.reshape(have * levels, 128))
        both = jnp.concatenate(parts, axis=1)
        if have < 16:
            both = jnp.concatenate([both, jnp.zeros(((16 - have) * levels, 256), BF)], axis=0)
        turned = jnp.dot(turn, both, preferred_element_type=F32).astype(BF)
        for l in range(levels):
            for p in range(2):
                piece = turned[16 * l : 16 * l + 16, 128 * p : 128 * p + 128]
                if split:
                    out_ref[l, p * padded + start : p * padded + start + 16, :] = piece
                else:
                    out_ref[p * levels + l, start : start + 16, :] = piece
    if split:
        out_ref[:, 2 * padded :, :] = extra[...]


def relayout_pair(fields, extra, padded):
    _, bands, cols, levels, lanes = fields.shape
    rows = 2 * padded + extra.shape[1]
    return pl.pallas_call(
        lambda i, e, o: relayout_kernel(i, e, o, cols=cols, levels=levels, padded=padded),
        grid=(bands,),
        in_specs=[
            pl.BlockSpec((2, 1, cols, levels, lanes), lambda g: (0, g, 0, 0, 0)),
            pl.BlockSpec(extra.shape, lambda g: (0, 0, 0)),
        ],
        out_specs=pl.BlockSpec((levels, rows, lanes), lambda g: (g, 0, 0)),
        out_shape=jax.ShapeDtypeStruct((bands * levels, rows, lanes), BF),
        compiler_params=params(58),
        name="relayout_pair",
    )(fields, extra)


def relayout_last(fields, padded):
    rounds, bands, cols, levels, lanes = fields.shape
    return pl.pallas_call(
        lambda i, o: relayout_kernel(i, None, o, cols=cols, levels=levels, padded=padded),
        grid=(bands // 2,),
        in_specs=[pl.BlockSpec((1, 2, cols, levels, lanes), lambda g: (rounds - 1, g, 0, 0, 0))],
        out_specs=pl.BlockSpec((2 * levels, padded, lanes), lambda g: (g, 0, 0)),
        out_shape=jax.ShapeDtypeStruct((bands * levels, padded, lanes), BF),
        compiler_params=params(58),
        name="relayout_last",
    )(fields)


def spread_kernel(place, row_ref, col_ref, level_ref, value_ref, out_ref, acc, *, half, levels, cols):
    mem, lat, lon = place[0], place[1], place[2]
    slots = levels * half
    col_start = lon * cols + mem * half
    acc[...] = jnp.zeros_like(acc)
    slot_ids = lax.broadcasted_iota(jnp.int32, (slots, 128), 0)
    row_ids = lax.broadcasted_iota(jnp.int32, (128, 128), 0)

    def add_group(g, carry):
        rows = pl.ds(pl.multiple_of(g * 8, 8), 8)
        within = col_ref[rows, :] - col_start
        inside = (within >= 0) & (within < half)
        keys = jnp.where(inside, level_ref[rows, :] * half + within, -1)
        lat_row = row_ref[rows, :] - lat * 128
        value = value_ref[rows, :]
        high = value.astype(BF).astype(F32)
        middle = value - high
        left = []
        right = []
        for r in range(8):
            hit = slot_ids == keys[r : r + 1, :]
            left.append(jnp.where(hit, 1.0, 0.0).astype(BF))
            row_hit = row_ids == lat_row[r : r + 1, :]
            top = jnp.where(row_hit, high[r : r + 1, :], 0.0)
            low = jnp.where(row_hit, middle[r : r + 1, :], 0.0)
            right.append(jnp.concatenate([top, low], axis=0).astype(BF))
        acc[...] += lax.dot_general(
            jnp.concatenate(left, axis=1),
            jnp.concatenate(right, axis=1),
            (((1,), (1,)), ((), ())),
            preferred_element_type=F32,
        )
        return carry

    lax.fori_loop(0, row_ref.shape[0] // 8, add_group, 0)
    out_ref[...] = (acc[:, :128] + acc[:, 128:]).astype(BF).reshape(levels, half, 128)


def spread(place, obs_row, obs_col, obs_level, obs_value, half, levels, cols):
    return pl.pallas_call(
        lambda *refs: spread_kernel(*refs, half=half, levels=levels, cols=cols),
        out_shape=jax.ShapeDtypeStruct((levels, half, 128), BF),
        in_specs=[sspec()] + [vspec()] * 4,
        out_specs=vspec(),
        scratch_shapes=[pltpu.VMEM((levels * half, 256), F32)],
        compiler_params=params(14),
        cost_estimate=cost(6e9),
        name="spread",
    )(place, obs_row, obs_col, obs_level, obs_value)


def turn_cos(turns):
    near = 0.25 - jnp.abs(turns - jnp.floor(turns + 0.5))
    square = near * near
    value = jnp.full_like(square, -15.094642576822990)
    for factor in (42.058693944897653, -76.705859753061386, 81.605249276075055, -41.341702240399755):
        value = value * square + factor
    return near * (value * square + 6.283185307179586)


def basis_kernel(lon_ref, lon_t_ref, lat_ref, lat_t_ref, *, cols, blocks, padded):
    total = cols * blocks
    half = total // 2
    tiles = lon_ref.shape[1] // 128
    lanes = lax.broadcasted_iota(jnp.int32, (padded, 128), 1)

    def turns_of(product):
        whole = (product.astype(F32) * (1.0 / total)).astype(jnp.int32)
        return (product - whole * total).astype(F32) * (1.0 / total)

    def lon_rows(j, carry):
        within = lax.broadcasted_iota(jnp.int32, (padded, 128), 0)
        x = within + cols * j
        fine = turns_of(x * lanes)
        coarse = turns_of(x * (lanes * 128))
        fine_cos = turn_cos(fine)
        fine_sin = turn_cos(fine - 0.25)
        scale = jnp.where(within < cols, math.sqrt(2.0 / total), 0.0)
        coarse_cos = turn_cos(coarse) * scale
        coarse_sin = turn_cos(coarse - 0.25) * scale
        sign = jnp.where((x & 1) == 0, 1.0, -1.0)
        rows = pl.ds(pl.multiple_of(j * padded, padded), padded)
        for t in range(tiles):
            c = lanes + 128 * t
            cos_t = coarse_cos[:, t : t + 1]
            sin_t = coarse_sin[:, t : t + 1]
            parts = []
            if 128 * t <= half:
                parts.append(fine_cos * cos_t - fine_sin * sin_t)
            if 128 * t + 127 > half:
                parts.append((fine_sin * cos_t + fine_cos * sin_t) * sign)
            value = parts[0] if len(parts) == 1 else jnp.where(c <= half, parts[0], parts[1])
            if t == 0 or 128 * t <= half < 128 * t + 128:
                value = jnp.where((c == 0) | (c == half), value * math.sqrt(0.5), value)
            if 128 * t + 127 >= total:
                value = jnp.where(c < total, value, 0.0)
            lon_ref[rows, 128 * t : 128 * t + 128] = value.astype(BF)
        return carry

    lax.fori_loop(0, blocks, lon_rows, 0)
    for t in range(tiles):
        strip = lon_ref[:, 128 * t : 128 * t + 128].astype(F32)
        lon_t_ref[128 * t : 128 * t + 128, :] = strip.T.astype(BF)

    length = lat_ref.shape[0]
    step = 64

    def lat_rows(i, carry):
        shape = (step, length)
        down = lax.broadcasted_iota(jnp.int32, shape, 0) + step * i
        across = lax.broadcasted_iota(jnp.int32, shape, 1)
        rows = pl.ds(pl.multiple_of(i * step, step), step)
        for grid, mode, ref in ((down, across, lat_ref), (across, down, lat_t_ref)):
            phase = (mode * (2 * grid + 1)) & (4 * length - 1)
            scale = jnp.where(mode == 0, 1.0 / math.sqrt(length), math.sqrt(2.0 / length))
            ref[rows, :] = (turn_cos(phase.astype(F32) * (0.25 / length)) * scale).astype(BF)
        return carry

    lax.fori_loop(0, length // step, lat_rows, 0)


def bases(cols, blocks, padded, lat_total):
    wide = padded * blocks
    return pl.pallas_call(
        lambda *refs: basis_kernel(*refs, cols=cols, blocks=blocks, padded=padded),
        out_shape=(
            jax.ShapeDtypeStruct((wide, wide), BF),
            jax.ShapeDtypeStruct((wide, wide), BF),
            jax.ShapeDtypeStruct((lat_total, lat_total), BF),
            jax.ShapeDtypeStruct((lat_total, lat_total), BF),
        ),
        out_specs=(vspec(),) * 4,
        compiler_params=params(58),
        cost_estimate=cost(12e9),
        name="bases",
    )()


def arrange_kernel(place, own, other, taper, *, rows_each):
    mem, lat = place[0], place[1]
    for ref, side in ((own, mem), (other, 1 - mem)):
        for u in range(RING):
            into = pl.ds(pl.multiple_of(lax.rem(lat + RING - u, RING) * rows_each, 8), rows_each)
            for q in range(2):
                taper[2 * side + q, into, :] = ref[u, :, 128 * q : 128 * q + 128]


def arrange(place, own, other):
    rows_each = own.shape[1]
    return pl.pallas_call(
        lambda *refs: arrange_kernel(*refs, rows_each=rows_each),
        out_shape=jax.ShapeDtypeStruct((4, RING * rows_each, 128), BF),
        in_specs=[sspec(), vspec(), vspec()],
        out_specs=vspec(),
        compiler_params=params(12),
        cost_estimate=cost(1e9),
        name="arrange",
    )(place, own, other)


def member_kernel(*refs, first, final, blocks, bands, padded, coefs):
    place, field, pair_hbm, other_hbm, taper_hbm, lon_hbm, lon_t_hbm, lat_hbm, lat_t_hbm = refs[:9]
    rest = list(refs[9:])
    so_far_hbm = None if first else rest.pop(0)
    if final:
        own_out, other_out, acc = rest[0], rest[1], rest.pop()
        rest = rest[2:]
    else:
        acc = rest.pop(0)
    weighted, inverse, innov, taper, lon_ref, lon_t_ref, lat_ref, lat_t_ref, sems = rest
    wide = padded * blocks
    step = coefs // 3
    group = 4
    tall = group * padded
    count = iter(range(16))

    def fetch(source, target):
        copy = pltpu.make_async_copy(source, target, sems.at[next(count)])
        copy.start()
        return copy

    half = padded // 2
    mem = place[0]
    own_rows = pl.ds(pl.multiple_of(mem * half, half), half)
    other_rows = pl.ds(pl.multiple_of((1 - mem) * half, half), half)
    innov_copies = [
        fetch(pair_hbm.at[:, pl.ds(2 * padded, half), :], innov.at[:, own_rows, :]),
        fetch(other_hbm, innov.at[:, other_rows, :]),
    ]
    lon_t_copies = [fetch(lon_t_hbm.at[pl.ds(0, step)], lon_t_ref.at[pl.ds(0, step)])]
    lat_copies = [fetch(lat_hbm, lat_ref), fetch(taper_hbm, taper), fetch(lat_t_hbm, lat_t_ref)]
    lon_t_copies += [
        fetch(lon_t_hbm.at[pl.ds(r * step, step)], lon_t_ref.at[pl.ds(r * step, step)]) for r in (1, 2)
    ]
    lon_copies = [
        fetch(lon_hbm.at[pl.ds(b * tall, tall)], lon_ref.at[pl.ds(b * tall, tall)]) for b in range(blocks // group)
    ]
    if not first:
        lon_copies.append(fetch(so_far_hbm, acc))
    inverse[coefs:, :] = jnp.zeros((wide - coefs, inverse.shape[1]), BF)
    for copy in innov_copies:
        copy.wait()

    def weigh(i):
        def body(j, carry):
            rows = pl.ds(pl.multiple_of(j * padded, padded), padded)
            for a in range(bands):
                spot = a * blocks + j
                weighted[rows, 128 * a : 128 * a + 128] = field[spot, i * padded : (i + 1) * padded, :] * innov[spot]
            return carry

        lax.fori_loop(0, blocks, body, 0)

    def spectral(r, carry):
        rows = pl.ds(pl.multiple_of(r * step, 16), step)
        zonal = jnp.dot(lon_t_ref[rows, :], weighted[...], preferred_element_type=F32).astype(BF)
        spectrum = jnp.dot(zonal, lat_ref[...], preferred_element_type=F32)
        weights = jnp.concatenate([taper[q, rows, :] for q in range(4)], axis=1).astype(F32)
        tapered = (spectrum * weights).astype(BF)
        inverse[rows, :] = jnp.dot(tapered, lat_t_ref[...], preferred_element_type=F32).astype(BF)
        return carry

    def gridded(i):
        def body(b, carry):
            rows = pl.ds(pl.multiple_of(b * tall, tall), tall)
            localized = jnp.dot(lon_ref[rows, :], inverse[...], preferred_element_type=F32)
            for g in range(group):
                for a in range(bands):
                    spot = a * blocks + b * group + g
                    piece = localized[g * padded : (g + 1) * padded, 128 * a : 128 * a + 128]
                    piece = piece * field[spot, i * padded : (i + 1) * padded, :].astype(F32)
                    acc[spot] = piece if first and i == 0 else piece + acc[spot]
            return carry

        lax.fori_loop(0, blocks // group, body, 0)

    for i in range(field.shape[1] // padded):
        weigh(i)
        if i == 0:
            for copy in [lon_t_copies[0], *lat_copies]:
                copy.wait()
            for copy in lon_t_copies[1:]:
                copy.wait()
        lax.fori_loop(0, coefs // step, spectral, 0)
        if i == 0:
            for copy in lon_copies:
                copy.wait()
        gridded(i)
    if final:
        own_out[...] = acc[:, own_rows, :]
        other_out[...] = acc[:, other_rows, :].astype(BF)


def member(place, field, pair, other, taper, tables, so_far, final, dims):
    _, blocks, bands, padded, coefs, lat_total = dims
    spots = bands * blocks
    half = padded // 2
    wide = padded * blocks
    first = so_far is None
    far = [pair, other, taper, *tables] + ([] if first else [so_far])
    scratch = [pltpu.VMEM((wide, lat_total), BF), pltpu.VMEM((wide, lat_total), BF)]
    scratch.append(pltpu.VMEM((spots, padded, 128), BF))
    scratch += [pltpu.VMEM(array.shape, array.dtype) for array in (taper, *tables)]
    scratch.append(pltpu.SemaphoreType.DMA((16,)))
    if final:
        out_shape = (
            jax.ShapeDtypeStruct((spots, half, 128), F32),
            jax.ShapeDtypeStruct((spots, half, 128), BF),
        )
        out_specs = (vspec(), vspec())
        scratch.append(pltpu.VMEM((spots, padded, 128), F32))
    else:
        out_shape = jax.ShapeDtypeStruct((spots, padded, 128), F32)
        out_specs = vspec()
    return pl.pallas_call(
        lambda *refs: member_kernel(
            *refs, first=first, final=final, blocks=blocks, bands=bands, padded=padded, coefs=coefs
        ),
        out_shape=out_shape,
        in_specs=[sspec(), vspec()] + [pl.BlockSpec(memory_space=pltpu.HBM)] * len(far),
        out_specs=out_specs,
        scratch_shapes=scratch,
        compiler_params=params(60),
        cost_estimate=cost(field.shape[1] // padded * 6e9),
        name="member_last" if final else "member_pair",
    )(place, field, *far)


def finish_kernel(place, own, other, out, *, levels, cols, half, scale):
    mem = place[0]
    bands = own.shape[0] // levels
    for side in range(2):
        rows = min(half, cols - side * half)
        for l in range(levels):
            mine = sum(own[a * levels + l].astype(F32) for a in range(bands))
            theirs = sum(other[a * levels + l].astype(F32) for a in range(bands))
            total = jnp.where(mem == side, mine, theirs) * scale
            out[side * half : side * half + rows, l, :] = total[:rows]


def finish(place, own, other, levels, cols, half, scale):
    return pl.pallas_call(
        lambda *refs: finish_kernel(*refs, levels=levels, cols=cols, half=half, scale=scale),
        out_shape=jax.ShapeDtypeStruct((cols, levels, 128), F32),
        in_specs=[sspec(), vspec(), vspec()],
        out_specs=vspec(),
        compiler_params=params(12),
        name="finish",
    )(place, own, other)


def local(anomalies, taper, obs_row, obs_col, obs_level, obs_value):
    members, levels, cols, lat_rows = anomalies.shape
    bands = lax.axis_size("lat")
    blocks = lax.axis_size("lon")
    mem, lat, lon = lax.axis_index("mem"), lax.axis_index("lat"), lax.axis_index("lon")
    coefs = cols * blocks
    lat_total = lat_rows * bands
    padded = -(-cols // 32) * 32
    half = padded // 2
    ensemble = members * lax.axis_size("mem")
    place = jnp.stack([mem, lat, lon]).astype(jnp.int32)

    n_half = lat_total // 2
    taper_mine = lax.dynamic_slice_in_dim(taper[0], mem * n_half, n_half, axis=1).astype(BF)
    ring = [taper_mine]
    for u in range(1, RING):
        ring.append(shift_lat(taper_mine, u))
    innovation = spread(place, obs_row, obs_col, obs_level, obs_value, half, levels, cols)

    by_round = jnp.transpose(anomalies, (0, 2, 1, 3)).reshape(members // bands, bands, cols, levels, lat_rows)
    pair_out = relayout_pair(by_round, innovation, padded)
    pair = over_all(pair_out)
    last_out = relayout_last(by_round, padded)
    last = over_all(last_out)
    own = jnp.stack(ring)
    weights = arrange(place, own, swap(own))
    other = swap(pair[:, 2 * padded :, :])

    tables = bases(cols, blocks, padded, lat_total)
    dims = (cols, blocks, bands, padded, coefs, lat_total)
    summed = member(place, pair, pair, other, weights, tables, None, False, dims)
    mine, theirs = member(place, last, pair, other, weights, tables, summed, True, dims)
    merged = (mine + swap(theirs).astype(F32)).astype(BF)
    pieces = over_all(merged)
    out = finish(place, pieces, swap(pieces), levels, cols, half, 1.0 / (ensemble - 1))
    return jnp.transpose(out, (1, 0, 2))


def solution(mesh):
    in_specs = (
        P("mem", None, "lon", "lat"),
        P("lon", "lat", None),
        P("lat", "lon"),
        P("lat", "lon"),
        P("lat", "lon"),
        P("lat", "lon"),
    )
    out_specs = P(None, "lon", "lat")

    return jax.shard_map(local, mesh=mesh, in_specs=in_specs, out_specs=out_specs, check_vma=False)
```

```python
import math

import jax
import jax.numpy as jnp
from jax import lax
from jax.experimental import pallas as pl
from jax.experimental.pallas import tpu as pltpu
from jax.sharding import PartitionSpec as P


BF = jnp.bfloat16
F32 = jnp.float32
LL = ("lat", "lon")
SWAP = [(0, 1), (1, 0)]
RING = 4


def vspec():
    return pl.BlockSpec(memory_space=pltpu.VMEM)


def sspec():
    return pl.BlockSpec(memory_space=pltpu.SMEM)


def params(mib, **more):
    return pltpu.CompilerParams(vmem_limit_bytes=mib * 1024 * 1024, **more)


def cost(flops):
    return pl.CostEstimate(flops=int(flops), bytes_accessed=1 << 20, transcendentals=0)


def over_all(x):
    return lax.all_to_all(x, LL, split_axis=0, concat_axis=0, tiled=True)


def shift_lat(x, s):
    return lax.ppermute(x, "lat", [(i, (i + s) % RING) for i in range(RING)])


def swap(x):
    return lax.ppermute(x, "mem", SWAP)


def turn_block(blocks, turn, levels):
    have = blocks[0].shape[0]
    both = jnp.concatenate([block.reshape(have * levels, 128) for block in blocks], axis=1)
    if have < 16:
        both = jnp.concatenate([both, jnp.zeros(((16 - have) * levels, 256), BF)], axis=0)
    return jnp.dot(turn, both, preferred_element_type=F32).astype(BF)


def turner(levels):
    size = 16 * levels
    to = lax.broadcasted_iota(jnp.int32, (size, size), 0)
    frm = lax.broadcasted_iota(jnp.int32, (size, size), 1)
    return jnp.where(frm == (to & 15) * levels + (to >> 4), 1.0, 0.0).astype(BF)


def head_kernel(place, fields, row_hbm, col_hbm, level_hbm, value_hbm, out, *scratch, half, levels, cols, padded):
    row_ref, col_ref, level_ref, value_ref, fields_in, staged, innov, acc, sems = scratch
    bands = fields.shape[1]
    count = iter(range(32))

    def fetch(source, target):
        copy = pltpu.make_async_copy(source, target, sems.at[next(count)])
        copy.start()
        return copy

    observed = [
        fetch(row_hbm, row_ref),
        fetch(col_hbm, col_ref),
        fetch(level_hbm, level_ref),
        fetch(value_hbm, value_ref),
    ]
    arriving = [fetch(fields.at[pl.ds(0, 2), g], fields_in.at[:, g]) for g in range(bands)]
    mem, lat, lon = place[0], place[1], place[2]
    slots = levels * half
    col_start = lon * cols + mem * half
    acc[...] = jnp.zeros_like(acc)
    slot_ids = lax.broadcasted_iota(jnp.int32, (slots, 128), 0)
    row_ids = lax.broadcasted_iota(jnp.int32, (128, 128), 0)
    for copy in observed:
        copy.wait()

    def add_group(g, carry):
        rows = pl.ds(pl.multiple_of(g * 8, 8), 8)
        within = col_ref[rows, :] - col_start
        inside = (within >= 0) & (within < half)
        keys = jnp.where(inside, level_ref[rows, :] * half + within, -1)
        lat_row = row_ref[rows, :] - lat * 128
        value = value_ref[rows, :]
        high = value.astype(BF).astype(F32)
        middle = value - high
        left = []
        right = []
        for r in range(8):
            hit = slot_ids == keys[r : r + 1, :]
            left.append(jnp.where(hit, 1.0, 0.0).astype(BF))
            row_hit = row_ids == lat_row[r : r + 1, :]
            top = jnp.where(row_hit, high[r : r + 1, :], 0.0)
            low = jnp.where(row_hit, middle[r : r + 1, :], 0.0)
            right.append(jnp.concatenate([top, low], axis=0).astype(BF))
        acc[...] += lax.dot_general(
            jnp.concatenate(left, axis=1),
            jnp.concatenate(right, axis=1),
            (((1,), (1,)), ((), ())),
            preferred_element_type=F32,
        )
        return carry

    lax.fori_loop(0, row_ref.shape[0] // 8, add_group, 0)
    innov[...] = (acc[:, :128] + acc[:, 128:]).astype(BF).reshape(levels, half, 128)
    leaving = [
        fetch(innov, out.at[pl.ds(g * levels, levels), pl.ds(2 * padded, half), :]) for g in range(bands)
    ]
    turn = turner(levels)
    for g in range(bands):
        arriving[g].wait()
        for start in range(0, padded, 16):
            have = min(16, cols - start)
            turned = turn_block([fields_in[p, g, start : start + have] for p in range(2)], turn, levels)
            for l in range(levels):
                for p in range(2):
                    piece = turned[16 * l : 16 * l + 16, 128 * p : 128 * p + 128]
                    staged[g * levels + l, p * padded + start : p * padded + start + 16, :] = piece
        leaving.append(
            fetch(
                staged.at[pl.ds(g * levels, levels)],
                out.at[pl.ds(g * levels, levels), pl.ds(0, 2 * padded), :],
            )
        )
    for copy in leaving:
        copy.wait()


def head(place, fields, obs_row, obs_col, obs_level, obs_value, half, padded):
    _, bands, cols, levels, lanes = fields.shape
    rows = 2 * padded + half
    hbm = pl.BlockSpec(memory_space=pltpu.HBM)
    observed = (obs_row, obs_col, obs_level, obs_value)
    return pl.pallas_call(
        lambda *refs: head_kernel(*refs, half=half, levels=levels, cols=cols, padded=padded),
        out_shape=jax.ShapeDtypeStruct((bands * levels, rows, lanes), BF),
        in_specs=[sspec()] + [hbm] * 5,
        out_specs=hbm,
        scratch_shapes=[pltpu.VMEM(array.shape, array.dtype) for array in observed]
        + [
            pltpu.VMEM((2, bands, cols, levels, lanes), BF),
            pltpu.VMEM((bands * levels, 2 * padded, lanes), BF),
            pltpu.VMEM((levels, half, lanes), BF),
            pltpu.VMEM((levels * half, 2 * lanes), F32),
            pltpu.SemaphoreType.DMA((32,)),
        ],
        compiler_params=params(61),
        cost_estimate=cost(6e9),
        name="head",
    )(place, fields, *observed)


def relayout_last_kernel(in_ref, out_ref, *, cols, levels, padded):
    turn = turner(levels)
    for start in range(0, padded, 16):
        have = min(16, cols - start)
        turned = turn_block([in_ref[0, p, start : start + have] for p in range(2)], turn, levels)
        for l in range(levels):
            for p in range(2):
                piece = turned[16 * l : 16 * l + 16, 128 * p : 128 * p + 128]
                out_ref[p * levels + l, start : start + 16, :] = piece


def relayout_last(fields, padded):
    rounds, bands, cols, levels, lanes = fields.shape
    return pl.pallas_call(
        lambda i, o: relayout_last_kernel(i, o, cols=cols, levels=levels, padded=padded),
        grid=(bands // 2,),
        in_specs=[pl.BlockSpec((1, 2, cols, levels, lanes), lambda g: (rounds - 1, g, 0, 0, 0))],
        out_specs=pl.BlockSpec((2 * levels, padded, lanes), lambda g: (g, 0, 0)),
        out_shape=jax.ShapeDtypeStruct((bands * levels, padded, lanes), BF),
        compiler_params=params(58),
        name="relayout_last",
    )(fields)


def turn_cos(turns):
    near = 0.25 - jnp.abs(turns - jnp.floor(turns + 0.5))
    square = near * near
    value = jnp.full_like(square, -15.094642576822990)
    for factor in (42.058693944897653, -76.705859753061386, 81.605249276075055, -41.341702240399755):
        value = value * square + factor
    return near * (value * square + 6.283185307179586)


def basis_kernel(lon_ref, lon_t_ref, lat_ref, lat_t_ref, *, cols, blocks, padded):
    total = cols * blocks
    half = total // 2
    tiles = lon_ref.shape[1] // 128
    lanes = lax.broadcasted_iota(jnp.int32, (padded, 128), 1)

    def turns_of(product):
        whole = (product.astype(F32) * (1.0 / total)).astype(jnp.int32)
        return (product - whole * total).astype(F32) * (1.0 / total)

    def lon_rows(j, carry):
        within = lax.broadcasted_iota(jnp.int32, (padded, 128), 0)
        x = within + cols * j
        fine = turns_of(x * lanes)
        coarse = turns_of(x * (lanes * 128))
        fine_cos = turn_cos(fine)
        fine_sin = turn_cos(fine - 0.25)
        scale = jnp.where(within < cols, math.sqrt(2.0 / total), 0.0)
        coarse_cos = turn_cos(coarse) * scale
        coarse_sin = turn_cos(coarse - 0.25) * scale
        sign = jnp.where((x & 1) == 0, 1.0, -1.0)
        rows = pl.ds(pl.multiple_of(j * padded, padded), padded)
        for t in range(tiles):
            c = lanes + 128 * t
            cos_t = coarse_cos[:, t : t + 1]
            sin_t = coarse_sin[:, t : t + 1]
            parts = []
            if 128 * t <= half:
                parts.append(fine_cos * cos_t - fine_sin * sin_t)
            if 128 * t + 127 > half:
                parts.append((fine_sin * cos_t + fine_cos * sin_t) * sign)
            value = parts[0] if len(parts) == 1 else jnp.where(c <= half, parts[0], parts[1])
            if t == 0 or 128 * t <= half < 128 * t + 128:
                value = jnp.where((c == 0) | (c == half), value * math.sqrt(0.5), value)
            if 128 * t + 127 >= total:
                value = jnp.where(c < total, value, 0.0)
            lon_ref[rows, 128 * t : 128 * t + 128] = value.astype(BF)
        return carry

    lax.fori_loop(0, blocks, lon_rows, 0)
    for t in range(tiles):
        strip = lon_ref[:, 128 * t : 128 * t + 128].astype(F32)
        lon_t_ref[128 * t : 128 * t + 128, :] = strip.T.astype(BF)

    length = lat_ref.shape[0]
    step = 64

    def lat_rows(i, carry):
        shape = (step, length)
        down = lax.broadcasted_iota(jnp.int32, shape, 0) + step * i
        across = lax.broadcasted_iota(jnp.int32, shape, 1)
        rows = pl.ds(pl.multiple_of(i * step, step), step)
        for grid, mode, ref in ((down, across, lat_ref), (across, down, lat_t_ref)):
            phase = (mode * (2 * grid + 1)) & (4 * length - 1)
            scale = jnp.where(mode == 0, 1.0 / math.sqrt(length), math.sqrt(2.0 / length))
            ref[rows, :] = (turn_cos(phase.astype(F32) * (0.25 / length)) * scale).astype(BF)
        return carry

    lax.fori_loop(0, length // step, lat_rows, 0)


def bases(cols, blocks, padded, lat_total):
    wide = padded * blocks
    return pl.pallas_call(
        lambda *refs: basis_kernel(*refs, cols=cols, blocks=blocks, padded=padded),
        out_shape=(
            jax.ShapeDtypeStruct((wide, wide), BF),
            jax.ShapeDtypeStruct((wide, wide), BF),
            jax.ShapeDtypeStruct((lat_total, lat_total), BF),
            jax.ShapeDtypeStruct((lat_total, lat_total), BF),
        ),
        out_specs=(vspec(),) * 4,
        compiler_params=params(58),
        cost_estimate=cost(12e9),
        name="bases",
    )()


def arrange_kernel(place, own, other, taper, *, rows_each):
    mem, lat = place[0], place[1]
    for ref, side in ((own, mem), (other, 1 - mem)):
        for u in range(RING):
            into = pl.ds(pl.multiple_of(lax.rem(lat + RING - u, RING) * rows_each, 8), rows_each)
            for q in range(2):
                taper[2 * side + q, into, :] = ref[u, :, 128 * q : 128 * q + 128]


def arrange(place, own, other):
    rows_each = own.shape[1]
    return pl.pallas_call(
        lambda *refs: arrange_kernel(*refs, rows_each=rows_each),
        out_shape=jax.ShapeDtypeStruct((4, RING * rows_each, 128), BF),
        in_specs=[sspec(), vspec(), vspec()],
        out_specs=vspec(),
        compiler_params=params(12),
        cost_estimate=cost(1e9),
        name="arrange",
    )(place, own, other)


def member_kernel(*refs, first, final, count, blocks, bands, padded, coefs):
    place, field_hbm, pair_hbm, other_hbm, taper_hbm, lon_hbm, lon_t_hbm, lat_hbm, lat_t_hbm = refs[:9]
    rest = list(refs[9:])
    so_far_hbm = None if first else rest.pop(0)
    outs = [rest.pop(0) for _ in range(2 if final else 1)]
    weighted, inverse, field, innov, taper, lon_ref, lon_t_ref, lat_ref, lat_t_ref, acc, sems = rest[:11]
    stages = rest[11:] if final else [acc]
    wide = padded * blocks
    parts = 3
    step = coefs // parts
    group = 4
    turns = blocks // group
    tall = group * padded
    half = padded // 2
    mem = place[0]
    own_rows = pl.ds(pl.multiple_of(mem * half, half), half)
    other_rows = pl.ds(pl.multiple_of((1 - mem) * half, half), half)

    def move(source, target, spot):
        return pltpu.make_async_copy(source, target, sems.at[spot])

    def lon_t_copy(r):
        rows = pl.ds(pl.multiple_of(r * step, 16), step)
        return move(lon_t_hbm.at[rows], lon_t_ref.at[rows], 10 + r)

    def lon_copy(b):
        rows = pl.ds(pl.multiple_of(b * tall, tall), tall)
        return move(lon_hbm.at[rows], lon_ref.at[rows], 14 + b)

    def so_far_copy(b):
        return move(so_far_hbm.at[:, pl.ds(b * group, group)], acc.at[:, pl.ds(b * group, group)], 18 + b)

    def out_copy(b, n):
        spots = pl.ds(b * group, group)
        return move(stages[n].at[:, spots], outs[n].at[:, spots], 22 + 4 * n + b)

    innov_copies = [
        move(pair_hbm.at[:, :, pl.ds(2 * padded, half), :], innov.at[:, :, own_rows, :], 0),
        move(other_hbm, innov.at[:, :, other_rows, :], 1),
    ]
    field_copies = [
        move(field_hbm.at[a, :, pl.ds(0, count * padded), :], field.at[a], 2 + a) for a in range(bands)
    ]
    table_copies = [
        lon_t_copy(0),
        move(lat_hbm, lat_ref, 7),
        move(taper_hbm, taper, 8),
        move(lat_t_hbm, lat_t_ref, 9),
    ]
    for copy in innov_copies + field_copies + table_copies:
        copy.start()
    inverse[coefs:, :] = jnp.zeros((wide - coefs, inverse.shape[1]), BF)
    for copy in innov_copies:
        copy.wait()

    def weigh(i, a):
        def body(j, carry):
            rows = pl.ds(pl.multiple_of(j * padded, padded), padded)
            product = field[a, j, i * padded : (i + 1) * padded, :] * innov[a, j]
            weighted[rows, 128 * a : 128 * a + 128] = product
            return carry

        lax.fori_loop(0, blocks, body, 0)

    def spectral(fresh):
        def body(r, carry):
            rows = pl.ds(pl.multiple_of(r * step, 16), step)
            if fresh:

                @pl.when(r > 0)
                def _():
                    lon_t_copy(r).wait()

            zonal = jnp.dot(lon_t_ref[rows, :], weighted[...], preferred_element_type=F32).astype(BF)
            spectrum = jnp.dot(zonal, lat_ref[...], preferred_element_type=F32)
            weights = jnp.concatenate([taper[q, rows, :] for q in range(4)], axis=1).astype(F32)
            tapered = (spectrum * weights).astype(BF)
            inverse[rows, :] = jnp.dot(tapered, lat_t_ref[...], preferred_element_type=F32).astype(BF)
            if fresh:

                @pl.when(r == 0)
                def _():
                    for b in range(turns):
                        lon_copy(b).start()
                        if not first:
                            so_far_copy(b).start()

            return carry

        lax.fori_loop(0, parts, body, 0)

    def gridded(i):
        def body(b, carry):
            rows = pl.ds(pl.multiple_of(b * tall, tall), tall)
            if i == 0:
                lon_copy(b).wait()
                if not first:
                    so_far_copy(b).wait()
            localized = jnp.dot(lon_ref[rows, :], inverse[...], preferred_element_type=F32)
            for g in range(group):
                for a in range(bands):
                    j = b * group + g
                    piece = localized[g * padded : (g + 1) * padded, 128 * a : 128 * a + 128]
                    piece = piece * field[a, j, i * padded : (i + 1) * padded, :].astype(F32)
                    piece = piece if first and i == 0 else piece + acc[a, j]
                    if final:
                        top, low = piece[:half], piece[half:]
                        stages[0][a, j] = jnp.where(mem == 0, top, low).astype(BF)
                        stages[1][a, j] = jnp.where(mem == 0, low, top).astype(BF)
                    else:
                        acc[a, j] = piece
            if i == count - 1:
                for n in range(len(outs)):
                    out_copy(b, n).start()
            return carry

        lax.fori_loop(0, turns, body, 0)

    for i in range(count):
        for a in range(bands):
            if i == 0:
                field_copies[a].wait()
            weigh(i, a)
        if i == 0:
            for r in range(1, parts):
                lon_t_copy(r).start()
            for copy in table_copies:
                copy.wait()
        spectral(i == 0)
        gridded(i)
    for b in range(turns):
        for n in range(len(outs)):
            out_copy(b, n).wait()


def member(place, field, pair, other, taper, tables, so_far, final, dims):
    _, blocks, bands, padded, coefs, lat_total = dims
    half = padded // 2
    wide = padded * blocks
    first = so_far is None
    count = 1 if final else 2
    split = lambda array: array.reshape(bands, blocks, *array.shape[1:])
    far = [split(field), split(pair), split(other), taper, *tables] + ([] if first else [so_far])
    block = lambda rows, dtype: ((bands, blocks, rows, 128), dtype)
    scratch = [((wide, lat_total), BF), ((wide, lat_total), BF), block(count * padded, BF), block(padded, BF)]
    scratch += [(array.shape, array.dtype) for array in (taper, *tables)]
    scratch.append(block(padded, F32))
    results = [block(half, BF), block(half, BF)] if final else [block(padded, F32)]
    hbm = pl.BlockSpec(memory_space=pltpu.HBM)
    return pl.pallas_call(
        lambda *refs: member_kernel(
            *refs, first=first, final=final, count=count, blocks=blocks, bands=bands, padded=padded, coefs=coefs
        ),
        out_shape=[jax.ShapeDtypeStruct(*each) for each in results],
        in_specs=[sspec()] + [hbm] * len(far),
        out_specs=[hbm] * len(results),
        scratch_shapes=[pltpu.VMEM(*each) for each in scratch]
        + [pltpu.SemaphoreType.DMA((32,))]
        + ([pltpu.VMEM(*each) for each in results] if final else []),
        compiler_params=params(60),
        cost_estimate=cost(count * 6e9),
        name="member_last" if final else "member_pair",
    )(place, *far)


def finish_kernel(place, own, other, out, *, levels, cols, half, scale):
    mem = place[0]
    bands = own.shape[0] // levels
    for side in range(2):
        rows = min(half, cols - side * half)
        for l in range(levels):
            mine = sum(own[a * levels + l].astype(F32) for a in range(bands))
            theirs = sum(other[a * levels + l].astype(F32) for a in range(bands))
            total = jnp.where(mem == side, mine, theirs) * scale
            out[side * half : side * half + rows, l, :] = total[:rows]


def finish(place, own, other, levels, cols, half, scale):
    return pl.pallas_call(
        lambda *refs: finish_kernel(*refs, levels=levels, cols=cols, half=half, scale=scale),
        out_shape=jax.ShapeDtypeStruct((cols, levels, 128), F32),
        in_specs=[sspec(), vspec(), vspec()],
        out_specs=vspec(),
        compiler_params=params(12),
        name="finish",
    )(place, own, other)


def local(anomalies, taper, obs_row, obs_col, obs_level, obs_value):
    members, levels, cols, lat_rows = anomalies.shape
    bands = lax.axis_size("lat")
    blocks = lax.axis_size("lon")
    mem, lat, lon = lax.axis_index("mem"), lax.axis_index("lat"), lax.axis_index("lon")
    coefs = cols * blocks
    lat_total = lat_rows * bands
    padded = -(-cols // 32) * 32
    half = padded // 2
    ensemble = members * lax.axis_size("mem")
    place = jnp.stack([mem, lat, lon]).astype(jnp.int32)

    by_round = jnp.transpose(anomalies, (0, 2, 1, 3)).reshape(members // bands, bands, cols, levels, lat_rows)
    pair_out = head(place, by_round, obs_row, obs_col, obs_level, obs_value, half, padded)
    pair = over_all(pair_out)
    n_half = lat_total // 2
    taper_mine = lax.dynamic_slice_in_dim(taper[0], mem * n_half, n_half, axis=1).astype(BF)
    ring = [taper_mine]
    for u in range(1, RING):
        ring.append(shift_lat(taper_mine, u))
    last_out = relayout_last(by_round, padded)
    last = over_all(last_out)
    own = jnp.stack(ring)
    weights = arrange(place, own, swap(own))
    other = swap(pair[:, 2 * padded :, :])

    tables = bases(cols, blocks, padded, lat_total)
    dims = (cols, blocks, bands, padded, coefs, lat_total)
    (summed,) = member(place, pair, pair, other, weights, tables, None, False, dims)
    mine, theirs = member(place, last, pair, other, weights, tables, summed, True, dims)
    merged = (mine.astype(F32) + swap(theirs).astype(F32)).astype(BF).reshape(bands * blocks, half, lat_rows)
    pieces = over_all(merged)
    out = finish(place, pieces, swap(pieces), levels, cols, half, 1.0 / (ensemble - 1))
    return jnp.transpose(out, (1, 0, 2))


def solution(mesh):
    in_specs = (
        P("mem", None, "lon", "lat"),
        P("lon", "lat", None),
        P("lat", "lon"),
        P("lat", "lon"),
        P("lat", "lon"),
        P("lat", "lon"),
    )
    out_specs = P(None, "lon", "lat")

    return jax.shard_map(local, mesh=mesh, in_specs=in_specs, out_specs=out_specs, check_vma=False)
```

```python
import math

import jax
import jax.numpy as jnp
from jax import lax
from jax.experimental import pallas as pl
from jax.experimental.pallas import tpu as pltpu
from jax.sharding import PartitionSpec as P


BF = jnp.bfloat16
F32 = jnp.float32
LL = ("lat", "lon")
SWAP = [(0, 1), (1, 0)]
RING = 4


def vspec():
    return pl.BlockSpec(memory_space=pltpu.VMEM)


def sspec():
    return pl.BlockSpec(memory_space=pltpu.SMEM)


def params(mib, **more):
    return pltpu.CompilerParams(vmem_limit_bytes=mib * 1024 * 1024, **more)


def cost(flops):
    return pl.CostEstimate(flops=int(flops), bytes_accessed=1 << 20, transcendentals=0)


def over_all(x):
    return lax.all_to_all(x, LL, split_axis=0, concat_axis=0, tiled=True)


def shift_lat(x, s):
    return lax.ppermute(x, "lat", [(i, (i + s) % RING) for i in range(RING)])


def swap(x):
    return lax.ppermute(x, "mem", SWAP)


LEAD = 6


def turn_block(blocks, turn, levels):
    both = jnp.concatenate([block.reshape(16 * levels, 128) for block in blocks], axis=1)
    return jnp.dot(turn, both, preferred_element_type=F32).astype(BF)


def turner(levels, mirrored, have):
    size = 16 * levels
    to = lax.broadcasted_iota(jnp.int32, (size, size), 0)
    frm = lax.broadcasted_iota(jnp.int32, (size, size), 1)
    within = to & 15
    taken = jnp.where(mirrored, 15 - within, within)
    return jnp.where((frm == taken * levels + (to >> 4)) & (within < have), 1.0, 0.0).astype(BF)


def turn_start(start, mirrored, cols):
    return jnp.where(mirrored, LEAD + cols - 15 - start, LEAD + start)


def head_kernel(place, fields, row_hbm, col_hbm, level_hbm, value_hbm, out, *scratch, half, levels, cols, padded):
    row_ref, col_ref, level_ref, value_ref, fields_in, staged, innov, acc, sems = scratch
    bands = fields.shape[1]
    count = iter(range(32))

    def fetch(source, target):
        copy = pltpu.make_async_copy(source, target, sems.at[next(count)])
        copy.start()
        return copy

    observed = [
        fetch(row_hbm, row_ref),
        fetch(col_hbm, col_ref),
        fetch(level_hbm, level_ref),
        fetch(value_hbm, value_ref),
    ]
    arriving = [
        (
            fetch(fields.at[pl.ds(0, 2), g], fields_in.at[:, g, pl.ds(LEAD, cols)]),
            fetch(fields.at[pl.ds(0, 2), g, pl.ds(0, 1)], fields_in.at[:, g, pl.ds(LEAD + cols, 1)]),
        )
        for g in range(bands)
    ]
    mem, lat, lon = place[0], place[1], place[2]
    mirrored = lon >= place[3]
    for p in range(2):
        for g in range(bands):
            fields_in[p, g, :LEAD] = jnp.zeros((LEAD, levels, 128), BF)
            fields_in[p, g, LEAD + cols + 1 :] = jnp.zeros((LEAD - 1, levels, 128), BF)
    slots = levels * half
    acc[...] = jnp.zeros_like(acc)
    slot_ids = lax.broadcasted_iota(jnp.int32, (slots, 128), 0)
    row_ids = lax.broadcasted_iota(jnp.int32, (128, 128), 0)
    for copy in observed:
        copy.wait()

    def add_group(g, carry):
        rows = pl.ds(pl.multiple_of(g * 8, 8), 8)
        column = col_ref[rows, :] - lon * cols
        within = jnp.where(mirrored & (column > 0), cols - column, column) - mem * half
        inside = (within >= 0) & (within < half)
        keys = jnp.where(inside, level_ref[rows, :] * half + within, -1)
        lat_row = row_ref[rows, :] - lat * 128
        value = value_ref[rows, :]
        high = value.astype(BF).astype(F32)
        middle = value - high
        left = []
        right = []
        for r in range(8):
            hit = slot_ids == keys[r : r + 1, :]
            left.append(jnp.where(hit, 1.0, 0.0).astype(BF))
            row_hit = row_ids == lat_row[r : r + 1, :]
            top = jnp.where(row_hit, high[r : r + 1, :], 0.0)
            low = jnp.where(row_hit, middle[r : r + 1, :], 0.0)
            right.append(jnp.concatenate([top, low], axis=0).astype(BF))
        acc[...] += lax.dot_general(
            jnp.concatenate(left, axis=1),
            jnp.concatenate(right, axis=1),
            (((1,), (1,)), ((), ())),
            preferred_element_type=F32,
        )
        return carry

    lax.fori_loop(0, row_ref.shape[0] // 8, add_group, 0)
    innov[...] = (acc[:, :128] + acc[:, 128:]).astype(BF).reshape(levels, half, 128)
    leaving = [
        fetch(innov, out.at[pl.ds(g * levels, levels), pl.ds(2 * padded, half), :]) for g in range(bands)
    ]
    turn = turner(levels, mirrored, 16)
    last_turn = turner(levels, mirrored, cols % 16)
    for g in range(bands):
        for copy in arriving[g]:
            copy.wait()
        for start in range(0, padded, 16):
            rows = pl.ds(turn_start(start, mirrored, cols), 16)
            matrix = turn if start + 16 <= cols else last_turn
            turned = turn_block([fields_in[p, g, rows] for p in range(2)], matrix, levels)
            for l in range(levels):
                for p in range(2):
                    piece = turned[16 * l : 16 * l + 16, 128 * p : 128 * p + 128]
                    staged[g * levels + l, p * padded + start : p * padded + start + 16, :] = piece
        leaving.append(
            fetch(
                staged.at[pl.ds(g * levels, levels)],
                out.at[pl.ds(g * levels, levels), pl.ds(0, 2 * padded), :],
            )
        )
    for copy in leaving:
        copy.wait()


def head(place, fields, obs_row, obs_col, obs_level, obs_value, half, padded):
    _, bands, cols, levels, lanes = fields.shape
    rows = 2 * padded + half
    hbm = pl.BlockSpec(memory_space=pltpu.HBM)
    observed = (obs_row, obs_col, obs_level, obs_value)
    return pl.pallas_call(
        lambda *refs: head_kernel(*refs, half=half, levels=levels, cols=cols, padded=padded),
        out_shape=jax.ShapeDtypeStruct((bands * levels, rows, lanes), BF),
        in_specs=[sspec()] + [hbm] * 5,
        out_specs=hbm,
        scratch_shapes=[pltpu.VMEM(array.shape, array.dtype) for array in observed]
        + [
            pltpu.VMEM((2, bands, cols + 2 * LEAD, levels, lanes), BF),
            pltpu.VMEM((bands * levels, 2 * padded, lanes), BF),
            pltpu.VMEM((levels, half, lanes), BF),
            pltpu.VMEM((levels * half, 2 * lanes), F32),
            pltpu.SemaphoreType.DMA((32,)),
        ],
        compiler_params=params(61),
        cost_estimate=cost(6e9),
        name="head",
    )(place, fields, *observed)


def relayout_last_kernel(place, in_ref, out_ref, room, *, cols, levels, padded):
    mirrored = place[2] >= place[3]
    for p in range(2):
        room[p, :LEAD] = jnp.zeros((LEAD, levels, 128), BF)
        room[p, LEAD : LEAD + cols] = in_ref[0, p]
        room[p, LEAD + cols] = in_ref[0, p, 0]
        room[p, LEAD + cols + 1 :] = jnp.zeros((LEAD - 1, levels, 128), BF)
    turn = turner(levels, mirrored, 16)
    last_turn = turner(levels, mirrored, cols % 16)
    for start in range(0, padded, 16):
        rows = pl.ds(turn_start(start, mirrored, cols), 16)
        matrix = turn if start + 16 <= cols else last_turn
        turned = turn_block([room[p, rows] for p in range(2)], matrix, levels)
        for l in range(levels):
            for p in range(2):
                piece = turned[16 * l : 16 * l + 16, 128 * p : 128 * p + 128]
                out_ref[p * levels + l, start : start + 16, :] = piece


def relayout_last(place, fields, padded):
    rounds, bands, cols, levels, lanes = fields.shape
    return pl.pallas_call(
        lambda *refs: relayout_last_kernel(*refs, cols=cols, levels=levels, padded=padded),
        grid=(bands // 2,),
        in_specs=[sspec(), pl.BlockSpec((1, 2, cols, levels, lanes), lambda g: (rounds - 1, g, 0, 0, 0))],
        out_specs=pl.BlockSpec((2 * levels, padded, lanes), lambda g: (g, 0, 0)),
        out_shape=jax.ShapeDtypeStruct((bands * levels, padded, lanes), BF),
        scratch_shapes=[pltpu.VMEM((2, cols + 2 * LEAD, levels, lanes), BF)],
        compiler_params=params(58),
        name="relayout_last",
    )(place, fields)


def turn_cos(turns):
    near = 0.25 - jnp.abs(turns - jnp.floor(turns + 0.5))
    square = near * near
    value = jnp.full_like(square, -15.094642576822990)
    for factor in (42.058693944897653, -76.705859753061386, 81.605249276075055, -41.341702240399755):
        value = value * square + factor
    return near * (value * square + 6.283185307179586)


def basis_kernel(lon_ref, lon_t_ref, lat_ref, lat_t_ref, *, cols, blocks, padded):
    total = cols * blocks
    nyquist = total // 2
    width = lon_ref.shape[1] // 2
    lanes = lax.broadcasted_iota(jnp.int32, (padded, 128), 1)

    def turns_of(product):
        whole = (product.astype(F32) * (1.0 / total)).astype(jnp.int32)
        return (product - whole * total).astype(F32) * (1.0 / total)

    def lon_rows(j, carry):
        within = lax.broadcasted_iota(jnp.int32, (padded, 128), 0)
        x = jnp.where(within < cols, within + cols * j, cols * (blocks - 1 - j))
        fine = turns_of(x * lanes)
        coarse = turns_of(x * (lanes * 128))
        fine_cos = turn_cos(fine)
        fine_sin = turn_cos(fine - 0.25)
        scale = jnp.where(within <= cols, math.sqrt(2.0 / total), 0.0)
        coarse_cos = turn_cos(coarse) * scale
        coarse_sin = turn_cos(coarse - 0.25) * scale
        rows = pl.ds(pl.multiple_of(j * padded, padded), padded)
        for t in range(width // 128):
            c = lanes + 128 * t
            cos_t = coarse_cos[:, t : t + 1]
            sin_t = coarse_sin[:, t : t + 1]
            even = fine_cos * cos_t - fine_sin * sin_t
            odd = fine_sin * cos_t + fine_cos * sin_t
            if t == 0 or 128 * t <= nyquist < 128 * t + 128:
                even = jnp.where((c == 0) | (c == nyquist), even * math.sqrt(0.5), even)
            if 128 * t + 127 >= nyquist:
                even = jnp.where(c <= nyquist, even, 0.0)
                odd = jnp.where(c < nyquist, odd, 0.0)
            lon_ref[rows, 128 * t : 128 * t + 128] = even.astype(BF)
            lon_ref[rows, width + 128 * t : width + 128 * t + 128] = odd.astype(BF)
        return carry

    lax.fori_loop(0, blocks // 2, lon_rows, 0)
    for t in range(lon_ref.shape[1] // 128):
        strip = lon_ref[:, 128 * t : 128 * t + 128].astype(F32)
        lon_t_ref[128 * t : 128 * t + 128, :] = strip.T.astype(BF)

    length = lat_ref.shape[0]
    step = 64

    def lat_rows(i, carry):
        shape = (step, length)
        down = lax.broadcasted_iota(jnp.int32, shape, 0) + step * i
        across = lax.broadcasted_iota(jnp.int32, shape, 1)
        rows = pl.ds(pl.multiple_of(i * step, step), step)
        for grid, mode, ref in ((down, across, lat_ref), (across, down, lat_t_ref)):
            phase = (mode * (2 * grid + 1)) & (4 * length - 1)
            scale = jnp.where(mode == 0, 1.0 / math.sqrt(length), math.sqrt(2.0 / length))
            ref[rows, :] = (turn_cos(phase.astype(F32) * (0.25 / length)) * scale).astype(BF)
        return carry

    lax.fori_loop(0, length // step, lat_rows, 0)


def bases(cols, blocks, padded, lat_total):
    tall = padded * blocks // 2
    return pl.pallas_call(
        lambda *refs: basis_kernel(*refs, cols=cols, blocks=blocks, padded=padded),
        out_shape=(
            jax.ShapeDtypeStruct((tall, 2 * tall), BF),
            jax.ShapeDtypeStruct((2 * tall, tall), BF),
            jax.ShapeDtypeStruct((lat_total, lat_total), BF),
            jax.ShapeDtypeStruct((lat_total, lat_total), BF),
        ),
        out_specs=(vspec(),) * 4,
        compiler_params=params(58),
        cost_estimate=cost(12e9),
        name="bases",
    )()


def arrange_kernel(place, own, other, taper, *, rows_each):
    mem, lat = place[0], place[1]
    spare = taper.shape[1] - RING * rows_each
    taper[:, RING * rows_each :, :] = jnp.zeros((4, spare, 128), BF)
    for ref, side in ((own, mem), (other, 1 - mem)):
        for u in range(RING):
            into = pl.ds(pl.multiple_of(lax.rem(lat + RING - u, RING) * rows_each, 8), rows_each)
            for q in range(2):
                taper[2 * side + q, into, :] = ref[u, :, 128 * q : 128 * q + 128]


def arrange(place, own, other):
    rows_each = own.shape[1]
    return pl.pallas_call(
        lambda *refs: arrange_kernel(*refs, rows_each=rows_each),
        out_shape=jax.ShapeDtypeStruct((4, RING * rows_each + 32, 128), BF),
        in_specs=[sspec(), vspec(), vspec()],
        out_specs=vspec(),
        compiler_params=params(12),
        cost_estimate=cost(1e9),
        name="arrange",
    )(place, own, other)


def member_kernel(*refs, first, final, count, blocks, bands, padded, coefs):
    place, field_hbm, pair_hbm, other_hbm, taper_hbm, lon_hbm, lon_t_hbm, lat_hbm, lat_t_hbm = refs[:9]
    rest = list(refs[9:])
    so_far_hbm = None if first else rest.pop(0)
    outs = [rest.pop(0) for _ in range(2 if final else 1)]
    folded, inverse, field, innov, taper, lon_ref, lon_t_ref, lat_ref, lat_t_ref, acc, sems = rest[:11]
    stages = rest[11:] if final else [acc]
    pairs = blocks // 2
    tall = padded * pairs
    nyquist = coefs // 2
    parts = 4
    step = (nyquist // 2 + 16) // 16 * 16
    group = 4
    turns = pairs // group
    half = padded // 2
    mem = place[0]
    own_rows = pl.ds(pl.multiple_of(mem * half, half), half)
    other_rows = pl.ds(pl.multiple_of((1 - mem) * half, half), half)

    def move(source, target, spot):
        return pltpu.make_async_copy(source, target, sems.at[spot])

    def lon_t_copy(r):
        rows = pl.ds(pl.multiple_of((r // 2) * tall + (r % 2) * step, 16), step)
        return move(lon_t_hbm.at[rows], lon_t_ref.at[rows], 10 + r)

    def lon_copy(b):
        rows = pl.ds(pl.multiple_of(b * group * padded, padded), group * padded)
        return move(lon_hbm.at[rows], lon_ref.at[rows], 14 + b)

    def spots(b, side):
        return pl.ds((blocks - group - b * group) if side else b * group, group)

    def so_far_copy(b, side):
        at = spots(b, side)
        return move(so_far_hbm.at[:, at], acc.at[:, at], 18 + 2 * b + side)

    def out_copy(b, side, n):
        at = spots(b, side)
        return move(stages[n].at[:, at], outs[n].at[:, at], 22 + 4 * n + 2 * b + side)

    innov_copies = [
        move(pair_hbm.at[:, :, pl.ds(2 * padded, half), :], innov.at[:, :, own_rows, :], 0),
        move(other_hbm, innov.at[:, :, other_rows, :], 1),
    ]
    field_copies = [
        move(field_hbm.at[a, :, pl.ds(0, count * padded), :], field.at[a], 2 + a) for a in range(bands)
    ]
    table_copies = [
        lon_t_copy(0),
        move(lat_hbm, lat_ref, 7),
        move(taper_hbm, taper, 8),
        move(lat_t_hbm, lat_t_ref, 9),
    ]
    for copy in innov_copies + field_copies + table_copies:
        copy.start()
    for side in range(2):
        inverse[side, 2 * step :, :] = jnp.zeros((tall - 2 * step, inverse.shape[2]), BF)
    for copy in innov_copies:
        copy.wait()
    down = lax.broadcasted_iota(jnp.int32, (padded, 128), 0)
    cols = coefs // blocks

    def weigh(i, a):
        def product(j):
            return field[a, j, i * padded : (i + 1) * padded, :].astype(F32) * innov[a, j].astype(F32)

        def body(j, carry):
            rows = pl.ds(pl.multiple_of(j * padded, padded), padded)
            near = product(j)
            far = product(blocks - 1 - j)
            near = jnp.where(down == cols, far[0:1, :], near)
            far = jnp.where(down == 0, 0.0, far)
            folded[0, rows, 128 * a : 128 * a + 128] = (near + far).astype(BF)
            folded[1, rows, 128 * a : 128 * a + 128] = (near - far).astype(BF)
            return carry

        lax.fori_loop(0, pairs, body, 0)

    def spectral(fresh):
        def body(r, carry):
            side = r // 2
            rows = pl.ds(pl.multiple_of((r % 2) * step, 16), step)
            table = pl.ds(pl.multiple_of(side * tall + (r % 2) * step, 16), step)
            weight_rows = pl.ds(pl.multiple_of(side * nyquist + (r % 2) * step, 16), step)
            if fresh:

                @pl.when(r > 0)
                def _():
                    lon_t_copy(r).wait()

            zonal = jnp.dot(lon_t_ref[table, :], folded[side], preferred_element_type=F32).astype(BF)
            spectrum = jnp.dot(zonal, lat_ref[...], preferred_element_type=F32)
            weights = jnp.concatenate([taper[q, weight_rows, :] for q in range(4)], axis=1).astype(F32)
            tapered = (spectrum * weights).astype(BF)
            back = jnp.dot(tapered, lat_t_ref[...], preferred_element_type=F32).astype(BF)
            inverse[side, rows, :] = back
            if fresh:

                @pl.when(r == 0)
                def _():
                    for b in range(turns):
                        lon_copy(b).start()
                        if not first:
                            so_far_copy(b, 0).start()
                            so_far_copy(b, 1).start()

            return carry

        lax.fori_loop(0, parts, body, 0)

    def gridded(i):
        def body(b, carry):
            rows = pl.ds(pl.multiple_of(b * group * padded, padded), group * padded)
            if i == 0:
                lon_copy(b).wait()
                if not first:
                    so_far_copy(b, 0).wait()
                    so_far_copy(b, 1).wait()
            even = jnp.dot(lon_ref[rows, :tall], inverse[0], preferred_element_type=F32)
            odd = jnp.dot(lon_ref[rows, tall:], inverse[1], preferred_element_type=F32)

            def put(piece, a, j):
                piece = piece * field[a, j, i * padded : (i + 1) * padded, :].astype(F32)
                piece = piece if first and i == 0 else piece + acc[a, j]
                if final:
                    top, low = piece[:half], piece[half:]
                    stages[0][a, j] = jnp.where(mem == 0, top, low).astype(BF)
                    stages[1][a, j] = jnp.where(mem == 0, low, top).astype(BF)
                else:
                    acc[a, j] = piece

            for g in range(group):
                for a in range(bands):
                    j = b * group + g
                    spot = (slice(g * padded, (g + 1) * padded), slice(128 * a, 128 * a + 128))
                    near = even[spot] + odd[spot]
                    far = jnp.where(down == 0, near[cols : cols + 1, :], even[spot] - odd[spot])
                    put(near, a, j)
                    put(far, a, blocks - 1 - j)
            if i == count - 1:
                for n in range(len(outs)):
                    out_copy(b, 0, n).start()
                    out_copy(b, 1, n).start()
            return carry

        lax.fori_loop(0, turns, body, 0)

    for i in range(count):
        for a in range(bands):
            if i == 0:
                field_copies[a].wait()
            weigh(i, a)
        if i == 0:
            for r in range(1, parts):
                lon_t_copy(r).start()
            for copy in table_copies:
                copy.wait()
        spectral(i == 0)
        gridded(i)
    for b in range(turns):
        for n in range(len(outs)):
            out_copy(b, 0, n).wait()
            out_copy(b, 1, n).wait()


def member(place, field, pair, other, taper, tables, so_far, final, dims):
    _, blocks, bands, padded, coefs, lat_total = dims
    half = padded // 2
    tall = padded * blocks // 2
    first = so_far is None
    count = 1 if final else 2
    split = lambda array: array.reshape(bands, blocks, *array.shape[1:])
    far = [split(field), split(pair), split(other), taper, *tables] + ([] if first else [so_far])
    block = lambda rows, dtype: ((bands, blocks, rows, 128), dtype)
    scratch = [((2, tall, lat_total), BF), ((2, tall, lat_total), BF), block(count * padded, BF), block(padded, BF)]
    scratch += [(array.shape, array.dtype) for array in (taper, *tables)]
    scratch.append(block(padded, F32))
    results = [block(half, BF), block(half, BF)] if final else [block(padded, F32)]
    hbm = pl.BlockSpec(memory_space=pltpu.HBM)
    return pl.pallas_call(
        lambda *refs: member_kernel(
            *refs, first=first, final=final, count=count, blocks=blocks, bands=bands, padded=padded, coefs=coefs
        ),
        out_shape=[jax.ShapeDtypeStruct(*each) for each in results],
        in_specs=[sspec()] + [hbm] * len(far),
        out_specs=[hbm] * len(results),
        scratch_shapes=[pltpu.VMEM(*each) for each in scratch]
        + [pltpu.SemaphoreType.DMA((32,))]
        + ([pltpu.VMEM(*each) for each in results] if final else []),
        compiler_params=params(60),
        cost_estimate=cost(count * 6e9),
        name="member_last" if final else "member_pair",
    )(place, *far)


def finish_kernel(place, own, other, out, *, levels, cols, half, scale):
    mem = place[0]
    mirrored = place[2] >= place[3]
    bands = own.shape[0] // levels
    to = lax.broadcasted_iota(jnp.int32, (2 * half, half), 0)
    frm = lax.broadcasted_iota(jnp.int32, (2 * half, half), 1)
    taken = jnp.where(mirrored & (to > 0), cols - to, to)
    picks = [jnp.where(taken == frm + side * half, 1.0, 0.0).astype(BF) for side in (mem, 1 - mem)]
    picks = jnp.concatenate(picks * bands, axis=1)
    columns = []
    for l in range(levels):
        parts = [ref[a * levels + l] for a in range(bands) for ref in (own, other)]
        columns.append(jnp.concatenate(parts, axis=0))
    summed = jnp.dot(picks, jnp.concatenate(columns, axis=1), preferred_element_type=F32) * scale
    for l in range(levels):
        out[:, l, :] = summed[:cols, 128 * l : 128 * l + 128]


def finish(place, own, other, levels, cols, half, scale):
    return pl.pallas_call(
        lambda *refs: finish_kernel(*refs, levels=levels, cols=cols, half=half, scale=scale),
        out_shape=jax.ShapeDtypeStruct((cols, levels, 128), F32),
        in_specs=[sspec(), vspec(), vspec()],
        out_specs=vspec(),
        compiler_params=params(16),
        name="finish",
    )(place, own, other)


def local(anomalies, taper, obs_row, obs_col, obs_level, obs_value):
    members, levels, cols, lat_rows = anomalies.shape
    bands = lax.axis_size("lat")
    blocks = lax.axis_size("lon")
    mem, lat, lon = lax.axis_index("mem"), lax.axis_index("lat"), lax.axis_index("lon")
    coefs = cols * blocks
    lat_total = lat_rows * bands
    padded = -(-cols // 32) * 32
    half = padded // 2
    ensemble = members * lax.axis_size("mem")
    place = jnp.stack([mem, lat, lon, jnp.int32(blocks // 2)]).astype(jnp.int32)

    by_round = jnp.transpose(anomalies, (0, 2, 1, 3)).reshape(members // bands, bands, cols, levels, lat_rows)
    pair_out = head(place, by_round, obs_row, obs_col, obs_level, obs_value, half, padded)
    pair = over_all(pair_out)
    n_half = lat_total // 2
    taper_mine = lax.dynamic_slice_in_dim(taper[0], mem * n_half, n_half, axis=1).astype(BF)
    ring = [taper_mine]
    for u in range(1, RING):
        ring.append(shift_lat(taper_mine, u))
    last_out = relayout_last(place, by_round, padded)
    last = over_all(last_out)
    own = jnp.stack(ring)
    weights = arrange(place, own, swap(own))
    other = swap(pair[:, 2 * padded :, :])

    tables = bases(cols, blocks, padded, lat_total)
    dims = (cols, blocks, bands, padded, coefs, lat_total)
    (summed,) = member(place, pair, pair, other, weights, tables, None, False, dims)
    mine, theirs = member(place, last, pair, other, weights, tables, summed, True, dims)
    merged = (mine.astype(F32) + swap(theirs).astype(F32)).astype(BF).reshape(bands * blocks, half, lat_rows)
    pieces = over_all(merged)
    out = finish(place, pieces, swap(pieces), levels, cols, half, 1.0 / (ensemble - 1))
    return jnp.transpose(out, (1, 0, 2))


def solution(mesh):
    in_specs = (
        P("mem", None, "lon", "lat"),
        P("lon", "lat", None),
        P("lat", "lon"),
        P("lat", "lon"),
        P("lat", "lon"),
        P("lat", "lon"),
    )
    out_specs = P(None, "lon", "lat")

    return jax.shard_map(local, mesh=mesh, in_specs=in_specs, out_specs=out_specs, check_vma=False)
```

```python
import math

import jax
import jax.numpy as jnp
from jax import lax
from jax.experimental import pallas as pl
from jax.experimental.pallas import tpu as pltpu
from jax.sharding import PartitionSpec as P


BF = jnp.bfloat16
F32 = jnp.float32
LL = ("lat", "lon")
SWAP = [(0, 1), (1, 0)]
RING = 4


def vspec():
    return pl.BlockSpec(memory_space=pltpu.VMEM)


def sspec():
    return pl.BlockSpec(memory_space=pltpu.SMEM)


def params(mib, **more):
    return pltpu.CompilerParams(vmem_limit_bytes=mib * 1024 * 1024, **more)


def cost(flops):
    return pl.CostEstimate(flops=int(flops), bytes_accessed=1 << 20, transcendentals=0)


def over_all(x):
    return lax.all_to_all(x, LL, split_axis=0, concat_axis=0, tiled=True)


def shift_lat(x, s):
    return lax.ppermute(x, "lat", [(i, (i + s) % RING) for i in range(RING)])


def swap(x):
    return lax.ppermute(x, "mem", SWAP)


LEAD = 6


def turn_block(blocks, turn, levels):
    both = jnp.concatenate([block.reshape(16 * levels, 128) for block in blocks], axis=1)
    return jnp.dot(turn, both, preferred_element_type=F32).astype(BF)


def turner(levels, mirrored, have):
    size = 16 * levels
    to = lax.broadcasted_iota(jnp.int32, (size, size), 0)
    frm = lax.broadcasted_iota(jnp.int32, (size, size), 1)
    within = to & 15
    taken = jnp.where(mirrored, 15 - within, within)
    return jnp.where((frm == taken * levels + (to >> 4)) & (within < have), 1.0, 0.0).astype(BF)


def turn_start(start, mirrored, cols):
    return jnp.where(mirrored, LEAD + cols - 15 - start, LEAD + start)


def head_kernel(place, fields, row_hbm, col_hbm, level_hbm, value_hbm, out, *scratch, half, levels, cols, padded):
    row_ref, col_ref, level_ref, value_ref, fields_in, staged, innov, acc, sems = scratch
    bands = fields.shape[1]
    count = iter(range(32))

    def fetch(source, target):
        copy = pltpu.make_async_copy(source, target, sems.at[next(count)])
        copy.start()
        return copy

    observed = [
        fetch(row_hbm, row_ref),
        fetch(col_hbm, col_ref),
        fetch(level_hbm, level_ref),
        fetch(value_hbm, value_ref),
    ]
    arriving = [
        (
            fetch(fields.at[pl.ds(0, 2), g], fields_in.at[:, g, pl.ds(LEAD, cols)]),
            fetch(fields.at[pl.ds(0, 2), g, pl.ds(0, 1)], fields_in.at[:, g, pl.ds(LEAD + cols, 1)]),
        )
        for g in range(bands)
    ]
    mem, lat, lon = place[0], place[1], place[2]
    mirrored = lon >= place[3]
    for p in range(2):
        for g in range(bands):
            fields_in[p, g, :LEAD] = jnp.zeros((LEAD, levels, 128), BF)
            fields_in[p, g, LEAD + cols + 1 :] = jnp.zeros((LEAD - 1, levels, 128), BF)
    slots = levels * half
    acc[...] = jnp.zeros_like(acc)
    slot_ids = lax.broadcasted_iota(jnp.int32, (slots, 128), 0)
    row_ids = lax.broadcasted_iota(jnp.int32, (128, 128), 0)
    for copy in observed:
        copy.wait()

    def add_group(g, carry):
        rows = pl.ds(pl.multiple_of(g * 8, 8), 8)
        column = col_ref[rows, :] - lon * cols
        within = jnp.where(mirrored & (column > 0), cols - column, column) - mem * half
        inside = (within >= 0) & (within < half)
        keys = jnp.where(inside, level_ref[rows, :] * half + within, -1)
        lat_row = row_ref[rows, :] - lat * 128
        value = value_ref[rows, :]
        high = value.astype(BF).astype(F32)
        middle = value - high
        left = []
        right = []
        for r in range(8):
            hit = slot_ids == keys[r : r + 1, :]
            left.append(jnp.where(hit, 1.0, 0.0).astype(BF))
            row_hit = row_ids == lat_row[r : r + 1, :]
            top = jnp.where(row_hit, high[r : r + 1, :], 0.0)
            low = jnp.where(row_hit, middle[r : r + 1, :], 0.0)
            right.append(jnp.concatenate([top, low], axis=0).astype(BF))
        acc[...] += lax.dot_general(
            jnp.concatenate(left, axis=1),
            jnp.concatenate(right, axis=1),
            (((1,), (1,)), ((), ())),
            preferred_element_type=F32,
        )
        return carry

    lax.fori_loop(0, row_ref.shape[0] // 8, add_group, 0)
    innov[...] = (acc[:, :128] + acc[:, 128:]).astype(BF).reshape(levels, half, 128)
    leaving = [
        fetch(innov, out.at[pl.ds(g * levels, levels), pl.ds(2 * padded, half), :]) for g in range(bands)
    ]
    turn = turner(levels, mirrored, 16)
    last_turn = turner(levels, mirrored, cols % 16)
    for g in range(bands):
        for copy in arriving[g]:
            copy.wait()
        for start in range(0, padded, 16):
            rows = pl.ds(turn_start(start, mirrored, cols), 16)
            matrix = turn if start + 16 <= cols else last_turn
            turned = turn_block([fields_in[p, g, rows] for p in range(2)], matrix, levels)
            for l in range(levels):
                for p in range(2):
                    piece = turned[16 * l : 16 * l + 16, 128 * p : 128 * p + 128]
                    staged[g * levels + l, p * padded + start : p * padded + start + 16, :] = piece
        leaving.append(
            fetch(
                staged.at[pl.ds(g * levels, levels)],
                out.at[pl.ds(g * levels, levels), pl.ds(0, 2 * padded), :],
            )
        )
    for copy in leaving:
        copy.wait()


def head(place, fields, obs_row, obs_col, obs_level, obs_value, half, padded):
    _, bands, cols, levels, lanes = fields.shape
    rows = 2 * padded + half
    hbm = pl.BlockSpec(memory_space=pltpu.HBM)
    observed = (obs_row, obs_col, obs_level, obs_value)
    return pl.pallas_call(
        lambda *refs: head_kernel(*refs, half=half, levels=levels, cols=cols, padded=padded),
        out_shape=jax.ShapeDtypeStruct((bands * levels, rows, lanes), BF),
        in_specs=[sspec()] + [hbm] * 5,
        out_specs=hbm,
        scratch_shapes=[pltpu.VMEM(array.shape, array.dtype) for array in observed]
        + [
            pltpu.VMEM((2, bands, cols + 2 * LEAD, levels, lanes), BF),
            pltpu.VMEM((bands * levels, 2 * padded, lanes), BF),
            pltpu.VMEM((levels, half, lanes), BF),
            pltpu.VMEM((levels * half, 2 * lanes), F32),
            pltpu.SemaphoreType.DMA((32,)),
        ],
        compiler_params=params(61),
        cost_estimate=cost(6e9),
        name="head",
    )(place, fields, *observed)


def relayout_last_kernel(place, in_ref, out_ref, room, *, cols, levels, padded):
    mirrored = place[2] >= place[3]
    for p in range(2):
        room[p, :LEAD] = jnp.zeros((LEAD, levels, 128), BF)
        room[p, LEAD : LEAD + cols] = in_ref[0, p]
        room[p, LEAD + cols] = in_ref[0, p, 0]
        room[p, LEAD + cols + 1 :] = jnp.zeros((LEAD - 1, levels, 128), BF)
    turn = turner(levels, mirrored, 16)
    last_turn = turner(levels, mirrored, cols % 16)
    for start in range(0, padded, 16):
        rows = pl.ds(turn_start(start, mirrored, cols), 16)
        matrix = turn if start + 16 <= cols else last_turn
        turned = turn_block([room[p, rows] for p in range(2)], matrix, levels)
        for l in range(levels):
            for p in range(2):
                piece = turned[16 * l : 16 * l + 16, 128 * p : 128 * p + 128]
                out_ref[p * levels + l, start : start + 16, :] = piece


def relayout_last(place, fields, padded):
    rounds, bands, cols, levels, lanes = fields.shape
    return pl.pallas_call(
        lambda *refs: relayout_last_kernel(*refs, cols=cols, levels=levels, padded=padded),
        grid=(bands // 2,),
        in_specs=[sspec(), pl.BlockSpec((1, 2, cols, levels, lanes), lambda g: (rounds - 1, g, 0, 0, 0))],
        out_specs=pl.BlockSpec((2 * levels, padded, lanes), lambda g: (g, 0, 0)),
        out_shape=jax.ShapeDtypeStruct((bands * levels, padded, lanes), BF),
        scratch_shapes=[pltpu.VMEM((2, cols + 2 * LEAD, levels, lanes), BF)],
        compiler_params=params(58),
        name="relayout_last",
    )(place, fields)


def turn_cos(turns):
    near = 0.25 - jnp.abs(turns - jnp.floor(turns + 0.5))
    square = near * near
    value = jnp.full_like(square, -15.094642576822990)
    for factor in (42.058693944897653, -76.705859753061386, 81.605249276075055, -41.341702240399755):
        value = value * square + factor
    return near * (value * square + 6.283185307179586)


def basis_kernel(lon_ref, lon_t_ref, lat_ref, lat_t_ref, *, cols, blocks, padded):
    total = cols * blocks
    nyquist = total // 2
    width = lon_ref.shape[1] // 2
    lanes = lax.broadcasted_iota(jnp.int32, (padded, 128), 1)

    def turns_of(product):
        whole = (product.astype(F32) * (1.0 / total)).astype(jnp.int32)
        return (product - whole * total).astype(F32) * (1.0 / total)

    def lon_rows(j, carry):
        within = lax.broadcasted_iota(jnp.int32, (padded, 128), 0)
        x = jnp.where(within < cols, within + cols * j, cols * (blocks - 1 - j))
        fine = turns_of(x * lanes)
        coarse = turns_of(x * (lanes * 128))
        fine_cos = turn_cos(fine)
        fine_sin = turn_cos(fine - 0.25)
        scale = jnp.where(within <= cols, math.sqrt(2.0 / total), 0.0)
        coarse_cos = turn_cos(coarse) * scale
        coarse_sin = turn_cos(coarse - 0.25) * scale
        rows = pl.ds(pl.multiple_of(j * padded, padded), padded)
        for t in range(width // 128):
            c = lanes + 128 * t
            cos_t = coarse_cos[:, t : t + 1]
            sin_t = coarse_sin[:, t : t + 1]
            even = fine_cos * cos_t - fine_sin * sin_t
            odd = fine_sin * cos_t + fine_cos * sin_t
            if t == 0 or 128 * t <= nyquist < 128 * t + 128:
                even = jnp.where((c == 0) | (c == nyquist), even * math.sqrt(0.5), even)
            if 128 * t + 127 >= nyquist:
                even = jnp.where(c <= nyquist, even, 0.0)
                odd = jnp.where(c < nyquist, odd, 0.0)
            lon_ref[rows, 128 * t : 128 * t + 128] = even.astype(BF)
            lon_ref[rows, width + 128 * t : width + 128 * t + 128] = odd.astype(BF)
        return carry

    lax.fori_loop(0, blocks // 2, lon_rows, 0)
    for t in range(lon_ref.shape[1] // 128):
        strip = lon_ref[:, 128 * t : 128 * t + 128].astype(F32)
        lon_t_ref[128 * t : 128 * t + 128, :] = strip.T.astype(BF)

    length = lat_ref.shape[0]
    step = 64

    def lat_rows(i, carry):
        shape = (step, length)
        down = lax.broadcasted_iota(jnp.int32, shape, 0) + step * i
        across = lax.broadcasted_iota(jnp.int32, shape, 1)
        rows = pl.ds(pl.multiple_of(i * step, step), step)
        for grid, mode, ref in ((down, across, lat_ref), (across, down, lat_t_ref)):
            phase = (mode * (2 * grid + 1)) & (4 * length - 1)
            scale = jnp.where(mode == 0, 1.0 / math.sqrt(length), math.sqrt(2.0 / length))
            ref[rows, :] = (turn_cos(phase.astype(F32) * (0.25 / length)) * scale).astype(BF)
        return carry

    lax.fori_loop(0, length // step, lat_rows, 0)


def bases(cols, blocks, padded, lat_total):
    tall = padded * blocks // 2
    return pl.pallas_call(
        lambda *refs: basis_kernel(*refs, cols=cols, blocks=blocks, padded=padded),
        out_shape=(
            jax.ShapeDtypeStruct((tall, 2 * tall), BF),
            jax.ShapeDtypeStruct((2 * tall, tall), BF),
            jax.ShapeDtypeStruct((lat_total, lat_total), BF),
            jax.ShapeDtypeStruct((lat_total, lat_total), BF),
        ),
        out_specs=(vspec(),) * 4,
        compiler_params=params(58),
        cost_estimate=cost(12e9),
        name="bases",
    )()


def arrange_kernel(place, own, other, taper, *, rows_each):
    mem, lat = place[0], place[1]
    spare = taper.shape[1] - RING * rows_each
    taper[:, RING * rows_each :, :] = jnp.zeros((4, spare, 128), BF)
    for ref, side in ((own, mem), (other, 1 - mem)):
        for u in range(RING):
            into = pl.ds(pl.multiple_of(lax.rem(lat + RING - u, RING) * rows_each, 8), rows_each)
            for q in range(2):
                taper[2 * side + q, into, :] = ref[u, :, 128 * q : 128 * q + 128]


def arrange(place, own, other):
    rows_each = own.shape[1]
    return pl.pallas_call(
        lambda *refs: arrange_kernel(*refs, rows_each=rows_each),
        out_shape=jax.ShapeDtypeStruct((4, RING * rows_each + 32, 128), BF),
        in_specs=[sspec(), vspec(), vspec()],
        out_specs=vspec(),
        compiler_params=params(12),
        cost_estimate=cost(1e9),
        name="arrange",
    )(place, own, other)


def member_kernel(*refs, first, final, count, blocks, bands, padded, coefs):
    place, field_hbm, pair_hbm, other_hbm, taper_hbm, lon_hbm, lon_t_hbm, lat_hbm, lat_t_hbm = refs[:9]
    rest = list(refs[9:])
    so_far_hbm = None if first else rest.pop(0)
    outs = [rest.pop(0) for _ in range(2 if final else 1)]
    folded, inverse, field, innov, taper, lon_ref, lon_t_ref, lat_ref, lat_t_ref, acc, sems = rest[:11]
    stages = rest[11:]
    pairs = blocks // 2
    tall = padded * pairs
    nyquist = coefs // 2
    parts = 4
    step = (nyquist // 2 + 16) // 16 * 16
    group = 4
    turns = pairs // group
    half = padded // 2
    mem = place[0]
    own_rows = pl.ds(pl.multiple_of(mem * half, half), half)
    other_rows = pl.ds(pl.multiple_of((1 - mem) * half, half), half)

    def move(source, target, spot):
        return pltpu.make_async_copy(source, target, sems.at[spot])

    def lon_t_copy(r):
        rows = pl.ds(pl.multiple_of((r // 2) * tall + (r % 2) * step, 16), step)
        return move(lon_t_hbm.at[rows], lon_t_ref.at[rows], 10 + r)

    def lon_copy(b):
        rows = pl.ds(pl.multiple_of(b * group * padded, padded), group * padded)
        return move(lon_hbm.at[rows], lon_ref.at[rows], 14 + b)

    def spots(b, side):
        return pl.ds((blocks - group - b * group) if side else b * group, group)

    def so_far_copy(b, side):
        at = spots(b, side)
        return move(so_far_hbm.at[:, at], acc.at[:, at], 18 + 2 * b + side)

    def out_copy(b, side, n):
        at = spots(b, side)
        return move(stages[n].at[:, at], outs[n].at[:, at], 22 + 4 * n + 2 * b + side)

    innov_copies = [
        move(pair_hbm.at[:, :, pl.ds(2 * padded, half), :], innov.at[:, :, own_rows, :], 0),
        move(other_hbm, innov.at[:, :, other_rows, :], 1),
    ]
    field_copies = [
        move(field_hbm.at[a, :, pl.ds(0, count * padded), :], field.at[a], 2 + a) for a in range(bands)
    ]
    table_copies = [
        lon_t_copy(0),
        lon_t_copy(2),
        move(lat_hbm, lat_ref, 7),
        move(taper_hbm, taper, 8),
        move(lat_t_hbm, lat_t_ref, 9),
    ]
    for copy in innov_copies + field_copies + table_copies:
        copy.start()
    for side in range(2):
        inverse[side, 2 * step :, :] = jnp.zeros((tall - 2 * step, inverse.shape[2]), BF)
    for copy in innov_copies:
        copy.wait()
    down = lax.broadcasted_iota(jnp.int32, (padded, 128), 0)
    cols = coefs // blocks

    def weigh(i, a):
        def product(j):
            return field[a, j, i * padded : (i + 1) * padded, :].astype(F32) * innov[a, j].astype(F32)

        def body(j, carry):
            rows = pl.ds(pl.multiple_of(j * padded, padded), padded)
            near = product(j)
            far = product(blocks - 1 - j)
            near = jnp.where(down == cols, far[0:1, :], near)
            far = jnp.where(down == 0, 0.0, far)
            folded[0, rows, 128 * a : 128 * a + 128] = (near + far).astype(BF)
            folded[1, rows, 128 * a : 128 * a + 128] = (near - far).astype(BF)
            return carry

        lax.fori_loop(0, pairs, body, 0)

    def spectral(fresh):
        def body(r, carry):
            rows = pl.ds(pl.multiple_of(r * step, 16), step)
            if fresh:

                @pl.when(r > 0)
                def _():
                    for side in range(2):
                        lon_t_copy(2 * side + r).wait()

            tables = [pl.ds(pl.multiple_of(side * tall + r * step, 16), step) for side in range(2)]
            zonal = [
                jnp.dot(lon_t_ref[tables[side], :], folded[side], preferred_element_type=F32).astype(BF)
                for side in range(2)
            ]
            spectrum = [jnp.dot(zonal[side], lat_ref[...], preferred_element_type=F32) for side in range(2)]
            tapered = []
            for side in range(2):
                weight_rows = pl.ds(pl.multiple_of(side * nyquist + r * step, 16), step)
                weights = jnp.concatenate([taper[q, weight_rows, :] for q in range(4)], axis=1).astype(F32)
                tapered.append((spectrum[side] * weights).astype(BF))
            for side in range(2):
                back = jnp.dot(tapered[side], lat_t_ref[...], preferred_element_type=F32)
                inverse[side, rows, :] = back.astype(BF)
            if fresh:

                @pl.when(r == 0)
                def _():
                    for b in range(turns):
                        lon_copy(b).start()
                        if not first:
                            so_far_copy(b, 0).start()
                            so_far_copy(b, 1).start()

            return carry

        lax.fori_loop(0, parts // 2, body, 0)

    def gridded(i):
        def body(b, carry):
            rows = pl.ds(pl.multiple_of(b * group * padded, padded), group * padded)
            if i == 0:
                lon_copy(b).wait()
                if not first:
                    so_far_copy(b, 0).wait()
                    so_far_copy(b, 1).wait()
            even = jnp.dot(lon_ref[rows, :tall], inverse[0], preferred_element_type=F32)
            odd = jnp.dot(lon_ref[rows, tall:], inverse[1], preferred_element_type=F32)

            def put(piece, a, j):
                piece = piece * field[a, j, i * padded : (i + 1) * padded, :].astype(F32)
                piece = piece if first and i == 0 else piece + acc[a, j].astype(F32)
                if final:
                    top, low = piece[:half], piece[half:]
                    stages[0][a, j] = jnp.where(mem == 0, top, low).astype(BF)
                    stages[1][a, j] = jnp.where(mem == 0, low, top).astype(BF)
                elif i == count - 1:
                    stages[0][a, j] = piece.astype(BF)
                else:
                    acc[a, j] = piece

            for g in range(group):
                for a in range(bands):
                    j = b * group + g
                    spot = (slice(g * padded, (g + 1) * padded), slice(128 * a, 128 * a + 128))
                    near = even[spot] + odd[spot]
                    far = jnp.where(down == 0, near[cols : cols + 1, :], even[spot] - odd[spot])
                    put(near, a, j)
                    put(far, a, blocks - 1 - j)
            if i == count - 1:
                for n in range(len(outs)):
                    out_copy(b, 0, n).start()
                    out_copy(b, 1, n).start()
            return carry

        for b in range(turns):
            body(b, 0)

    for i in range(count):
        for a in range(bands):
            if i == 0:
                field_copies[a].wait()
            weigh(i, a)
        if i == 0:
            for r in (1, 3):
                lon_t_copy(r).start()
            for copy in table_copies:
                copy.wait()
        spectral(i == 0)
        gridded(i)
    for b in range(turns):
        for n in range(len(outs)):
            out_copy(b, 0, n).wait()
            out_copy(b, 1, n).wait()


def member(place, field, pair, other, taper, tables, so_far, final, dims):
    _, blocks, bands, padded, coefs, lat_total = dims
    half = padded // 2
    tall = padded * blocks // 2
    first = so_far is None
    count = 1 if final else 2
    split = lambda array: array.reshape(bands, blocks, *array.shape[1:])
    far = [split(field), split(pair), split(other), taper, *tables] + ([] if first else [so_far])
    block = lambda rows, dtype: ((bands, blocks, rows, 128), dtype)
    scratch = [((2, tall, lat_total), BF), ((2, tall, lat_total), BF), block(count * padded, BF), block(padded, BF)]
    scratch += [(array.shape, array.dtype) for array in (taper, *tables)]
    scratch.append(block(padded, F32 if first else BF))
    results = [block(half, BF), block(half, BF)] if final else [block(padded, BF)]
    hbm = pl.BlockSpec(memory_space=pltpu.HBM)
    return pl.pallas_call(
        lambda *refs: member_kernel(
            *refs, first=first, final=final, count=count, blocks=blocks, bands=bands, padded=padded, coefs=coefs
        ),
        out_shape=[jax.ShapeDtypeStruct(*each) for each in results],
        in_specs=[sspec()] + [hbm] * len(far),
        out_specs=[hbm] * len(results),
        scratch_shapes=[pltpu.VMEM(*each) for each in scratch]
        + [pltpu.SemaphoreType.DMA((32,))]
        + [pltpu.VMEM(*each) for each in results],
        compiler_params=params(60),
        cost_estimate=cost(count * 6e9),
        name="member_last" if final else "member_pair",
    )(place, *far)


def finish_kernel(place, own, other, out, *, levels, cols, half, scale):
    mem = place[0]
    mirrored = place[2] >= place[3]
    bands = own.shape[0] // levels
    to = lax.broadcasted_iota(jnp.int32, (2 * half, half), 0)
    frm = lax.broadcasted_iota(jnp.int32, (2 * half, half), 1)
    taken = jnp.where(mirrored & (to > 0), cols - to, to)
    picks = [jnp.where(taken == frm + side * half, 1.0, 0.0).astype(BF) for side in (mem, 1 - mem)]
    picks = jnp.concatenate(picks * bands, axis=1)
    columns = []
    for l in range(levels):
        parts = [ref[a * levels + l] for a in range(bands) for ref in (own, other)]
        columns.append(jnp.concatenate(parts, axis=0))
    summed = jnp.dot(picks, jnp.concatenate(columns, axis=1), preferred_element_type=F32) * scale
    for l in range(levels):
        out[:, l, :] = summed[:cols, 128 * l : 128 * l + 128]


def finish(place, own, other, levels, cols, half, scale):
    return pl.pallas_call(
        lambda *refs: finish_kernel(*refs, levels=levels, cols=cols, half=half, scale=scale),
        out_shape=jax.ShapeDtypeStruct((cols, levels, 128), F32),
        in_specs=[sspec(), vspec(), vspec()],
        out_specs=vspec(),
        compiler_params=params(16),
        name="finish",
    )(place, own, other)


def local(anomalies, taper, obs_row, obs_col, obs_level, obs_value):
    members, levels, cols, lat_rows = anomalies.shape
    bands = lax.axis_size("lat")
    blocks = lax.axis_size("lon")
    mem, lat, lon = lax.axis_index("mem"), lax.axis_index("lat"), lax.axis_index("lon")
    coefs = cols * blocks
    lat_total = lat_rows * bands
    padded = -(-cols // 32) * 32
    half = padded // 2
    ensemble = members * lax.axis_size("mem")
    place = jnp.stack([mem, lat, lon, jnp.int32(blocks // 2)]).astype(jnp.int32)

    by_round = jnp.transpose(anomalies, (0, 2, 1, 3)).reshape(members // bands, bands, cols, levels, lat_rows)
    pair_out = head(place, by_round, obs_row, obs_col, obs_level, obs_value, half, padded)
    pair = over_all(pair_out)
    n_half = lat_total // 2
    taper_mine = lax.dynamic_slice_in_dim(taper[0], mem * n_half, n_half, axis=1).astype(BF)
    ring = [taper_mine]
    for u in range(1, RING):
        ring.append(shift_lat(taper_mine, u))
    last_out = relayout_last(place, by_round, padded)
    last = over_all(last_out)
    own = jnp.stack(ring)
    weights = arrange(place, own, swap(own))
    other = swap(pair[:, 2 * padded :, :])

    tables = bases(cols, blocks, padded, lat_total)
    dims = (cols, blocks, bands, padded, coefs, lat_total)
    (summed,) = member(place, pair, pair, other, weights, tables, None, False, dims)
    mine, theirs = member(place, last, pair, other, weights, tables, summed, True, dims)
    merged = (mine.astype(F32) + swap(theirs).astype(F32)).astype(BF).reshape(bands * blocks, half, lat_rows)
    pieces = over_all(merged)
    out = finish(place, pieces, swap(pieces), levels, cols, half, 1.0 / (ensemble - 1))
    return jnp.transpose(out, (1, 0, 2))


def solution(mesh):
    in_specs = (
        P("mem", None, "lon", "lat"),
        P("lon", "lat", None),
        P("lat", "lon"),
        P("lat", "lon"),
        P("lat", "lon"),
        P("lat", "lon"),
    )
    out_specs = P(None, "lon", "lat")

    return jax.shard_map(local, mesh=mesh, in_specs=in_specs, out_specs=out_specs, check_vma=False)
```

```python
import math

import jax
import jax.numpy as jnp
from jax import lax
from jax.experimental import pallas as pl
from jax.experimental.pallas import tpu as pltpu
from jax.sharding import PartitionSpec as P


BF = jnp.bfloat16
F32 = jnp.float32
LL = ("lat", "lon")
SWAP = [(0, 1), (1, 0)]
RING = 4


def vspec():
    return pl.BlockSpec(memory_space=pltpu.VMEM)


def sspec():
    return pl.BlockSpec(memory_space=pltpu.SMEM)


def params(mib, **more):
    return pltpu.CompilerParams(vmem_limit_bytes=mib * 1024 * 1024, **more)


def cost(flops):
    return pl.CostEstimate(flops=int(flops), bytes_accessed=1 << 20, transcendentals=0)


def over_all(x):
    return lax.all_to_all(x, LL, split_axis=0, concat_axis=0, tiled=True)


def shift_lat(x, s):
    return lax.ppermute(x, "lat", [(i, (i + s) % RING) for i in range(RING)])


def swap(x):
    return lax.ppermute(x, "mem", SWAP)


LEAD = 6


def turn_block(blocks, turn, levels):
    both = jnp.concatenate([block.reshape(16 * levels, 128) for block in blocks], axis=1)
    return jnp.dot(turn, both, preferred_element_type=F32).astype(BF)


def turner(levels, mirrored, have):
    size = 16 * levels
    to = lax.broadcasted_iota(jnp.int32, (size, size), 0)
    frm = lax.broadcasted_iota(jnp.int32, (size, size), 1)
    within = to & 15
    taken = jnp.where(mirrored, 15 - within, within)
    return jnp.where((frm == taken * levels + (to >> 4)) & (within < have), 1.0, 0.0).astype(BF)


def turn_start(start, mirrored, cols):
    return jnp.where(mirrored, LEAD + cols - 15 - start, LEAD + start)


def head_kernel(place, fields, row_hbm, col_hbm, level_hbm, value_hbm, out, *scratch, half, levels, cols, padded):
    row_ref, col_ref, level_ref, value_ref, fields_in, staged, innov, acc, sems = scratch
    bands = fields.shape[1]
    count = iter(range(32))

    def fetch(source, target):
        copy = pltpu.make_async_copy(source, target, sems.at[next(count)])
        copy.start()
        return copy

    observed = [
        fetch(row_hbm, row_ref),
        fetch(col_hbm, col_ref),
        fetch(level_hbm, level_ref),
        fetch(value_hbm, value_ref),
    ]
    arriving = [
        (
            fetch(fields.at[pl.ds(0, 2), g], fields_in.at[:, g, pl.ds(LEAD, cols)]),
            fetch(fields.at[pl.ds(0, 2), g, pl.ds(0, 1)], fields_in.at[:, g, pl.ds(LEAD + cols, 1)]),
        )
        for g in range(bands)
    ]
    mem, lat, lon = place[0], place[1], place[2]
    mirrored = lon >= place[3]
    for p in range(2):
        for g in range(bands):
            fields_in[p, g, :LEAD] = jnp.zeros((LEAD, levels, 128), BF)
            fields_in[p, g, LEAD + cols + 1 :] = jnp.zeros((LEAD - 1, levels, 128), BF)
    slots = levels * half
    acc[...] = jnp.zeros_like(acc)

    def spots_of(count):
        major = lax.broadcasted_iota(jnp.int32, (count // 16, 16, 128), 0)
        minor = lax.broadcasted_iota(jnp.int32, (count // 16, 16, 128), 1)
        return (major * 16 + minor).astype(F32).astype(BF)

    def packed(row):
        return jnp.broadcast_to(row, (16, 128)).astype(BF)[None]

    slot_ids = spots_of(256)
    row_ids = spots_of(128)
    one = jnp.ones((), BF)
    zero = jnp.zeros((), BF)
    for copy in observed:
        copy.wait()

    def add_group(g, carry):
        rows = pl.ds(pl.multiple_of(g * 16, 8), 16)
        column = col_ref[rows, :] - lon * cols
        within = jnp.where(mirrored & (column > 0), cols - column, column) - mem * half
        inside = (within >= 0) & (within < half)
        keys = jnp.where(inside, level_ref[rows, :] * half + within, -1)
        lat_row = (row_ref[rows, :] - lat * 128).astype(F32)
        value = value_ref[rows, :]
        high = value.astype(BF).astype(F32)
        middle = value - high
        parts = []
        for start in range(0, slots, 256):
            part = keys - start
            parts.append(jnp.where((part >= 0) & (part < 256), part, -1).astype(F32))
        left = []
        right = []
        for r in range(16):
            at = slice(r, r + 1)
            hits = [jnp.where(slot_ids == packed(part[at]), one, zero).reshape(256, 128) for part in parts]
            left.append(jnp.concatenate(hits, axis=0))
            row_hit = row_ids == packed(lat_row[at])
            sides = [jnp.where(row_hit, packed(side[at]), zero).reshape(128, 128) for side in (high, middle)]
            right.append(jnp.concatenate(sides, axis=0))
        acc[...] += lax.dot_general(
            jnp.concatenate(left, axis=1),
            jnp.concatenate(right, axis=1),
            (((1,), (1,)), ((), ())),
            preferred_element_type=F32,
        )
        return carry

    leaving = []
    lax.fori_loop(0, 2, add_group, 0)
    turn = turner(levels, mirrored, 16)
    last_turn = turner(levels, mirrored, cols % 16)
    for first in range(0, bands, 2):
        group = range(first, first + 2)
        for g in group:
            for copy in arriving[g]:
                copy.wait()
        for start in range(0, padded, 16):
            rows = pl.ds(turn_start(start, mirrored, cols), 16)
            matrix = turn if start + 16 <= cols else last_turn
            turned = turn_block([fields_in[p, g, rows] for g in group for p in range(2)], matrix, levels)
            for l in range(levels):
                for n, g in enumerate(group):
                    for p in range(2):
                        lane = 256 * n + 128 * p
                        piece = turned[16 * l : 16 * l + 16, lane : lane + 128]
                        staged[g * levels + l, p * padded + start : p * padded + start + 16, :] = piece
        for g in group:
            leaving.append(
                fetch(
                    staged.at[pl.ds(g * levels, levels)],
                    out.at[pl.ds(g * levels, levels), pl.ds(0, 2 * padded), :],
                )
            )
    lax.fori_loop(2, row_ref.shape[0] // 16, add_group, 0)
    innov[...] = (acc[:, :128] + acc[:, 128:]).astype(BF).reshape(levels, half, 128)
    leaving += [
        fetch(innov, out.at[pl.ds(g * levels, levels), pl.ds(2 * padded, half), :]) for g in range(bands)
    ]
    for copy in leaving:
        copy.wait()


def head(place, fields, obs_row, obs_col, obs_level, obs_value, half, padded):
    _, bands, cols, levels, lanes = fields.shape
    rows = 2 * padded + half
    hbm = pl.BlockSpec(memory_space=pltpu.HBM)
    observed = (obs_row, obs_col, obs_level, obs_value)
    return pl.pallas_call(
        lambda *refs: head_kernel(*refs, half=half, levels=levels, cols=cols, padded=padded),
        out_shape=jax.ShapeDtypeStruct((bands * levels, rows, lanes), BF),
        in_specs=[sspec()] + [hbm] * 5,
        out_specs=hbm,
        scratch_shapes=[pltpu.VMEM(array.shape, array.dtype) for array in observed]
        + [
            pltpu.VMEM((2, bands, cols + 2 * LEAD, levels, lanes), BF),
            pltpu.VMEM((bands * levels, 2 * padded, lanes), BF),
            pltpu.VMEM((levels, half, lanes), BF),
            pltpu.VMEM((levels * half, 2 * lanes), F32),
            pltpu.SemaphoreType.DMA((32,)),
        ],
        compiler_params=params(61),
        cost_estimate=cost(6e9),
        name="head",
    )(place, fields, *observed)


def relayout_last_kernel(place, in_ref, out_ref, room, *, cols, levels, padded):
    mirrored = place[2] >= place[3]
    for p in range(2):
        room[p, :LEAD] = jnp.zeros((LEAD, levels, 128), BF)
        room[p, LEAD : LEAD + cols] = in_ref[0, p]
        room[p, LEAD + cols] = in_ref[0, p, 0]
        room[p, LEAD + cols + 1 :] = jnp.zeros((LEAD - 1, levels, 128), BF)
    turn = turner(levels, mirrored, 16)
    last_turn = turner(levels, mirrored, cols % 16)
    for start in range(0, padded, 16):
        rows = pl.ds(turn_start(start, mirrored, cols), 16)
        matrix = turn if start + 16 <= cols else last_turn
        turned = turn_block([room[p, rows] for p in range(2)], matrix, levels)
        for l in range(levels):
            for p in range(2):
                piece = turned[16 * l : 16 * l + 16, 128 * p : 128 * p + 128]
                out_ref[p * levels + l, start : start + 16, :] = piece


def relayout_last(place, fields, padded):
    rounds, bands, cols, levels, lanes = fields.shape
    return pl.pallas_call(
        lambda *refs: relayout_last_kernel(*refs, cols=cols, levels=levels, padded=padded),
        grid=(bands // 2,),
        in_specs=[sspec(), pl.BlockSpec((1, 2, cols, levels, lanes), lambda g: (rounds - 1, g, 0, 0, 0))],
        out_specs=pl.BlockSpec((2 * levels, padded, lanes), lambda g: (g, 0, 0)),
        out_shape=jax.ShapeDtypeStruct((bands * levels, padded, lanes), BF),
        scratch_shapes=[pltpu.VMEM((2, cols + 2 * LEAD, levels, lanes), BF)],
        compiler_params=params(58),
        name="relayout_last",
    )(place, fields)


def turn_cos(turns):
    near = 0.25 - jnp.abs(turns - jnp.floor(turns + 0.5))
    square = near * near
    value = jnp.full_like(square, -15.094642576822990)
    for factor in (42.058693944897653, -76.705859753061386, 81.605249276075055, -41.341702240399755):
        value = value * square + factor
    return near * (value * square + 6.283185307179586)


def basis_kernel(lon_ref, lon_t_ref, lat_ref, lat_t_ref, *, cols, blocks, padded):
    total = cols * blocks
    nyquist = total // 2
    width = lon_ref.shape[1] // 2
    lanes = lax.broadcasted_iota(jnp.int32, (padded, 128), 1)

    def turns_of(product):
        whole = (product.astype(F32) * (1.0 / total)).astype(jnp.int32)
        return (product - whole * total).astype(F32) * (1.0 / total)

    def lon_rows(j, carry):
        within = lax.broadcasted_iota(jnp.int32, (padded, 128), 0)
        x = jnp.where(within < cols, within + cols * j, cols * (blocks - 1 - j))
        fine = turns_of(x * lanes)
        coarse = turns_of(x * (lanes * 128))
        fine_cos = turn_cos(fine)
        fine_sin = turn_cos(fine - 0.25)
        scale = jnp.where(within <= cols, math.sqrt(2.0 / total), 0.0)
        coarse_cos = turn_cos(coarse) * scale
        coarse_sin = turn_cos(coarse - 0.25) * scale
        rows = pl.ds(pl.multiple_of(j * padded, padded), padded)
        for t in range(width // 128):
            c = lanes + 128 * t
            cos_t = coarse_cos[:, t : t + 1]
            sin_t = coarse_sin[:, t : t + 1]
            even = fine_cos * cos_t - fine_sin * sin_t
            odd = fine_sin * cos_t + fine_cos * sin_t
            if t == 0 or 128 * t <= nyquist < 128 * t + 128:
                even = jnp.where((c == 0) | (c == nyquist), even * math.sqrt(0.5), even)
            if 128 * t + 127 >= nyquist:
                even = jnp.where(c <= nyquist, even, 0.0)
                odd = jnp.where(c < nyquist, odd, 0.0)
            lon_ref[rows, 128 * t : 128 * t + 128] = even.astype(BF)
            lon_ref[rows, width + 128 * t : width + 128 * t + 128] = odd.astype(BF)
        return carry

    lax.fori_loop(0, blocks // 2, lon_rows, 0)
    for t in range(lon_ref.shape[1] // 128):
        strip = lon_ref[:, 128 * t : 128 * t + 128].astype(F32)
        lon_t_ref[128 * t : 128 * t + 128, :] = strip.T.astype(BF)

    length = lat_ref.shape[0]
    step = 64

    def lat_rows(i, carry):
        shape = (step, length)
        down = lax.broadcasted_iota(jnp.int32, shape, 0) + step * i
        across = lax.broadcasted_iota(jnp.int32, shape, 1)
        rows = pl.ds(pl.multiple_of(i * step, step), step)
        for grid, mode, ref in ((down, across, lat_ref), (across, down, lat_t_ref)):
            phase = (mode * (2 * grid + 1)) & (4 * length - 1)
            scale = jnp.where(mode == 0, 1.0 / math.sqrt(length), math.sqrt(2.0 / length))
            ref[rows, :] = (turn_cos(phase.astype(F32) * (0.25 / length)) * scale).astype(BF)
        return carry

    lax.fori_loop(0, length // step, lat_rows, 0)


def bases(cols, blocks, padded, lat_total):
    tall = padded * blocks // 2
    return pl.pallas_call(
        lambda *refs: basis_kernel(*refs, cols=cols, blocks=blocks, padded=padded),
        out_shape=(
            jax.ShapeDtypeStruct((tall, 2 * tall), BF),
            jax.ShapeDtypeStruct((2 * tall, tall), BF),
            jax.ShapeDtypeStruct((lat_total, lat_total), BF),
            jax.ShapeDtypeStruct((lat_total, lat_total), BF),
        ),
        out_specs=(vspec(),) * 4,
        compiler_params=params(58),
        cost_estimate=cost(12e9),
        name="bases",
    )()


def arrange_kernel(place, own, other, taper, *, rows_each):
    mem, lat = place[0], place[1]
    spare = taper.shape[1] - RING * rows_each
    taper[:, RING * rows_each :, :] = jnp.zeros((4, spare, 128), BF)
    for ref, side in ((own, mem), (other, 1 - mem)):
        for u in range(RING):
            into = pl.ds(pl.multiple_of(lax.rem(lat + RING - u, RING) * rows_each, 8), rows_each)
            for q in range(2):
                taper[2 * side + q, into, :] = ref[u, :, 128 * q : 128 * q + 128]


def arrange(place, own, other):
    rows_each = own.shape[1]
    return pl.pallas_call(
        lambda *refs: arrange_kernel(*refs, rows_each=rows_each),
        out_shape=jax.ShapeDtypeStruct((4, RING * rows_each + 32, 128), BF),
        in_specs=[sspec(), vspec(), vspec()],
        out_specs=vspec(),
        compiler_params=params(12),
        cost_estimate=cost(1e9),
        name="arrange",
    )(place, own, other)


def member_kernel(*refs, first, final, count, blocks, bands, padded, coefs):
    place, field_in, own_in, other_in, taper_hbm, lon_hbm, lon_t_hbm, lat_hbm, lat_t_hbm = refs[:9]
    rest = list(refs[9:])
    so_far_hbm = None if first else rest.pop(0)
    outs = [rest.pop(0) for _ in range(2 if final else 1)]
    folded, inverse, taper, lon_ref, lon_t_ref, lat_ref, lat_t_ref, acc, sems = rest[:9]
    stages = rest[9 : 9 + len(outs)]
    field, own, other = (field_in, own_in, other_in) if final else rest[9 + len(outs) :]
    pairs = blocks // 2
    tall = padded * pairs
    nyquist = coefs // 2
    parts = 4
    step = (nyquist // 2 + 16) // 16 * 16
    group = 4
    turns = pairs // group
    half = padded // 2
    mem = place[0]

    def move(source, target, spot):
        return pltpu.make_async_copy(source, target, sems.at[spot])

    def lon_t_copy(r):
        rows = pl.ds(pl.multiple_of((r // 2) * tall + (r % 2) * step, 16), step)
        return move(lon_t_hbm.at[rows], lon_t_ref.at[rows], 10 + r)

    def lon_copy(b):
        rows = pl.ds(pl.multiple_of(b * group * padded, padded), group * padded)
        return move(lon_hbm.at[rows], lon_ref.at[rows], 14 + b)

    def spots(b, side):
        return pl.ds((blocks - group - b * group) if side else b * group, group)

    def so_far_copy(b, side):
        at = spots(b, side)
        return move(so_far_hbm.at[:, at], acc.at[:, at], 18 + 2 * b + side)

    def out_copy(b, side, n):
        at = spots(b, side)
        return move(stages[n].at[:, at], outs[n].at[:, at], 22 + 4 * n + 2 * b + side)

    field_copies = []
    if not final:
        field_copies = [
            move(own_in, own, 0),
            move(other_in, other, 1),
            *[move(field_in.at[a, :, pl.ds(0, count * padded), :], field.at[a], 2 + a) for a in range(bands)],
        ]
    table_copies = [
        lon_t_copy(0),
        lon_t_copy(2),
        move(lat_hbm, lat_ref, 7),
        move(taper_hbm, taper, 8),
        move(lat_t_hbm, lat_t_ref, 9),
    ]
    for copy in field_copies + table_copies:
        copy.start()
    for side in range(2):
        inverse[side, 2 * step :, :] = jnp.zeros((tall - 2 * step, inverse.shape[2]), BF)
    for copy in field_copies:
        copy.wait()
    down = lax.broadcasted_iota(jnp.int32, (padded, 128), 0)
    cols = coefs // blocks

    def weigh(i, a):
        def product(j):
            mine, theirs = own[a, j], other[a, j]
            innov = jnp.concatenate(
                [jnp.where(mem == 0, mine, theirs), jnp.where(mem == 0, theirs, mine)], axis=0
            )
            return field[a, j, i * padded : (i + 1) * padded, :].astype(F32) * innov.astype(F32)

        def body(j, carry):
            rows = pl.ds(pl.multiple_of(j * padded, padded), padded)
            near = product(j)
            far = product(blocks - 1 - j)
            near = jnp.where(down == cols, far[0:1, :], near)
            far = jnp.where(down == 0, 0.0, far)
            folded[0, rows, 128 * a : 128 * a + 128] = (near + far).astype(BF)
            folded[1, rows, 128 * a : 128 * a + 128] = (near - far).astype(BF)
            return carry

        lax.fori_loop(0, pairs, body, 0)

    def spectral(fresh):
        def body(r, carry):
            rows = pl.ds(pl.multiple_of(r * step, 16), step)
            if fresh:

                @pl.when(r > 0)
                def _():
                    for side in range(2):
                        lon_t_copy(2 * side + r).wait()

            tables = [pl.ds(pl.multiple_of(side * tall + r * step, 16), step) for side in range(2)]
            zonal = [
                jnp.dot(lon_t_ref[tables[side], :], folded[side], preferred_element_type=F32).astype(BF)
                for side in range(2)
            ]
            if fresh:

                @pl.when(r == 0)
                def _():
                    for copy in table_copies[2:]:
                        copy.wait()

            spectrum = [jnp.dot(zonal[side], lat_ref[...], preferred_element_type=F32) for side in range(2)]
            tapered = []
            for side in range(2):
                weight_rows = pl.ds(pl.multiple_of(side * nyquist + r * step, 16), step)
                weights = jnp.concatenate([taper[q, weight_rows, :] for q in range(4)], axis=1).astype(F32)
                tapered.append((spectrum[side] * weights).astype(BF))
            for side in range(2):
                back = jnp.dot(tapered[side], lat_t_ref[...], preferred_element_type=F32)
                inverse[side, rows, :] = back.astype(BF)
            if fresh:

                @pl.when(r == 0)
                def _():
                    for b in range(turns):
                        lon_copy(b).start()
                        if not first:
                            so_far_copy(b, 0).start()
                            so_far_copy(b, 1).start()

            return carry

        lax.fori_loop(0, parts // 2, body, 0)

    def gridded(i):
        def body(b, carry):
            rows = pl.ds(pl.multiple_of(b * group * padded, padded), group * padded)
            if i == 0:
                lon_copy(b).wait()
                if not first:
                    so_far_copy(b, 0).wait()
                    so_far_copy(b, 1).wait()
            even = jnp.dot(lon_ref[rows, :tall], inverse[0], preferred_element_type=F32)
            odd = jnp.dot(lon_ref[rows, tall:], inverse[1], preferred_element_type=F32)

            def put(piece, a, j):
                piece = piece * field[a, j, i * padded : (i + 1) * padded, :].astype(F32)
                piece = piece if first and i == 0 else piece + acc[a, j].astype(F32)
                if final:
                    top, low = piece[:half], piece[half:]
                    stages[0][a, j] = jnp.where(mem == 0, top, low).astype(BF)
                    stages[1][a, j] = jnp.where(mem == 0, low, top).astype(BF)
                elif i == count - 1:
                    stages[0][a, j] = piece.astype(BF)
                else:
                    acc[a, j] = piece

            for g in range(group):
                for a in range(bands):
                    j = b * group + g
                    spot = (slice(g * padded, (g + 1) * padded), slice(128 * a, 128 * a + 128))
                    near = even[spot] + odd[spot]
                    far = jnp.where(down == 0, near[cols : cols + 1, :], even[spot] - odd[spot])
                    put(near, a, j)
                    put(far, a, blocks - 1 - j)
            if i == count - 1:
                for n in range(len(outs)):
                    out_copy(b, 0, n).start()
                    out_copy(b, 1, n).start()
            return carry

        for b in range(turns):
            body(b, 0)

    for i in range(count):
        if i == 0:
            for r in (1, 3):
                lon_t_copy(r).start()
        for a in range(bands):
            weigh(i, a)
        if i == 0:
            for copy in table_copies[:2]:
                copy.wait()
        spectral(i == 0)
        gridded(i)
    for b in range(turns):
        for n in range(len(outs)):
            out_copy(b, 0, n).wait()
            out_copy(b, 1, n).wait()


def member(place, field, own, other, taper, tables, so_far, final, dims):
    _, blocks, bands, padded, coefs, lat_total = dims
    half = padded // 2
    tall = padded * blocks // 2
    first = so_far is None
    count = 1 if final else 2
    split = lambda array: array.reshape(bands, blocks, *array.shape[1:])
    near = [split(field), split(own), split(other)]
    far = [taper, *tables] + ([] if first else [so_far])
    block = lambda rows, dtype: ((bands, blocks, rows, 128), dtype)
    scratch = [((2, tall, lat_total), BF), ((2, tall, lat_total), BF)]
    fields = [] if final else [block(count * padded, BF), block(half, BF), block(half, BF)]
    scratch += [(array.shape, array.dtype) for array in (taper, *tables)]
    scratch.append(block(padded, F32 if first else BF))
    results = [block(half, BF), block(half, BF)] if final else [block(padded, BF)]
    hbm = pl.BlockSpec(memory_space=pltpu.HBM)
    return pl.pallas_call(
        lambda *refs: member_kernel(
            *refs, first=first, final=final, count=count, blocks=blocks, bands=bands, padded=padded, coefs=coefs
        ),
        out_shape=[jax.ShapeDtypeStruct(*each) for each in results],
        in_specs=[sspec()] + [vspec() if final else hbm] * len(near) + [hbm] * len(far),
        out_specs=[hbm] * len(results),
        scratch_shapes=[pltpu.VMEM(*each) for each in scratch]
        + [pltpu.SemaphoreType.DMA((32,))]
        + [pltpu.VMEM(*each) for each in results + fields],
        compiler_params=params(62),
        cost_estimate=cost(count * 6e9),
        name="member_last" if final else "member_pair",
    )(place, *near, *far)


def finish_kernel(place, own, other, out, *, levels, cols, half, scale):
    mem = place[0]
    mirrored = place[2] >= place[3]
    bands = own.shape[0] // levels
    to = lax.broadcasted_iota(jnp.int32, (2 * half, half), 0)
    frm = lax.broadcasted_iota(jnp.int32, (2 * half, half), 1)
    taken = jnp.where(mirrored & (to > 0), cols - to, to)
    picks = [jnp.where(taken == frm + side * half, 1.0, 0.0).astype(BF) for side in (mem, 1 - mem)]
    picks = jnp.concatenate(picks * bands, axis=1)
    columns = []
    for l in range(levels):
        parts = [ref[a * levels + l] for a in range(bands) for ref in (own, other)]
        columns.append(jnp.concatenate(parts, axis=0))
    summed = jnp.dot(picks, jnp.concatenate(columns, axis=1), preferred_element_type=F32) * scale
    for l in range(levels):
        out[:, l, :] = summed[:cols, 128 * l : 128 * l + 128]


def finish(place, own, other, levels, cols, half, scale):
    return pl.pallas_call(
        lambda *refs: finish_kernel(*refs, levels=levels, cols=cols, half=half, scale=scale),
        out_shape=jax.ShapeDtypeStruct((cols, levels, 128), F32),
        in_specs=[sspec(), vspec(), vspec()],
        out_specs=vspec(),
        compiler_params=params(16),
        name="finish",
    )(place, own, other)


def local(anomalies, taper, obs_row, obs_col, obs_level, obs_value):
    members, levels, cols, lat_rows = anomalies.shape
    bands = lax.axis_size("lat")
    blocks = lax.axis_size("lon")
    mem, lat, lon = lax.axis_index("mem"), lax.axis_index("lat"), lax.axis_index("lon")
    coefs = cols * blocks
    lat_total = lat_rows * bands
    padded = -(-cols // 32) * 32
    half = padded // 2
    ensemble = members * lax.axis_size("mem")
    place = jnp.stack([mem, lat, lon, jnp.int32(blocks // 2)]).astype(jnp.int32)

    by_round = jnp.transpose(anomalies, (0, 2, 1, 3)).reshape(members // bands, bands, cols, levels, lat_rows)
    pair_out = head(place, by_round, obs_row, obs_col, obs_level, obs_value, half, padded)
    pair = over_all(pair_out)
    n_half = lat_total // 2
    taper_mine = lax.dynamic_slice_in_dim(taper[0], mem * n_half, n_half, axis=1).astype(BF)
    ring = [taper_mine]
    for u in range(1, RING):
        ring.append(shift_lat(taper_mine, u))
    last_out = relayout_last(place, by_round, padded)
    last = over_all(last_out)
    stacked = jnp.stack(ring)
    weights = arrange(place, stacked, swap(stacked))
    own = pair[:, 2 * padded :, :]
    other = swap(own)

    tables = bases(cols, blocks, padded, lat_total)
    dims = (cols, blocks, bands, padded, coefs, lat_total)
    (summed,) = member(place, pair, own, other, weights, tables, None, False, dims)
    mine, theirs = member(place, last, own, other, weights, tables, summed, True, dims)
    merged = (mine.astype(F32) + swap(theirs).astype(F32)).astype(BF).reshape(bands * blocks, half, lat_rows)
    pieces = over_all(merged)
    out = finish(place, pieces, swap(pieces), levels, cols, half, 1.0 / (ensemble - 1))
    return jnp.transpose(out, (1, 0, 2))


def solution(mesh):
    in_specs = (
        P("mem", None, "lon", "lat"),
        P("lon", "lat", None),
        P("lat", "lon"),
        P("lat", "lon"),
        P("lat", "lon"),
        P("lat", "lon"),
    )
    out_specs = P(None, "lon", "lat")

    return jax.shard_map(local, mesh=mesh, in_specs=in_specs, out_specs=out_specs, check_vma=False)
```

```python
import math

import jax
import jax.numpy as jnp
from jax import lax
from jax.experimental import pallas as pl
from jax.experimental.pallas import tpu as pltpu
from jax.sharding import PartitionSpec as P


BF = jnp.bfloat16
F32 = jnp.float32
LL = ("lat", "lon")
SWAP = [(0, 1), (1, 0)]
RING = 4


def vspec():
    return pl.BlockSpec(memory_space=pltpu.VMEM)


def sspec():
    return pl.BlockSpec(memory_space=pltpu.SMEM)


def params(mib, **more):
    return pltpu.CompilerParams(vmem_limit_bytes=mib * 1024 * 1024, **more)


def cost(flops):
    return pl.CostEstimate(flops=int(flops), bytes_accessed=1 << 20, transcendentals=0)


def over_all(x):
    return lax.all_to_all(x, LL, split_axis=0, concat_axis=0, tiled=True)


def shift_lat(x, s):
    return lax.ppermute(x, "lat", [(i, (i + s) % RING) for i in range(RING)])


def swap(x):
    return lax.ppermute(x, "mem", SWAP)


LEAD = 6


def turn_block(blocks, turn, levels):
    both = jnp.concatenate([block.reshape(16 * levels, 128) for block in blocks], axis=1)
    return jnp.dot(turn, both, preferred_element_type=F32).astype(BF)


def turner(levels, mirrored, have):
    size = 16 * levels
    to = lax.broadcasted_iota(jnp.int32, (size, size), 0)
    frm = lax.broadcasted_iota(jnp.int32, (size, size), 1)
    within = to & 15
    taken = jnp.where(mirrored, 15 - within, within)
    return jnp.where((frm == taken * levels + (to >> 4)) & (within < have), 1.0, 0.0).astype(BF)


def turn_start(start, mirrored, cols):
    return jnp.where(mirrored, LEAD + cols - 15 - start, LEAD + start)


def head_kernel(fields, row_hbm, col_hbm, level_hbm, value_hbm, out, *scratch, half, levels, cols, padded):
    row_ref, col_ref, level_ref, value_ref, fields_in, staged, innov, acc, sems = scratch
    bands = fields.shape[1]
    count = iter(range(32))

    def fetch(source, target):
        copy = pltpu.make_async_copy(source, target, sems.at[next(count)])
        copy.start()
        return copy

    observed = [
        fetch(row_hbm, row_ref),
        fetch(col_hbm, col_ref),
        fetch(level_hbm, level_ref),
        fetch(value_hbm, value_ref),
    ]
    arriving = [
        (
            fetch(fields.at[pl.ds(0, 2), g], fields_in.at[:, g, pl.ds(LEAD, cols)]),
            fetch(fields.at[pl.ds(0, 2), g, pl.ds(0, 1)], fields_in.at[:, g, pl.ds(LEAD + cols, 1)]),
        )
        for g in range(bands)
    ]
    mem, lat, lon = lax.axis_index("mem"), lax.axis_index("lat"), lax.axis_index("lon")
    mirrored = lon >= lax.axis_size("lon") // 2
    for p in range(2):
        for g in range(bands):
            fields_in[p, g, :LEAD] = jnp.zeros((LEAD, levels, 128), BF)
            fields_in[p, g, LEAD + cols + 1 :] = jnp.zeros((LEAD - 1, levels, 128), BF)
    slots = levels * half
    acc[...] = jnp.zeros_like(acc)

    def spots_of(count):
        major = lax.broadcasted_iota(jnp.int32, (count // 16, 16, 128), 0)
        minor = lax.broadcasted_iota(jnp.int32, (count // 16, 16, 128), 1)
        return (major * 16 + minor).astype(F32).astype(BF)

    def packed(row):
        return jnp.broadcast_to(row, (16, 128)).astype(BF)[None]

    slot_ids = spots_of(256)
    row_ids = spots_of(128)
    one = jnp.ones((), BF)
    zero = jnp.zeros((), BF)
    for copy in observed:
        copy.wait()

    def add_group(g, carry):
        rows = pl.ds(pl.multiple_of(g * 16, 8), 16)
        column = col_ref[rows, :] - lon * cols
        within = jnp.where(mirrored & (column > 0), cols - column, column) - mem * half
        inside = (within >= 0) & (within < half)
        keys = jnp.where(inside, level_ref[rows, :] * half + within, -1)
        lat_row = (row_ref[rows, :] - lat * 128).astype(F32)
        value = value_ref[rows, :]
        high = value.astype(BF).astype(F32)
        middle = value - high
        parts = []
        for start in range(0, slots, 256):
            part = keys - start
            parts.append(jnp.where((part >= 0) & (part < 256), part, -1).astype(F32))
        left = []
        right = []
        for r in range(16):
            at = slice(r, r + 1)
            hits = [jnp.where(slot_ids == packed(part[at]), one, zero).reshape(256, 128) for part in parts]
            left.append(jnp.concatenate(hits, axis=0))
            row_hit = row_ids == packed(lat_row[at])
            sides = [jnp.where(row_hit, packed(side[at]), zero).reshape(128, 128) for side in (high, middle)]
            right.append(jnp.concatenate(sides, axis=0))
        acc[...] += lax.dot_general(
            jnp.concatenate(left, axis=1),
            jnp.concatenate(right, axis=1),
            (((1,), (1,)), ((), ())),
            preferred_element_type=F32,
        )
        return carry

    leaving = []
    lax.fori_loop(0, 2, add_group, 0)
    turn = turner(levels, mirrored, 16)
    last_turn = turner(levels, mirrored, cols % 16)
    for first in range(0, bands, 2):
        group = range(first, first + 2)
        for g in group:
            for copy in arriving[g]:
                copy.wait()
        for start in range(0, padded, 16):
            rows = pl.ds(turn_start(start, mirrored, cols), 16)
            matrix = turn if start + 16 <= cols else last_turn
            turned = turn_block([fields_in[p, g, rows] for g in group for p in range(2)], matrix, levels)
            for l in range(levels):
                for n, g in enumerate(group):
                    for p in range(2):
                        lane = 256 * n + 128 * p
                        piece = turned[16 * l : 16 * l + 16, lane : lane + 128]
                        staged[g * levels + l, p * padded + start : p * padded + start + 16, :] = piece
        for g in group:
            leaving.append(
                fetch(
                    staged.at[pl.ds(g * levels, levels)],
                    out.at[pl.ds(g * levels, levels), pl.ds(0, 2 * padded), :],
                )
            )
    lax.fori_loop(2, row_ref.shape[0] // 16, add_group, 0)
    innov[...] = (acc[:, :128] + acc[:, 128:]).astype(BF).reshape(levels, half, 128)
    leaving += [
        fetch(innov, out.at[pl.ds(g * levels, levels), pl.ds(2 * padded, half), :]) for g in range(bands)
    ]
    for copy in leaving:
        copy.wait()


def head(fields, obs_row, obs_col, obs_level, obs_value, half, padded):
    _, bands, cols, levels, lanes = fields.shape
    rows = 2 * padded + half
    hbm = pl.BlockSpec(memory_space=pltpu.HBM)
    observed = (obs_row, obs_col, obs_level, obs_value)
    return pl.pallas_call(
        lambda *refs: head_kernel(*refs, half=half, levels=levels, cols=cols, padded=padded),
        out_shape=jax.ShapeDtypeStruct((bands * levels, rows, lanes), BF),
        in_specs=[hbm] * 5,
        out_specs=hbm,
        scratch_shapes=[pltpu.VMEM(array.shape, array.dtype) for array in observed]
        + [
            pltpu.VMEM((2, bands, cols + 2 * LEAD, levels, lanes), BF),
            pltpu.VMEM((bands * levels, 2 * padded, lanes), BF),
            pltpu.VMEM((levels, half, lanes), BF),
            pltpu.VMEM((levels * half, 2 * lanes), F32),
            pltpu.SemaphoreType.DMA((32,)),
        ],
        compiler_params=params(61),
        cost_estimate=cost(6e9),
        name="head",
    )(fields, *observed)


def relayout_last_kernel(place, in_ref, out_ref, room, *, cols, levels, padded):
    mirrored = place[2] >= place[3]
    for p in range(2):
        room[p, :LEAD] = jnp.zeros((LEAD, levels, 128), BF)
        room[p, LEAD : LEAD + cols] = in_ref[0, p]
        room[p, LEAD + cols] = in_ref[0, p, 0]
        room[p, LEAD + cols + 1 :] = jnp.zeros((LEAD - 1, levels, 128), BF)
    turn = turner(levels, mirrored, 16)
    last_turn = turner(levels, mirrored, cols % 16)
    for start in range(0, padded, 16):
        rows = pl.ds(turn_start(start, mirrored, cols), 16)
        matrix = turn if start + 16 <= cols else last_turn
        turned = turn_block([room[p, rows] for p in range(2)], matrix, levels)
        for l in range(levels):
            for p in range(2):
                piece = turned[16 * l : 16 * l + 16, 128 * p : 128 * p + 128]
                out_ref[p * levels + l, start : start + 16, :] = piece


def relayout_last(place, fields, padded):
    rounds, bands, cols, levels, lanes = fields.shape
    return pl.pallas_call(
        lambda *refs: relayout_last_kernel(*refs, cols=cols, levels=levels, padded=padded),
        grid=(bands // 2,),
        in_specs=[sspec(), pl.BlockSpec((1, 2, cols, levels, lanes), lambda g: (rounds - 1, g, 0, 0, 0))],
        out_specs=pl.BlockSpec((2 * levels, padded, lanes), lambda g: (g, 0, 0)),
        out_shape=jax.ShapeDtypeStruct((bands * levels, padded, lanes), BF),
        scratch_shapes=[pltpu.VMEM((2, cols + 2 * LEAD, levels, lanes), BF)],
        compiler_params=params(58),
        name="relayout_last",
    )(place, fields)


def turn_cos(turns):
    near = 0.25 - jnp.abs(turns - jnp.floor(turns + 0.5))
    square = near * near
    value = jnp.full_like(square, -15.094642576822990)
    for factor in (42.058693944897653, -76.705859753061386, 81.605249276075055, -41.341702240399755):
        value = value * square + factor
    return near * (value * square + 6.283185307179586)


def basis_kernel(lon_ref, lon_t_ref, lat_ref, lat_t_ref, *, cols, blocks, padded):
    total = cols * blocks
    nyquist = total // 2
    width = lon_ref.shape[1] // 2
    lanes = lax.broadcasted_iota(jnp.int32, (padded, 128), 1)

    def turns_of(product):
        whole = (product.astype(F32) * (1.0 / total)).astype(jnp.int32)
        return (product - whole * total).astype(F32) * (1.0 / total)

    def lon_rows(j, carry):
        within = lax.broadcasted_iota(jnp.int32, (padded, 128), 0)
        x = jnp.where(within < cols, within + cols * j, cols * (blocks - 1 - j))
        fine = turns_of(x * lanes)
        coarse = turns_of(x * (lanes * 128))
        fine_cos = turn_cos(fine)
        fine_sin = turn_cos(fine - 0.25)
        scale = jnp.where(within <= cols, math.sqrt(2.0 / total), 0.0)
        coarse_cos = turn_cos(coarse) * scale
        coarse_sin = turn_cos(coarse - 0.25) * scale
        rows = pl.ds(pl.multiple_of(j * padded, padded), padded)
        for t in range(width // 128):
            c = lanes + 128 * t
            cos_t = coarse_cos[:, t : t + 1]
            sin_t = coarse_sin[:, t : t + 1]
            even = fine_cos * cos_t - fine_sin * sin_t
            odd = fine_sin * cos_t + fine_cos * sin_t
            if t == 0 or 128 * t <= nyquist < 128 * t + 128:
                even = jnp.where((c == 0) | (c == nyquist), even * math.sqrt(0.5), even)
            if 128 * t + 127 >= nyquist:
                even = jnp.where(c <= nyquist, even, 0.0)
                odd = jnp.where(c < nyquist, odd, 0.0)
            lon_ref[rows, 128 * t : 128 * t + 128] = even.astype(BF)
            lon_ref[rows, width + 128 * t : width + 128 * t + 128] = odd.astype(BF)
        return carry

    lax.fori_loop(0, blocks // 2, lon_rows, 0)
    for t in range(lon_ref.shape[1] // 128):
        strip = lon_ref[:, 128 * t : 128 * t + 128].astype(F32)
        lon_t_ref[128 * t : 128 * t + 128, :] = strip.T.astype(BF)

    length = lat_ref.shape[0]
    step = 64

    def lat_rows(i, carry):
        shape = (step, length)
        down = lax.broadcasted_iota(jnp.int32, shape, 0) + step * i
        across = lax.broadcasted_iota(jnp.int32, shape, 1)
        rows = pl.ds(pl.multiple_of(i * step, step), step)
        for grid, mode, ref in ((down, across, lat_ref), (across, down, lat_t_ref)):
            phase = (mode * (2 * grid + 1)) & (4 * length - 1)
            scale = jnp.where(mode == 0, 1.0 / math.sqrt(length), math.sqrt(2.0 / length))
            ref[rows, :] = (turn_cos(phase.astype(F32) * (0.25 / length)) * scale).astype(BF)
        return carry

    lax.fori_loop(0, length // step, lat_rows, 0)


def bases(cols, blocks, padded, lat_total):
    tall = padded * blocks // 2
    return pl.pallas_call(
        lambda *refs: basis_kernel(*refs, cols=cols, blocks=blocks, padded=padded),
        out_shape=(
            jax.ShapeDtypeStruct((tall, 2 * tall), BF),
            jax.ShapeDtypeStruct((2 * tall, tall), BF),
            jax.ShapeDtypeStruct((lat_total, lat_total), BF),
            jax.ShapeDtypeStruct((lat_total, lat_total), BF),
        ),
        out_specs=(vspec(),) * 4,
        compiler_params=params(58),
        cost_estimate=cost(12e9),
        name="bases",
    )()


def arrange_kernel(place, own, other, taper, *, rows_each):
    mem, lat = place[0], place[1]
    spare = taper.shape[1] - RING * rows_each
    taper[:, RING * rows_each :, :] = jnp.zeros((4, spare, 128), BF)
    for ref, side in ((own, mem), (other, 1 - mem)):
        for u in range(RING):
            into = pl.ds(pl.multiple_of(lax.rem(lat + RING - u, RING) * rows_each, 8), rows_each)
            for q in range(2):
                taper[2 * side + q, into, :] = ref[u, :, 128 * q : 128 * q + 128]


def arrange(place, own, other):
    rows_each = own.shape[1]
    return pl.pallas_call(
        lambda *refs: arrange_kernel(*refs, rows_each=rows_each),
        out_shape=jax.ShapeDtypeStruct((4, RING * rows_each + 32, 128), BF),
        in_specs=[sspec(), vspec(), vspec()],
        out_specs=vspec(),
        compiler_params=params(12),
        cost_estimate=cost(1e9),
        name="arrange",
    )(place, own, other)


def member_kernel(*refs, first, final, count, blocks, bands, padded, coefs):
    place, field_in, own_in, other_in, taper_hbm, lon_hbm, lon_t_hbm, lat_hbm, lat_t_hbm = refs[:9]
    rest = list(refs[9:])
    so_far_hbm = None if first else rest.pop(0)
    outs = [rest.pop(0) for _ in range(2 if final else 1)]
    folded, inverse, taper, lon_ref, lon_t_ref, lat_ref, lat_t_ref, acc, sems = rest[:9]
    stages = rest[9 : 9 + len(outs)]
    field, own, other = (field_in, own_in, other_in) if final else rest[9 + len(outs) :]
    pairs = blocks // 2
    tall = padded * pairs
    nyquist = coefs // 2
    parts = 4
    step = (nyquist // 2 + 16) // 16 * 16
    group = 4
    turns = pairs // group
    half = padded // 2
    mem = place[0]

    def move(source, target, spot):
        return pltpu.make_async_copy(source, target, sems.at[spot])

    def lon_t_copy(r):
        rows = pl.ds(pl.multiple_of((r // 2) * tall + (r % 2) * step, 16), step)
        return move(lon_t_hbm.at[rows], lon_t_ref.at[rows], 10 + r)

    def lon_copy(b):
        rows = pl.ds(pl.multiple_of(b * group * padded, padded), group * padded)
        return move(lon_hbm.at[rows], lon_ref.at[rows], 14 + b)

    def spots(b, side):
        return pl.ds((blocks - group - b * group) if side else b * group, group)

    def so_far_copy(b, side):
        at = spots(b, side)
        return move(so_far_hbm.at[:, at], acc.at[:, at], 18 + 2 * b + side)

    def out_copy(b, side, n):
        at = spots(b, side)
        return move(stages[n].at[:, at], outs[n].at[:, at], 22 + 4 * n + 2 * b + side)

    field_copies = []
    if not final:
        field_copies = [
            move(own_in, own, 0),
            move(other_in, other, 1),
            *[move(field_in.at[a, :, pl.ds(0, count * padded), :], field.at[a], 2 + a) for a in range(bands)],
        ]
    table_copies = [
        lon_t_copy(0),
        lon_t_copy(2),
        move(lat_hbm, lat_ref, 7),
        move(taper_hbm, taper, 8),
        move(lat_t_hbm, lat_t_ref, 9),
    ]
    for copy in field_copies + table_copies:
        copy.start()
    for side in range(2):
        inverse[side, 2 * step :, :] = jnp.zeros((tall - 2 * step, inverse.shape[2]), BF)
    for copy in field_copies:
        copy.wait()
    down = lax.broadcasted_iota(jnp.int32, (padded, 128), 0)
    cols = coefs // blocks

    def weigh(i, a):
        def product(j):
            mine, theirs = own[a, j], other[a, j]
            innov = jnp.concatenate(
                [jnp.where(mem == 0, mine, theirs), jnp.where(mem == 0, theirs, mine)], axis=0
            )
            return field[a, j, i * padded : (i + 1) * padded, :].astype(F32) * innov.astype(F32)

        def body(j, carry):
            rows = pl.ds(pl.multiple_of(j * padded, padded), padded)
            near = product(j)
            far = product(blocks - 1 - j)
            near = jnp.where(down == cols, far[0:1, :], near)
            far = jnp.where(down == 0, 0.0, far)
            folded[0, rows, 128 * a : 128 * a + 128] = (near + far).astype(BF)
            folded[1, rows, 128 * a : 128 * a + 128] = (near - far).astype(BF)
            return carry

        lax.fori_loop(0, pairs, body, 0)

    def spectral(fresh):
        def body(r, carry):
            rows = pl.ds(pl.multiple_of(r * step, 16), step)
            if fresh:

                @pl.when(r > 0)
                def _():
                    for side in range(2):
                        lon_t_copy(2 * side + r).wait()

            tables = [pl.ds(pl.multiple_of(side * tall + r * step, 16), step) for side in range(2)]
            zonal = [
                jnp.dot(lon_t_ref[tables[side], :], folded[side], preferred_element_type=F32).astype(BF)
                for side in range(2)
            ]
            if fresh:

                @pl.when(r == 0)
                def _():
                    for copy in table_copies[2:]:
                        copy.wait()

            spectrum = [jnp.dot(zonal[side], lat_ref[...], preferred_element_type=F32) for side in range(2)]
            tapered = []
            for side in range(2):
                weight_rows = pl.ds(pl.multiple_of(side * nyquist + r * step, 16), step)
                weights = jnp.concatenate([taper[q, weight_rows, :] for q in range(4)], axis=1).astype(F32)
                tapered.append((spectrum[side] * weights).astype(BF))
            for side in range(2):
                back = jnp.dot(tapered[side], lat_t_ref[...], preferred_element_type=F32)
                inverse[side, rows, :] = back.astype(BF)
            if fresh:

                @pl.when(r == 0)
                def _():
                    for b in range(turns):
                        lon_copy(b).start()
                        if not first:
                            so_far_copy(b, 0).start()
                            so_far_copy(b, 1).start()

            return carry

        lax.fori_loop(0, parts // 2, body, 0)

    def gridded(i):
        def body(b, carry):
            rows = pl.ds(pl.multiple_of(b * group * padded, padded), group * padded)
            if i == 0:
                lon_copy(b).wait()
                if not first:
                    so_far_copy(b, 0).wait()
                    so_far_copy(b, 1).wait()
            even = jnp.dot(lon_ref[rows, :tall], inverse[0], preferred_element_type=F32)
            odd = jnp.dot(lon_ref[rows, tall:], inverse[1], preferred_element_type=F32)

            def put(piece, a, j):
                piece = piece * field[a, j, i * padded : (i + 1) * padded, :].astype(F32)
                piece = piece if first and i == 0 else piece + acc[a, j].astype(F32)
                if final:
                    top, low = piece[:half], piece[half:]
                    stages[0][a, j] = jnp.where(mem == 0, top, low).astype(BF)
                    stages[1][a, j] = jnp.where(mem == 0, low, top).astype(BF)
                elif i == count - 1:
                    stages[0][a, j] = piece.astype(BF)
                else:
                    acc[a, j] = piece

            for g in range(group):
                for a in range(bands):
                    j = b * group + g
                    spot = (slice(g * padded, (g + 1) * padded), slice(128 * a, 128 * a + 128))
                    near = even[spot] + odd[spot]
                    far = jnp.where(down == 0, near[cols : cols + 1, :], even[spot] - odd[spot])
                    put(near, a, j)
                    put(far, a, blocks - 1 - j)
            if i == count - 1:
                for n in range(len(outs)):
                    out_copy(b, 0, n).start()
                    out_copy(b, 1, n).start()
            return carry

        for b in range(turns):
            body(b, 0)

    for i in range(count):
        if i == 0:
            for r in (1, 3):
                lon_t_copy(r).start()
        for a in range(bands):
            weigh(i, a)
        if i == 0:
            for copy in table_copies[:2]:
                copy.wait()
        spectral(i == 0)
        gridded(i)
    for b in range(turns):
        for n in range(len(outs)):
            out_copy(b, 0, n).wait()
            out_copy(b, 1, n).wait()


def member(place, field, own, other, taper, tables, so_far, final, dims):
    _, blocks, bands, padded, coefs, lat_total = dims
    half = padded // 2
    tall = padded * blocks // 2
    first = so_far is None
    count = 1 if final else 2
    split = lambda array: array.reshape(bands, blocks, *array.shape[1:])
    near = [split(field), split(own), split(other)]
    far = [taper, *tables] + ([] if first else [so_far])
    block = lambda rows, dtype: ((bands, blocks, rows, 128), dtype)
    scratch = [((2, tall, lat_total), BF), ((2, tall, lat_total), BF)]
    fields = [] if final else [block(count * padded, BF), block(half, BF), block(half, BF)]
    scratch += [(array.shape, array.dtype) for array in (taper, *tables)]
    scratch.append(block(padded, F32 if first else BF))
    results = [block(half, BF), block(half, BF)] if final else [block(padded, BF)]
    hbm = pl.BlockSpec(memory_space=pltpu.HBM)
    return pl.pallas_call(
        lambda *refs: member_kernel(
            *refs, first=first, final=final, count=count, blocks=blocks, bands=bands, padded=padded, coefs=coefs
        ),
        out_shape=[jax.ShapeDtypeStruct(*each) for each in results],
        in_specs=[sspec()] + [vspec() if final else hbm] * len(near) + [hbm] * len(far),
        out_specs=[hbm] * len(results),
        scratch_shapes=[pltpu.VMEM(*each) for each in scratch]
        + [pltpu.SemaphoreType.DMA((32,))]
        + [pltpu.VMEM(*each) for each in results + fields],
        compiler_params=params(62),
        cost_estimate=cost(count * 6e9),
        name="member_last" if final else "member_pair",
    )(place, *near, *far)


def finish_kernel(place, own, other, out, *, levels, cols, half, scale):
    mem = place[0]
    mirrored = place[2] >= place[3]
    bands = own.shape[0] // levels
    to = lax.broadcasted_iota(jnp.int32, (2 * half, half), 0)
    frm = lax.broadcasted_iota(jnp.int32, (2 * half, half), 1)
    taken = jnp.where(mirrored & (to > 0), cols - to, to)
    picks = [jnp.where(taken == frm + side * half, 1.0, 0.0).astype(BF) for side in (mem, 1 - mem)]
    picks = jnp.concatenate(picks * bands, axis=1)
    columns = []
    for l in range(levels):
        parts = [ref[a * levels + l] for a in range(bands) for ref in (own, other)]
        columns.append(jnp.concatenate(parts, axis=0))
    summed = jnp.dot(picks, jnp.concatenate(columns, axis=1), preferred_element_type=F32) * scale
    for l in range(levels):
        out[:, l, :] = summed[:cols, 128 * l : 128 * l + 128]


def finish(place, own, other, levels, cols, half, scale):
    return pl.pallas_call(
        lambda *refs: finish_kernel(*refs, levels=levels, cols=cols, half=half, scale=scale),
        out_shape=jax.ShapeDtypeStruct((cols, levels, 128), F32),
        in_specs=[sspec(), vspec(), vspec()],
        out_specs=vspec(),
        compiler_params=params(16),
        name="finish",
    )(place, own, other)


def local(anomalies, taper, obs_row, obs_col, obs_level, obs_value):
    members, levels, cols, lat_rows = anomalies.shape
    bands = lax.axis_size("lat")
    blocks = lax.axis_size("lon")
    mem, lat, lon = lax.axis_index("mem"), lax.axis_index("lat"), lax.axis_index("lon")
    coefs = cols * blocks
    lat_total = lat_rows * bands
    padded = -(-cols // 32) * 32
    half = padded // 2
    ensemble = members * lax.axis_size("mem")
    place = jnp.stack([mem, lat, lon, jnp.int32(blocks // 2)]).astype(jnp.int32)

    by_round = jnp.transpose(anomalies, (0, 2, 1, 3)).reshape(members // bands, bands, cols, levels, lat_rows)
    pair_out = head(by_round, obs_row, obs_col, obs_level, obs_value, half, padded)
    pair_out, taper = lax.optimization_barrier((pair_out, taper))
    pair = over_all(pair_out)
    n_half = lat_total // 2
    taper_mine = lax.dynamic_slice_in_dim(taper[0], mem * n_half, n_half, axis=1).astype(BF)
    ring = [taper_mine]
    for u in range(1, RING):
        ring.append(shift_lat(taper_mine, u))
    last_out = relayout_last(place, by_round, padded)
    last = over_all(last_out)
    stacked = jnp.stack(ring)
    weights = arrange(place, stacked, swap(stacked))
    own = pair[:, 2 * padded :, :]
    other = swap(own)

    tables = bases(cols, blocks, padded, lat_total)
    dims = (cols, blocks, bands, padded, coefs, lat_total)
    (summed,) = member(place, pair, own, other, weights, tables, None, False, dims)
    mine, theirs = member(place, last, own, other, weights, tables, summed, True, dims)
    merged = (mine.astype(F32) + swap(theirs).astype(F32)).astype(BF).reshape(bands * blocks, half, lat_rows)
    pieces = over_all(merged)
    out = finish(place, pieces, swap(pieces), levels, cols, half, 1.0 / (ensemble - 1))
    return jnp.transpose(out, (1, 0, 2))


def solution(mesh):
    in_specs = (
        P("mem", None, "lon", "lat"),
        P("lon", "lat", None),
        P("lat", "lon"),
        P("lat", "lon"),
        P("lat", "lon"),
        P("lat", "lon"),
    )
    out_specs = P(None, "lon", "lat")

    return jax.shard_map(local, mesh=mesh, in_specs=in_specs, out_specs=out_specs, check_vma=False)
```

```python
import math

import jax
import jax.numpy as jnp
from jax import lax
from jax.experimental import pallas as pl
from jax.experimental.pallas import tpu as pltpu
from jax.sharding import PartitionSpec as P


BF = jnp.bfloat16
F32 = jnp.float32
LL = ("lat", "lon")
SWAP = [(0, 1), (1, 0)]
RING = 4


def vspec():
    return pl.BlockSpec(memory_space=pltpu.VMEM)


def sspec():
    return pl.BlockSpec(memory_space=pltpu.SMEM)


def params(mib, **more):
    return pltpu.CompilerParams(vmem_limit_bytes=mib * 1024 * 1024, **more)


def cost(flops):
    return pl.CostEstimate(flops=int(flops), bytes_accessed=1 << 20, transcendentals=0)


def over_all(x):
    return lax.all_to_all(x, LL, split_axis=0, concat_axis=0, tiled=True)


def shift_lat(x, s):
    return lax.ppermute(x, "lat", [(i, (i + s) % RING) for i in range(RING)])


def beside_pairs():
    turns = (1, RING - 1)
    return [(2 * i + m, 2 * ((i + turns[m]) % RING) + m) for i in range(RING) for m in range(2)]


def swap(x):
    return lax.ppermute(x, "mem", SWAP)


LEAD = 6


def turn_block(blocks, turn, levels):
    both = jnp.concatenate([block.reshape(16 * levels, 128) for block in blocks], axis=1)
    return jnp.dot(turn, both, preferred_element_type=F32).astype(BF)


def turner(levels, mirrored, have):
    size = 16 * levels
    to = lax.broadcasted_iota(jnp.int32, (size, size), 0)
    frm = lax.broadcasted_iota(jnp.int32, (size, size), 1)
    within = to & 15
    taken = jnp.where(mirrored, 15 - within, within)
    return jnp.where((frm == taken * levels + (to >> 4)) & (within < have), 1.0, 0.0).astype(BF)


def turn_start(start, mirrored, cols):
    return jnp.where(mirrored, LEAD + cols - 15 - start, LEAD + start)


def head_kernel(fields, row_hbm, col_hbm, level_hbm, value_hbm, out, *scratch, half, levels, cols, padded):
    row_ref, col_ref, level_ref, value_ref, fields_in, staged, innov, acc, sems = scratch
    bands = fields.shape[1]
    count = iter(range(32))

    def fetch(source, target):
        copy = pltpu.make_async_copy(source, target, sems.at[next(count)])
        copy.start()
        return copy

    observed = [
        fetch(row_hbm, row_ref),
        fetch(col_hbm, col_ref),
        fetch(level_hbm, level_ref),
        fetch(value_hbm, value_ref),
    ]
    arriving = [
        (
            fetch(fields.at[pl.ds(0, 2), g], fields_in.at[:, g, pl.ds(LEAD, cols)]),
            fetch(fields.at[pl.ds(0, 2), g, pl.ds(0, 1)], fields_in.at[:, g, pl.ds(LEAD + cols, 1)]),
        )
        for g in range(bands)
    ]
    mem, lat, lon = lax.axis_index("mem"), lax.axis_index("lat"), lax.axis_index("lon")
    mirrored = lon >= lax.axis_size("lon") // 2
    for p in range(2):
        for g in range(bands):
            fields_in[p, g, :LEAD] = jnp.zeros((LEAD, levels, 128), BF)
            fields_in[p, g, LEAD + cols + 1 :] = jnp.zeros((LEAD - 1, levels, 128), BF)
    slots = levels * half
    acc[...] = jnp.zeros_like(acc)

    def spots_of(count):
        major = lax.broadcasted_iota(jnp.int32, (count // 16, 16, 128), 0)
        minor = lax.broadcasted_iota(jnp.int32, (count // 16, 16, 128), 1)
        return (major * 16 + minor).astype(F32).astype(BF)

    def packed(row):
        return jnp.broadcast_to(row, (16, 128)).astype(BF)[None]

    slot_ids = spots_of(256)
    row_ids = spots_of(128)
    one = jnp.ones((), BF)
    zero = jnp.zeros((), BF)
    for copy in observed:
        copy.wait()

    def add_group(g, carry):
        rows = pl.ds(pl.multiple_of(g * 16, 8), 16)
        column = col_ref[rows, :] - lon * cols
        within = jnp.where(mirrored & (column > 0), cols - column, column) - mem * half
        inside = (within >= 0) & (within < half)
        keys = jnp.where(inside, level_ref[rows, :] * half + within, -1)
        lat_row = (row_ref[rows, :] - lat * 128).astype(F32)
        value = value_ref[rows, :]
        high = value.astype(BF).astype(F32)
        middle = value - high
        parts = []
        for start in range(0, slots, 256):
            part = keys - start
            parts.append(jnp.where((part >= 0) & (part < 256), part, -1).astype(F32))
        left = []
        right = []
        for r in range(16):
            at = slice(r, r + 1)
            hits = [jnp.where(slot_ids == packed(part[at]), one, zero).reshape(256, 128) for part in parts]
            left.append(jnp.concatenate(hits, axis=0))
            row_hit = row_ids == packed(lat_row[at])
            sides = [jnp.where(row_hit, packed(side[at]), zero).reshape(128, 128) for side in (high, middle)]
            right.append(jnp.concatenate(sides, axis=0))
        acc[...] += lax.dot_general(
            jnp.concatenate(left, axis=1),
            jnp.concatenate(right, axis=1),
            (((1,), (1,)), ((), ())),
            preferred_element_type=F32,
        )
        return carry

    leaving = []
    lax.fori_loop(0, 2, add_group, 0)
    turn = turner(levels, mirrored, 16)
    last_turn = turner(levels, mirrored, cols % 16)
    for first in range(0, bands, 2):
        group = range(first, first + 2)
        for g in group:
            for copy in arriving[g]:
                copy.wait()
        for start in range(0, padded, 16):
            rows = pl.ds(turn_start(start, mirrored, cols), 16)
            matrix = turn if start + 16 <= cols else last_turn
            turned = turn_block([fields_in[p, g, rows] for g in group for p in range(2)], matrix, levels)
            for l in range(levels):
                for n, g in enumerate(group):
                    for p in range(2):
                        lane = 256 * n + 128 * p
                        piece = turned[16 * l : 16 * l + 16, lane : lane + 128]
                        staged[g * levels + l, p * padded + start : p * padded + start + 16, :] = piece
        for g in group:
            leaving.append(
                fetch(
                    staged.at[pl.ds(g * levels, levels)],
                    out.at[pl.ds(g * levels, levels), pl.ds(0, 2 * padded), :],
                )
            )
    lax.fori_loop(2, row_ref.shape[0] // 16, add_group, 0)
    innov[...] = (acc[:, :128] + acc[:, 128:]).astype(BF).reshape(levels, half, 128)
    leaving += [
        fetch(innov, out.at[pl.ds(g * levels, levels), pl.ds(2 * padded, half), :]) for g in range(bands)
    ]
    for copy in leaving:
        copy.wait()


def head(fields, obs_row, obs_col, obs_level, obs_value, half, padded):
    _, bands, cols, levels, lanes = fields.shape
    rows = 2 * padded + half
    hbm = pl.BlockSpec(memory_space=pltpu.HBM)
    observed = (obs_row, obs_col, obs_level, obs_value)
    return pl.pallas_call(
        lambda *refs: head_kernel(*refs, half=half, levels=levels, cols=cols, padded=padded),
        out_shape=jax.ShapeDtypeStruct((bands * levels, rows, lanes), BF),
        in_specs=[hbm] * 5,
        out_specs=hbm,
        scratch_shapes=[pltpu.VMEM(array.shape, array.dtype) for array in observed]
        + [
            pltpu.VMEM((2, bands, cols + 2 * LEAD, levels, lanes), BF),
            pltpu.VMEM((bands * levels, 2 * padded, lanes), BF),
            pltpu.VMEM((levels, half, lanes), BF),
            pltpu.VMEM((levels * half, 2 * lanes), F32),
            pltpu.SemaphoreType.DMA((32,)),
        ],
        compiler_params=params(61),
        cost_estimate=cost(6e9),
        name="head",
    )(fields, *observed)


def relayout_last_kernel(place, in_ref, out_ref, room, *, cols, levels, padded):
    mirrored = place[2] >= place[3]
    for p in range(2):
        room[p, :LEAD] = jnp.zeros((LEAD, levels, 128), BF)
        room[p, LEAD : LEAD + cols] = in_ref[0, p]
        room[p, LEAD + cols] = in_ref[0, p, 0]
        room[p, LEAD + cols + 1 :] = jnp.zeros((LEAD - 1, levels, 128), BF)
    turn = turner(levels, mirrored, 16)
    last_turn = turner(levels, mirrored, cols % 16)
    for start in range(0, padded, 16):
        rows = pl.ds(turn_start(start, mirrored, cols), 16)
        matrix = turn if start + 16 <= cols else last_turn
        turned = turn_block([room[p, rows] for p in range(2)], matrix, levels)
        for l in range(levels):
            for p in range(2):
                piece = turned[16 * l : 16 * l + 16, 128 * p : 128 * p + 128]
                out_ref[p * levels + l, start : start + 16, :] = piece


def relayout_last(place, fields, padded):
    rounds, bands, cols, levels, lanes = fields.shape
    return pl.pallas_call(
        lambda *refs: relayout_last_kernel(*refs, cols=cols, levels=levels, padded=padded),
        grid=(bands // 2,),
        in_specs=[sspec(), pl.BlockSpec((1, 2, cols, levels, lanes), lambda g: (rounds - 1, g, 0, 0, 0))],
        out_specs=pl.BlockSpec((2 * levels, padded, lanes), lambda g: (g, 0, 0)),
        out_shape=jax.ShapeDtypeStruct((bands * levels, padded, lanes), BF),
        scratch_shapes=[pltpu.VMEM((2, cols + 2 * LEAD, levels, lanes), BF)],
        compiler_params=params(58),
        name="relayout_last",
    )(place, fields)


def turn_cos(turns):
    near = 0.25 - jnp.abs(turns - jnp.floor(turns + 0.5))
    square = near * near
    value = jnp.full_like(square, -15.094642576822990)
    for factor in (42.058693944897653, -76.705859753061386, 81.605249276075055, -41.341702240399755):
        value = value * square + factor
    return near * (value * square + 6.283185307179586)


def basis_kernel(lon_ref, lon_t_ref, lat_ref, lat_t_ref, *, cols, blocks, padded):
    total = cols * blocks
    nyquist = total // 2
    width = lon_ref.shape[1] // 2
    lanes = lax.broadcasted_iota(jnp.int32, (padded, 128), 1)

    def turns_of(product):
        whole = (product.astype(F32) * (1.0 / total)).astype(jnp.int32)
        return (product - whole * total).astype(F32) * (1.0 / total)

    def lon_rows(j, carry):
        within = lax.broadcasted_iota(jnp.int32, (padded, 128), 0)
        x = jnp.where(within < cols, within + cols * j, cols * (blocks - 1 - j))
        fine = turns_of(x * lanes)
        coarse = turns_of(x * (lanes * 128))
        fine_cos = turn_cos(fine)
        fine_sin = turn_cos(fine - 0.25)
        scale = jnp.where(within <= cols, math.sqrt(2.0 / total), 0.0)
        coarse_cos = turn_cos(coarse) * scale
        coarse_sin = turn_cos(coarse - 0.25) * scale
        rows = pl.ds(pl.multiple_of(j * padded, padded), padded)
        for t in range(width // 128):
            c = lanes + 128 * t
            cos_t = coarse_cos[:, t : t + 1]
            sin_t = coarse_sin[:, t : t + 1]
            even = fine_cos * cos_t - fine_sin * sin_t
            odd = fine_sin * cos_t + fine_cos * sin_t
            if t == 0 or 128 * t <= nyquist < 128 * t + 128:
                even = jnp.where((c == 0) | (c == nyquist), even * math.sqrt(0.5), even)
            if 128 * t + 127 >= nyquist:
                even = jnp.where(c <= nyquist, even, 0.0)
                odd = jnp.where(c < nyquist, odd, 0.0)
            lon_ref[rows, 128 * t : 128 * t + 128] = even.astype(BF)
            lon_ref[rows, width + 128 * t : width + 128 * t + 128] = odd.astype(BF)
        return carry

    lax.fori_loop(0, blocks // 2, lon_rows, 0)
    for t in range(lon_ref.shape[1] // 128):
        strip = lon_ref[:, 128 * t : 128 * t + 128].astype(F32)
        lon_t_ref[128 * t : 128 * t + 128, :] = strip.T.astype(BF)

    length = lat_ref.shape[0]
    step = 64

    def lat_rows(i, carry):
        shape = (step, length)
        down = lax.broadcasted_iota(jnp.int32, shape, 0) + step * i
        across = lax.broadcasted_iota(jnp.int32, shape, 1)
        rows = pl.ds(pl.multiple_of(i * step, step), step)
        for grid, mode, ref in ((down, across, lat_ref), (across, down, lat_t_ref)):
            phase = (mode * (2 * grid + 1)) & (4 * length - 1)
            scale = jnp.where(mode == 0, 1.0 / math.sqrt(length), math.sqrt(2.0 / length))
            ref[rows, :] = (turn_cos(phase.astype(F32) * (0.25 / length)) * scale).astype(BF)
        return carry

    lax.fori_loop(0, length // step, lat_rows, 0)


def bases(cols, blocks, padded, lat_total):
    tall = padded * blocks // 2
    return pl.pallas_call(
        lambda *refs: basis_kernel(*refs, cols=cols, blocks=blocks, padded=padded),
        out_shape=(
            jax.ShapeDtypeStruct((tall, 2 * tall), BF),
            jax.ShapeDtypeStruct((2 * tall, tall), BF),
            jax.ShapeDtypeStruct((lat_total, lat_total), BF),
            jax.ShapeDtypeStruct((lat_total, lat_total), BF),
        ),
        out_specs=(vspec(),) * 4,
        compiler_params=params(58),
        cost_estimate=cost(12e9),
        name="bases",
    )()


def arrange_kernel(place, band, own, other, taper, *, rows_each):
    mem, lat = place[0], place[1]
    spare = taper.shape[1] - RING * rows_each
    taper[:, RING * rows_each :, :] = jnp.zeros((4, spare, 128), BF)

    def rows_of(turn):
        return pl.ds(pl.multiple_of(lax.rem(lat + turn, RING) * rows_each, 8), rows_each)

    for q in range(4):
        taper[q, rows_of(0), :] = band[:, 128 * q : 128 * q + 128]
    for ref, side in ((own, mem), (other, 1 - mem)):
        beside = rows_of(jnp.where(side == 0, RING - 1, 1))
        for q in range(4):
            taper[q, beside, :] = ref[q // 2, :, 128 * (q % 2) : 128 * (q % 2) + 128]
        for q in range(2):
            taper[2 * side + q, rows_of(2), :] = ref[2, :, 128 * q : 128 * q + 128]


def arrange(place, band, own, other):
    rows_each = own.shape[1]
    return pl.pallas_call(
        lambda *refs: arrange_kernel(*refs, rows_each=rows_each),
        out_shape=jax.ShapeDtypeStruct((4, RING * rows_each + 32, 128), BF),
        in_specs=[sspec(), vspec(), vspec(), vspec()],
        out_specs=vspec(),
        compiler_params=params(12),
        cost_estimate=cost(1e9),
        name="arrange",
    )(place, band, own, other)


def member_kernel(*refs, first, final, count, blocks, bands, padded, coefs):
    place, field_in, own_in, other_in, taper_hbm, lon_hbm, lon_t_hbm, lat_hbm, lat_t_hbm = refs[:9]
    rest = list(refs[9:])
    so_far_hbm = None if first else rest.pop(0)
    outs = [rest.pop(0) for _ in range(2 if final else 1)]
    folded, inverse, taper, lon_ref, lon_t_ref, lat_ref, lat_t_ref, acc, sems = rest[:9]
    stages = rest[9:10]
    field, own, other = (field_in, own_in, other_in) if final else rest[10:]
    pairs = blocks // 2
    tall = padded * pairs
    nyquist = coefs // 2
    parts = 4
    step = (nyquist // 2 + 16) // 16 * 16
    group = 4
    turns = pairs // group
    half = padded // 2
    mem = place[0]

    def move(source, target, spot):
        return pltpu.make_async_copy(source, target, sems.at[spot])

    def lon_t_copy(r):
        rows = pl.ds(pl.multiple_of((r // 2) * tall + (r % 2) * step, 16), step)
        return move(lon_t_hbm.at[rows], lon_t_ref.at[rows], 10 + r)

    def lon_copy(b):
        rows = pl.ds(pl.multiple_of(b * group * padded, padded), group * padded)
        return move(lon_hbm.at[rows], lon_ref.at[rows], 14 + b)

    def spots(b, side):
        return pl.ds((blocks - group - b * group) if side else b * group, group)

    def so_far_copy(b, side):
        at = spots(b, side)
        return move(so_far_hbm.at[:, at], acc.at[:, at], 18 + 2 * b + side)

    def out_copy(b, side, n):
        at = spots(b, side)
        stage = stages[0].at[n] if final else stages[0]
        return move(stage.at[:, at], outs[n].at[:, at], 22 + 4 * n + 2 * b + side)

    field_copies = []
    if not final:
        field_copies = [
            move(own_in, own, 0),
            move(other_in, other, 1),
            *[move(field_in.at[a, :, pl.ds(0, count * padded), :], field.at[a], 2 + a) for a in range(bands)],
        ]
    table_copies = [
        lon_t_copy(0),
        lon_t_copy(2),
        move(lat_hbm, lat_ref, 7),
        move(taper_hbm, taper, 8),
        move(lat_t_hbm, lat_t_ref, 9),
    ]
    for copy in field_copies + table_copies:
        copy.start()
    for side in range(2):
        inverse[side, 2 * step :, :] = jnp.zeros((tall - 2 * step, inverse.shape[2]), BF)
    for copy in field_copies:
        copy.wait()
    down = lax.broadcasted_iota(jnp.int32, (padded, 128), 0)
    cols = coefs // blocks

    def weigh(i, a):
        def product(j):
            mine, theirs = own[a, j], other[a, j]
            innov = jnp.concatenate(
                [jnp.where(mem == 0, mine, theirs), jnp.where(mem == 0, theirs, mine)], axis=0
            )
            return field[a, j, i * padded : (i + 1) * padded, :].astype(F32) * innov.astype(F32)

        def body(j, carry):
            rows = pl.ds(pl.multiple_of(j * padded, padded), padded)
            near = product(j)
            far = product(blocks - 1 - j)
            near = jnp.where(down == cols, far[0:1, :], near)
            far = jnp.where(down == 0, 0.0, far)
            folded[0, rows, 128 * a : 128 * a + 128] = (near + far).astype(BF)
            folded[1, rows, 128 * a : 128 * a + 128] = (near - far).astype(BF)
            return carry

        lax.fori_loop(0, pairs, body, 0)

    def spectral(fresh):
        def body(r, carry):
            rows = pl.ds(pl.multiple_of(r * step, 16), step)
            if fresh:

                @pl.when(r > 0)
                def _():
                    for side in range(2):
                        lon_t_copy(2 * side + r).wait()

            tables = [pl.ds(pl.multiple_of(side * tall + r * step, 16), step) for side in range(2)]
            zonal = [
                jnp.dot(lon_t_ref[tables[side], :], folded[side], preferred_element_type=F32).astype(BF)
                for side in range(2)
            ]
            if fresh:

                @pl.when(r == 0)
                def _():
                    for copy in table_copies[2:]:
                        copy.wait()

            spectrum = [jnp.dot(zonal[side], lat_ref[...], preferred_element_type=F32) for side in range(2)]
            tapered = []
            for side in range(2):
                weight_rows = pl.ds(pl.multiple_of(side * nyquist + r * step, 16), step)
                weights = jnp.concatenate([taper[q, weight_rows, :] for q in range(4)], axis=1).astype(F32)
                tapered.append((spectrum[side] * weights).astype(BF))
            for side in range(2):
                back = jnp.dot(tapered[side], lat_t_ref[...], preferred_element_type=F32)
                inverse[side, rows, :] = back.astype(BF)
            if fresh:

                @pl.when(r == 0)
                def _():
                    for b in range(turns):
                        lon_copy(b).start()
                        if not first:
                            so_far_copy(b, 0).start()
                            so_far_copy(b, 1).start()

            return carry

        lax.fori_loop(0, parts // 2, body, 0)

    def gridded(i):
        def body(b, carry):
            rows = pl.ds(pl.multiple_of(b * group * padded, padded), group * padded)
            if i == 0:
                lon_copy(b).wait()
                if not first:
                    so_far_copy(b, 0).wait()
                    so_far_copy(b, 1).wait()
            even = jnp.dot(lon_ref[rows, :tall], inverse[0], preferred_element_type=F32)
            odd = jnp.dot(lon_ref[rows, tall:], inverse[1], preferred_element_type=F32)

            def put(piece, a, j):
                piece = piece * field[a, j, i * padded : (i + 1) * padded, :].astype(F32)
                piece = piece if first and i == 0 else piece + acc[a, j].astype(F32)
                if final:
                    stages[0][mem, a, j] = piece[:half].astype(BF)
                    stages[0][1 - mem, a, j] = piece[half:].astype(BF)
                elif i == count - 1:
                    stages[0][a, j] = piece.astype(BF)
                else:
                    acc[a, j] = piece

            for g in range(group):
                for a in range(bands):
                    j = b * group + g
                    spot = (slice(g * padded, (g + 1) * padded), slice(128 * a, 128 * a + 128))
                    near = even[spot] + odd[spot]
                    far = jnp.where(down == 0, near[cols : cols + 1, :], even[spot] - odd[spot])
                    put(near, a, j)
                    put(far, a, blocks - 1 - j)
            if i == count - 1:
                for n in range(len(outs)):
                    out_copy(b, 0, n).start()
                    out_copy(b, 1, n).start()
            return carry

        for b in range(turns):
            body(b, 0)

    for i in range(count):
        if i == 0:
            for r in (1, 3):
                lon_t_copy(r).start()
        for a in range(bands):
            weigh(i, a)
        if i == 0:
            for copy in table_copies[:2]:
                copy.wait()
        spectral(i == 0)
        gridded(i)
    for b in range(turns):
        for n in range(len(outs)):
            out_copy(b, 0, n).wait()
            out_copy(b, 1, n).wait()


def member(place, field, own, other, taper, tables, so_far, final, dims):
    _, blocks, bands, padded, coefs, lat_total = dims
    half = padded // 2
    tall = padded * blocks // 2
    first = so_far is None
    count = 1 if final else 2
    split = lambda array: array.reshape(bands, blocks, *array.shape[1:])
    near = [split(field), split(own), split(other)]
    far = [taper, *tables] + ([] if first else [so_far])
    block = lambda rows, dtype: ((bands, blocks, rows, 128), dtype)
    scratch = [((2, tall, lat_total), BF), ((2, tall, lat_total), BF)]
    fields = [] if final else [block(count * padded, BF), block(half, BF), block(half, BF)]
    scratch += [(array.shape, array.dtype) for array in (taper, *tables)]
    scratch.append(block(padded, F32 if first else BF))
    results = [block(half, BF), block(half, BF)] if final else [block(padded, BF)]
    staged = ((2, bands, blocks, half, 128), BF) if final else block(padded, BF)
    hbm = pl.BlockSpec(memory_space=pltpu.HBM)
    return pl.pallas_call(
        lambda *refs: member_kernel(
            *refs, first=first, final=final, count=count, blocks=blocks, bands=bands, padded=padded, coefs=coefs
        ),
        out_shape=[jax.ShapeDtypeStruct(*each) for each in results],
        in_specs=[sspec()] + [vspec() if final else hbm] * len(near) + [hbm] * len(far),
        out_specs=[hbm] * len(results),
        scratch_shapes=[pltpu.VMEM(*each) for each in scratch]
        + [pltpu.SemaphoreType.DMA((32,))]
        + [pltpu.VMEM(*each) for each in [staged, *fields]],
        compiler_params=params(63),
        cost_estimate=cost(count * 6e9),
        name="member_last" if final else "member_pair",
    )(place, *near, *far)


def finish_kernel(place, own, other, out, *, levels, cols, half, scale):
    mem = place[0]
    mirrored = place[2] >= place[3]
    bands = own.shape[0] // levels
    to = lax.broadcasted_iota(jnp.int32, (2 * half, half), 0)
    frm = lax.broadcasted_iota(jnp.int32, (2 * half, half), 1)
    taken = jnp.where(mirrored & (to > 0), cols - to, to)
    picks = [jnp.where(taken == frm + side * half, 1.0, 0.0).astype(BF) for side in (mem, 1 - mem)]
    picks = jnp.concatenate(picks * bands, axis=1)
    columns = []
    for l in range(levels):
        parts = [ref[a * levels + l] for a in range(bands) for ref in (own, other)]
        columns.append(jnp.concatenate(parts, axis=0))
    summed = jnp.dot(picks, jnp.concatenate(columns, axis=1), preferred_element_type=F32) * scale
    for l in range(levels):
        out[:, l, :] = summed[:cols, 128 * l : 128 * l + 128]


def finish(place, own, other, levels, cols, half, scale):
    return pl.pallas_call(
        lambda *refs: finish_kernel(*refs, levels=levels, cols=cols, half=half, scale=scale),
        out_shape=jax.ShapeDtypeStruct((cols, levels, 128), F32),
        in_specs=[sspec(), vspec(), vspec()],
        out_specs=vspec(),
        compiler_params=params(16),
        name="finish",
    )(place, own, other)


def local(anomalies, taper, obs_row, obs_col, obs_level, obs_value):
    members, levels, cols, lat_rows = anomalies.shape
    bands = lax.axis_size("lat")
    blocks = lax.axis_size("lon")
    mem, lat, lon = lax.axis_index("mem"), lax.axis_index("lat"), lax.axis_index("lon")
    coefs = cols * blocks
    lat_total = lat_rows * bands
    padded = -(-cols // 32) * 32
    half = padded // 2
    ensemble = members * lax.axis_size("mem")
    place = jnp.stack([mem, lat, lon, jnp.int32(blocks // 2)]).astype(jnp.int32)

    by_round = jnp.transpose(anomalies, (0, 2, 1, 3)).reshape(members // bands, bands, cols, levels, lat_rows)
    pair_out = head(by_round, obs_row, obs_col, obs_level, obs_value, half, padded)
    pair_out, taper = lax.optimization_barrier((pair_out, taper))
    pair = over_all(pair_out)
    n_half = lat_total // 2
    band = taper[0].astype(BF)
    band_half = lax.dynamic_slice_in_dim(taper[0], mem * n_half, n_half, axis=1).astype(BF)
    beside = lax.ppermute(band, ("lat", "mem"), beside_pairs())
    across = shift_lat(band_half, 2)
    last_out = relayout_last(place, by_round, padded)
    last = over_all(last_out)
    held = jnp.stack([beside[:, :n_half], beside[:, n_half:], across])
    weights = arrange(place, band, held, swap(held))
    own = pair[:, 2 * padded :, :]
    other = swap(own)

    tables = bases(cols, blocks, padded, lat_total)
    dims = (cols, blocks, bands, padded, coefs, lat_total)
    (summed,) = member(place, pair, own, other, weights, tables, None, False, dims)
    mine, theirs = member(place, last, own, other, weights, tables, summed, True, dims)
    merged = (mine.astype(F32) + swap(theirs).astype(F32)).astype(BF).reshape(bands * blocks, half, lat_rows)
    pieces = over_all(merged)
    out = finish(place, pieces, swap(pieces), levels, cols, half, 1.0 / (ensemble - 1))
    return jnp.transpose(out, (1, 0, 2))


def solution(mesh):
    in_specs = (
        P("mem", None, "lon", "lat"),
        P("lon", "lat", None),
        P("lat", "lon"),
        P("lat", "lon"),
        P("lat", "lon"),
        P("lat", "lon"),
    )
    out_specs = P(None, "lon", "lat")

    return jax.shard_map(local, mesh=mesh, in_specs=in_specs, out_specs=out_specs, check_vma=False)
```

```python
import math

import jax
import jax.numpy as jnp
from jax import lax
from jax.experimental import pallas as pl
from jax.experimental.pallas import tpu as pltpu
from jax.sharding import PartitionSpec as P


BF = jnp.bfloat16
F32 = jnp.float32
LL = ("lat", "lon")
SWAP = [(0, 1), (1, 0)]
RING = 4


def vspec():
    return pl.BlockSpec(memory_space=pltpu.VMEM)


def sspec():
    return pl.BlockSpec(memory_space=pltpu.SMEM)


def params(mib, **more):
    return pltpu.CompilerParams(vmem_limit_bytes=mib * 1024 * 1024, **more)


def cost(flops):
    return pl.CostEstimate(flops=int(flops), bytes_accessed=1 << 20, transcendentals=0)


def over_all(x):
    return lax.all_to_all(x, LL, split_axis=0, concat_axis=0, tiled=True)


def shift_lat(x, s):
    return lax.ppermute(x, "lat", [(i, (i + s) % RING) for i in range(RING)])


def beside_pairs():
    turns = (1, RING - 1)
    return [(2 * i + m, 2 * ((i + turns[m]) % RING) + m) for i in range(RING) for m in range(2)]


def swap(x):
    return lax.ppermute(x, "mem", SWAP)


LEAD = 6


def turn_block(blocks, turn, levels):
    both = jnp.concatenate([block.reshape(16 * levels, 128) for block in blocks], axis=1)
    return jnp.dot(turn, both, preferred_element_type=F32).astype(BF)


def turner(levels, mirrored, have):
    size = 16 * levels
    to = lax.broadcasted_iota(jnp.int32, (size, size), 0)
    frm = lax.broadcasted_iota(jnp.int32, (size, size), 1)
    within = to & 15
    taken = jnp.where(mirrored, 15 - within, within)
    return jnp.where((frm == taken * levels + (to >> 4)) & (within < have), 1.0, 0.0).astype(BF)


def turn_start(start, mirrored, cols):
    return jnp.where(mirrored, LEAD + cols - 15 - start, LEAD + start)


def head_kernel(fields, row_hbm, col_hbm, level_hbm, value_hbm, out, *scratch, half, levels, cols, padded):
    row_ref, col_ref, level_ref, value_ref, fields_in, staged, innov, acc, sems = scratch
    bands = fields.shape[1]
    count = iter(range(32))

    def fetch(source, target):
        copy = pltpu.make_async_copy(source, target, sems.at[next(count)])
        copy.start()
        return copy

    observed = [
        fetch(row_hbm, row_ref),
        fetch(col_hbm, col_ref),
        fetch(level_hbm, level_ref),
        fetch(value_hbm, value_ref),
    ]
    arriving = [
        (
            fetch(fields.at[pl.ds(0, 2), g], fields_in.at[:, g, pl.ds(LEAD, cols)]),
            fetch(fields.at[pl.ds(0, 2), g, pl.ds(0, 1)], fields_in.at[:, g, pl.ds(LEAD + cols, 1)]),
        )
        for g in range(bands)
    ]
    mem, lat, lon = lax.axis_index("mem"), lax.axis_index("lat"), lax.axis_index("lon")
    mirrored = lon >= lax.axis_size("lon") // 2
    for p in range(2):
        for g in range(bands):
            fields_in[p, g, :LEAD] = jnp.zeros((LEAD, levels, 128), BF)
            fields_in[p, g, LEAD + cols + 1 :] = jnp.zeros((LEAD - 1, levels, 128), BF)
    slots = levels * half
    acc[...] = jnp.zeros_like(acc)

    def spots_of(count):
        major = lax.broadcasted_iota(jnp.int32, (count // 16, 16, 128), 0)
        minor = lax.broadcasted_iota(jnp.int32, (count // 16, 16, 128), 1)
        return (major * 16 + minor).astype(F32).astype(BF)

    def packed(row):
        return jnp.broadcast_to(row, (16, 128)).astype(BF)[None]

    slot_ids = spots_of(256)
    row_ids = spots_of(128)
    one = jnp.ones((), BF)
    zero = jnp.zeros((), BF)
    for copy in observed:
        copy.wait()

    def add_group(g, carry):
        rows = pl.ds(pl.multiple_of(g * 16, 8), 16)
        column = col_ref[rows, :] - lon * cols
        within = jnp.where(mirrored & (column > 0), cols - column, column) - mem * half
        inside = (within >= 0) & (within < half)
        keys = jnp.where(inside, level_ref[rows, :] * half + within, -1)
        lat_row = (row_ref[rows, :] - lat * 128).astype(F32)
        value = value_ref[rows, :]
        high = value.astype(BF).astype(F32)
        middle = value - high
        parts = []
        for start in range(0, slots, 256):
            part = keys - start
            parts.append(jnp.where((part >= 0) & (part < 256), part, -1).astype(F32))
        left = []
        right = []
        for r in range(16):
            at = slice(r, r + 1)
            hits = [jnp.where(slot_ids == packed(part[at]), one, zero).reshape(256, 128) for part in parts]
            left.append(jnp.concatenate(hits, axis=0))
            row_hit = row_ids == packed(lat_row[at])
            sides = [jnp.where(row_hit, packed(side[at]), zero).reshape(128, 128) for side in (high, middle)]
            right.append(jnp.concatenate(sides, axis=0))
        acc[...] += lax.dot_general(
            jnp.concatenate(left, axis=1),
            jnp.concatenate(right, axis=1),
            (((1,), (1,)), ((), ())),
            preferred_element_type=F32,
        )
        return carry

    leaving = []
    lax.fori_loop(0, 2, add_group, 0)
    turn = turner(levels, mirrored, 16)
    last_turn = turner(levels, mirrored, cols % 16)
    for first in range(0, bands, 2):
        group = range(first, first + 2)
        for g in group:
            for copy in arriving[g]:
                copy.wait()
        for start in range(0, padded, 16):
            rows = pl.ds(turn_start(start, mirrored, cols), 16)
            matrix = turn if start + 16 <= cols else last_turn
            turned = turn_block([fields_in[p, g, rows] for g in group for p in range(2)], matrix, levels)
            for l in range(levels):
                for n, g in enumerate(group):
                    for p in range(2):
                        lane = 256 * n + 128 * p
                        piece = turned[16 * l : 16 * l + 16, lane : lane + 128]
                        staged[g * levels + l, p * padded + start : p * padded + start + 16, :] = piece
        for g in group:
            leaving.append(
                fetch(
                    staged.at[pl.ds(g * levels, levels)],
                    out.at[pl.ds(g * levels, levels), pl.ds(0, 2 * padded), :],
                )
            )
    lax.fori_loop(2, row_ref.shape[0] // 16, add_group, 0)
    innov[...] = (acc[:, :128] + acc[:, 128:]).astype(BF).reshape(levels, half, 128)
    leaving += [
        fetch(innov, out.at[pl.ds(g * levels, levels), pl.ds(2 * padded, half), :]) for g in range(bands)
    ]
    for copy in leaving:
        copy.wait()


def head(fields, obs_row, obs_col, obs_level, obs_value, half, padded):
    _, bands, cols, levels, lanes = fields.shape
    rows = 2 * padded + half
    hbm = pl.BlockSpec(memory_space=pltpu.HBM)
    observed = (obs_row, obs_col, obs_level, obs_value)
    return pl.pallas_call(
        lambda *refs: head_kernel(*refs, half=half, levels=levels, cols=cols, padded=padded),
        out_shape=jax.ShapeDtypeStruct((bands * levels, rows, lanes), BF),
        in_specs=[hbm] * 5,
        out_specs=hbm,
        scratch_shapes=[pltpu.VMEM(array.shape, array.dtype) for array in observed]
        + [
            pltpu.VMEM((2, bands, cols + 2 * LEAD, levels, lanes), BF),
            pltpu.VMEM((bands * levels, 2 * padded, lanes), BF),
            pltpu.VMEM((levels, half, lanes), BF),
            pltpu.VMEM((levels * half, 2 * lanes), F32),
            pltpu.SemaphoreType.DMA((32,)),
        ],
        compiler_params=params(61),
        cost_estimate=cost(6e9),
        name="head",
    )(fields, *observed)


def relayout_last_kernel(place, in_ref, out_ref, room, *, cols, levels, padded):
    mirrored = place[2] >= place[3]
    for p in range(2):
        room[p, :LEAD] = jnp.zeros((LEAD, levels, 128), BF)
        room[p, LEAD : LEAD + cols] = in_ref[0, p]
        room[p, LEAD + cols] = in_ref[0, p, 0]
        room[p, LEAD + cols + 1 :] = jnp.zeros((LEAD - 1, levels, 128), BF)
    turn = turner(levels, mirrored, 16)
    last_turn = turner(levels, mirrored, cols % 16)
    for start in range(0, padded, 16):
        rows = pl.ds(turn_start(start, mirrored, cols), 16)
        matrix = turn if start + 16 <= cols else last_turn
        turned = turn_block([room[p, rows] for p in range(2)], matrix, levels)
        for l in range(levels):
            for p in range(2):
                piece = turned[16 * l : 16 * l + 16, 128 * p : 128 * p + 128]
                out_ref[p * levels + l, start : start + 16, :] = piece


def relayout_last(place, fields, padded):
    rounds, bands, cols, levels, lanes = fields.shape
    return pl.pallas_call(
        lambda *refs: relayout_last_kernel(*refs, cols=cols, levels=levels, padded=padded),
        grid=(bands // 2,),
        in_specs=[sspec(), pl.BlockSpec((1, 2, cols, levels, lanes), lambda g: (rounds - 1, g, 0, 0, 0))],
        out_specs=pl.BlockSpec((2 * levels, padded, lanes), lambda g: (g, 0, 0)),
        out_shape=jax.ShapeDtypeStruct((bands * levels, padded, lanes), BF),
        scratch_shapes=[pltpu.VMEM((2, cols + 2 * LEAD, levels, lanes), BF)],
        compiler_params=params(58),
        name="relayout_last",
    )(place, fields)


def turn_cos(turns):
    near = 0.25 - jnp.abs(turns - jnp.floor(turns + 0.5))
    square = near * near
    value = jnp.full_like(square, -15.094642576822990)
    for factor in (42.058693944897653, -76.705859753061386, 81.605249276075055, -41.341702240399755):
        value = value * square + factor
    return near * (value * square + 6.283185307179586)


def basis_kernel(lon_ref, lon_t_ref, lat_ref, lat_t_ref, *, cols, blocks, padded):
    total = cols * blocks
    nyquist = total // 2
    width = lon_ref.shape[1] // 2
    lanes = lax.broadcasted_iota(jnp.int32, (padded, 128), 1)

    def turns_of(product):
        whole = (product.astype(F32) * (1.0 / total)).astype(jnp.int32)
        return (product - whole * total).astype(F32) * (1.0 / total)

    def lon_rows(j, carry):
        within = lax.broadcasted_iota(jnp.int32, (padded, 128), 0)
        x = jnp.where(within < cols, within + cols * j, cols * (blocks - 1 - j))
        fine = turns_of(x * lanes)
        coarse = turns_of(x * (lanes * 128))
        fine_cos = turn_cos(fine)
        fine_sin = turn_cos(fine - 0.25)
        scale = jnp.where(within <= cols, math.sqrt(2.0 / total), 0.0)
        coarse_cos = turn_cos(coarse) * scale
        coarse_sin = turn_cos(coarse - 0.25) * scale
        rows = pl.ds(pl.multiple_of(j * padded, padded), padded)
        for t in range(width // 128):
            c = lanes + 128 * t
            cos_t = coarse_cos[:, t : t + 1]
            sin_t = coarse_sin[:, t : t + 1]
            even = fine_cos * cos_t - fine_sin * sin_t
            odd = fine_sin * cos_t + fine_cos * sin_t
            if t == 0 or 128 * t <= nyquist < 128 * t + 128:
                even = jnp.where((c == 0) | (c == nyquist), even * math.sqrt(0.5), even)
            if 128 * t + 127 >= nyquist:
                even = jnp.where(c <= nyquist, even, 0.0)
                odd = jnp.where(c < nyquist, odd, 0.0)
            lon_ref[rows, 128 * t : 128 * t + 128] = even.astype(BF)
            lon_ref[rows, width + 128 * t : width + 128 * t + 128] = odd.astype(BF)
        return carry

    lax.fori_loop(0, blocks // 2, lon_rows, 0)
    for t in range(lon_ref.shape[1] // 128):
        strip = lon_ref[:, 128 * t : 128 * t + 128].astype(F32)
        lon_t_ref[128 * t : 128 * t + 128, :] = strip.T.astype(BF)

    length = lat_ref.shape[0]
    step = 64

    def lat_rows(i, carry):
        shape = (step, length)
        down = lax.broadcasted_iota(jnp.int32, shape, 0) + step * i
        across = lax.broadcasted_iota(jnp.int32, shape, 1)
        rows = pl.ds(pl.multiple_of(i * step, step), step)
        for grid, mode, ref in ((down, across, lat_ref), (across, down, lat_t_ref)):
            phase = (mode * (2 * grid + 1)) & (4 * length - 1)
            scale = jnp.where(mode == 0, 1.0 / math.sqrt(length), math.sqrt(2.0 / length))
            ref[rows, :] = (turn_cos(phase.astype(F32) * (0.25 / length)) * scale).astype(BF)
        return carry

    lax.fori_loop(0, length // step, lat_rows, 0)


def bases(cols, blocks, padded, lat_total):
    tall = padded * blocks // 2
    return pl.pallas_call(
        lambda *refs: basis_kernel(*refs, cols=cols, blocks=blocks, padded=padded),
        out_shape=(
            jax.ShapeDtypeStruct((tall, 2 * tall), BF),
            jax.ShapeDtypeStruct((2 * tall, tall), BF),
            jax.ShapeDtypeStruct((lat_total, lat_total), BF),
            jax.ShapeDtypeStruct((lat_total, lat_total), BF),
        ),
        out_specs=(vspec(),) * 4,
        compiler_params=params(58),
        cost_estimate=cost(12e9),
        name="bases",
    )()


def arrange_kernel(place, band, own, other, taper, *, rows_each):
    mem, lat = place[0], place[1]
    spare = taper.shape[1] - RING * rows_each
    taper[:, RING * rows_each :, :] = jnp.zeros((4, spare, 128), BF)

    def rows_of(turn):
        return pl.ds(pl.multiple_of(lax.rem(lat + turn, RING) * rows_each, 8), rows_each)

    for q in range(4):
        taper[q, rows_of(0), :] = band[:, 128 * q : 128 * q + 128]
    for ref, side in ((own, mem), (other, 1 - mem)):
        beside = rows_of(jnp.where(side == 0, RING - 1, 1))
        for q in range(4):
            taper[q, beside, :] = ref[q // 2, :, 128 * (q % 2) : 128 * (q % 2) + 128]
        for q in range(2):
            taper[2 * side + q, rows_of(2), :] = ref[2, :, 128 * q : 128 * q + 128]


def arrange(place, band, own, other):
    rows_each = own.shape[1]
    return pl.pallas_call(
        lambda *refs: arrange_kernel(*refs, rows_each=rows_each),
        out_shape=jax.ShapeDtypeStruct((4, RING * rows_each + 32, 128), BF),
        in_specs=[sspec(), vspec(), vspec(), vspec()],
        out_specs=vspec(),
        compiler_params=params(12),
        cost_estimate=cost(1e9),
        name="arrange",
    )(place, band, own, other)


def member_kernel(*refs, first, final, count, blocks, bands, padded, coefs):
    place, field_in, own_in, other_in, taper_hbm, lon_hbm, lon_t_hbm, lat_hbm, _ = refs[:9]
    rest = list(refs[9:])
    so_far_hbm = None if first else rest.pop(0)
    outs = [rest.pop(0) for _ in range(2 if final else 1)]
    folded, inverse, taper, lon_ref, lon_t_ref, lat_ref, _, acc, sems = rest[:9]
    stages = rest[9:10]
    field, own, other = (field_in, own_in, other_in) if final else rest[10:]
    pairs = blocks // 2
    tall = padded * pairs
    nyquist = coefs // 2
    parts = 4
    step = (nyquist // 2 + 16) // 16 * 16
    group = 4
    turns = pairs // group
    half = padded // 2
    mem = place[0]

    def move(source, target, spot):
        return pltpu.make_async_copy(source, target, sems.at[spot])

    def lon_t_copy(r):
        rows = pl.ds(pl.multiple_of((r // 2) * tall + (r % 2) * step, 16), step)
        return move(lon_t_hbm.at[rows], lon_t_ref.at[rows], 10 + r)

    def lon_copy(b):
        rows = pl.ds(pl.multiple_of(b * group * padded, padded), group * padded)
        return move(lon_hbm.at[rows], lon_ref.at[rows], 14 + b)

    def spots(b, side):
        return pl.ds((blocks - group - b * group) if side else b * group, group)

    def so_far_copy(b, side):
        at = spots(b, side)
        return move(so_far_hbm.at[:, at], acc.at[:, at], 18 + 2 * b + side)

    def out_copy(b, side, n):
        at = spots(b, side)
        stage = stages[0].at[n] if final else stages[0]
        return move(stage.at[:, at], outs[n].at[:, at], 22 + 4 * n + 2 * b + side)

    field_copies = []
    if not final:
        field_copies = [
            move(own_in, own, 0),
            move(other_in, other, 1),
            *[move(field_in.at[a, :, pl.ds(0, count * padded), :], field.at[a], 2 + a) for a in range(bands)],
        ]
    table_copies = [
        lon_t_copy(0),
        lon_t_copy(2),
        move(lat_hbm, lat_ref, 7),
        move(taper_hbm, taper, 8),
    ]
    for copy in field_copies + table_copies:
        copy.start()
    for side in range(2):
        inverse[side, 2 * step :, :] = jnp.zeros((tall - 2 * step, inverse.shape[2]), BF)
    for copy in field_copies:
        copy.wait()
    down = lax.broadcasted_iota(jnp.int32, (padded, 128), 0)
    cols = coefs // blocks

    def weigh(i, a):
        def product(j):
            mine, theirs = own[a, j], other[a, j]
            innov = jnp.concatenate(
                [jnp.where(mem == 0, mine, theirs), jnp.where(mem == 0, theirs, mine)], axis=0
            )
            return field[a, j, i * padded : (i + 1) * padded, :].astype(F32) * innov.astype(F32)

        def body(j, carry):
            rows = pl.ds(pl.multiple_of(j * padded, padded), padded)
            near = product(j)
            far = product(blocks - 1 - j)
            near = jnp.where(down == cols, far[0:1, :], near)
            far = jnp.where(down == 0, 0.0, far)
            folded[0, rows, 128 * a : 128 * a + 128] = (near + far).astype(BF)
            folded[1, rows, 128 * a : 128 * a + 128] = (near - far).astype(BF)
            return carry

        lax.fori_loop(0, pairs, body, 0)

    def spectral(fresh):
        def body(r, carry):
            rows = pl.ds(pl.multiple_of(r * step, 16), step)
            if fresh:

                @pl.when(r > 0)
                def _():
                    for side in range(2):
                        lon_t_copy(2 * side + r).wait()

            tables = [pl.ds(pl.multiple_of(side * tall + r * step, 16), step) for side in range(2)]
            zonal = [
                jnp.dot(lon_t_ref[tables[side], :], folded[side], preferred_element_type=F32).astype(BF)
                for side in range(2)
            ]
            if fresh:

                @pl.when(r == 0)
                def _():
                    for copy in table_copies[2:]:
                        copy.wait()

            spectrum = [jnp.dot(zonal[side], lat_ref[...], preferred_element_type=F32) for side in range(2)]
            tapered = []
            for side in range(2):
                weight_rows = pl.ds(pl.multiple_of(side * nyquist + r * step, 16), step)
                weights = jnp.concatenate([taper[q, weight_rows, :] for q in range(4)], axis=1).astype(F32)
                tapered.append((spectrum[side] * weights).astype(BF))
            for side in range(2):
                back = lax.dot_general(
                    tapered[side], lat_ref[...], (((1,), (1,)), ((), ())), preferred_element_type=F32
                )
                inverse[side, rows, :] = back.astype(BF)
            return carry

        lax.fori_loop(0, parts // 2, body, 0)

    def gridded(i):
        def body(b, carry):
            rows = pl.ds(pl.multiple_of(b * group * padded, padded), group * padded)
            if i == 0:
                lon_copy(b).wait()
                if not first:
                    so_far_copy(b, 0).wait()
                    so_far_copy(b, 1).wait()
            even = jnp.dot(lon_ref[rows, :tall], inverse[0], preferred_element_type=F32)
            odd = jnp.dot(lon_ref[rows, tall:], inverse[1], preferred_element_type=F32)

            def put(piece, a, j):
                piece = piece * field[a, j, i * padded : (i + 1) * padded, :].astype(F32)
                piece = piece if first and i == 0 else piece + acc[a, j].astype(F32)
                if final:
                    stages[0][mem, a, j] = piece[:half].astype(BF)
                    stages[0][1 - mem, a, j] = piece[half:].astype(BF)
                elif i == count - 1:
                    stages[0][a, j] = piece.astype(BF)
                else:
                    acc[a, j] = piece

            for g in range(group):
                for a in range(bands):
                    j = b * group + g
                    spot = (slice(g * padded, (g + 1) * padded), slice(128 * a, 128 * a + 128))
                    near = even[spot] + odd[spot]
                    far = jnp.where(down == 0, near[cols : cols + 1, :], even[spot] - odd[spot])
                    put(near, a, j)
                    put(far, a, blocks - 1 - j)
            if i == count - 1:
                for n in range(len(outs)):
                    out_copy(b, 0, n).start()
                    out_copy(b, 1, n).start()
            return carry

        for b in range(turns):
            body(b, 0)

    for i in range(count):
        if i == 0:
            for r in (1, 3):
                lon_t_copy(r).start()
        for a in range(bands):
            weigh(i, a)
        if i == 0:
            for copy in table_copies[:2]:
                copy.wait()
            for b in range(turns):
                lon_copy(b).start()
                if not first:
                    so_far_copy(b, 0).start()
                    so_far_copy(b, 1).start()
        spectral(i == 0)
        gridded(i)
    for b in range(turns):
        for n in range(len(outs)):
            out_copy(b, 0, n).wait()
            out_copy(b, 1, n).wait()


def member(place, field, own, other, taper, tables, so_far, final, dims):
    _, blocks, bands, padded, coefs, lat_total = dims
    half = padded // 2
    tall = padded * blocks // 2
    first = so_far is None
    count = 1 if final else 2
    split = lambda array: array.reshape(bands, blocks, *array.shape[1:])
    near = [split(field), split(own), split(other)]
    far = [taper, *tables] + ([] if first else [so_far])
    block = lambda rows, dtype: ((bands, blocks, rows, 128), dtype)
    scratch = [((2, tall, lat_total), BF), ((2, tall, lat_total), BF)]
    fields = [] if final else [block(count * padded, BF), block(half, BF), block(half, BF)]
    scratch += [(array.shape, array.dtype) for array in (taper, *tables)]
    scratch.append(block(padded, F32 if first else BF))
    results = [block(half, BF), block(half, BF)] if final else [block(padded, BF)]
    staged = ((2, bands, blocks, half, 128), BF) if final else block(padded, BF)
    hbm = pl.BlockSpec(memory_space=pltpu.HBM)
    return pl.pallas_call(
        lambda *refs: member_kernel(
            *refs, first=first, final=final, count=count, blocks=blocks, bands=bands, padded=padded, coefs=coefs
        ),
        out_shape=[jax.ShapeDtypeStruct(*each) for each in results],
        in_specs=[sspec()] + [vspec() if final else hbm] * len(near) + [hbm] * len(far),
        out_specs=[hbm] * len(results),
        scratch_shapes=[pltpu.VMEM(*each) for each in scratch]
        + [pltpu.SemaphoreType.DMA((32,))]
        + [pltpu.VMEM(*each) for each in [staged, *fields]],
        compiler_params=params(63),
        cost_estimate=cost(count * 6e9),
        name="member_last" if final else "member_pair",
    )(place, *near, *far)


def finish_kernel(place, own, other, out, *, levels, cols, half, scale):
    mem = place[0]
    mirrored = place[2] >= place[3]
    bands = own.shape[0] // levels
    to = lax.broadcasted_iota(jnp.int32, (2 * half, half), 0)
    frm = lax.broadcasted_iota(jnp.int32, (2 * half, half), 1)
    taken = jnp.where(mirrored & (to > 0), cols - to, to)
    picks = [jnp.where(taken == frm + side * half, 1.0, 0.0).astype(BF) for side in (mem, 1 - mem)]
    picks = jnp.concatenate(picks * bands, axis=1)
    columns = []
    for l in range(levels):
        parts = [ref[a * levels + l] for a in range(bands) for ref in (own, other)]
        columns.append(jnp.concatenate(parts, axis=0))
    summed = jnp.dot(picks, jnp.concatenate(columns, axis=1), preferred_element_type=F32) * scale
    for l in range(levels):
        out[:, l, :] = summed[:cols, 128 * l : 128 * l + 128]


def finish(place, own, other, levels, cols, half, scale):
    return pl.pallas_call(
        lambda *refs: finish_kernel(*refs, levels=levels, cols=cols, half=half, scale=scale),
        out_shape=jax.ShapeDtypeStruct((cols, levels, 128), F32),
        in_specs=[sspec(), vspec(), vspec()],
        out_specs=vspec(),
        compiler_params=params(16),
        name="finish",
    )(place, own, other)


def local(anomalies, taper, obs_row, obs_col, obs_level, obs_value):
    members, levels, cols, lat_rows = anomalies.shape
    bands = lax.axis_size("lat")
    blocks = lax.axis_size("lon")
    mem, lat, lon = lax.axis_index("mem"), lax.axis_index("lat"), lax.axis_index("lon")
    coefs = cols * blocks
    lat_total = lat_rows * bands
    padded = -(-cols // 32) * 32
    half = padded // 2
    ensemble = members * lax.axis_size("mem")
    place = jnp.stack([mem, lat, lon, jnp.int32(blocks // 2)]).astype(jnp.int32)

    by_round = jnp.transpose(anomalies, (0, 2, 1, 3)).reshape(members // bands, bands, cols, levels, lat_rows)
    pair_out = head(by_round, obs_row, obs_col, obs_level, obs_value, half, padded)
    pair_out, taper = lax.optimization_barrier((pair_out, taper))
    pair = over_all(pair_out)
    n_half = lat_total // 2
    band = taper[0].astype(BF)
    band_half = lax.dynamic_slice_in_dim(taper[0], mem * n_half, n_half, axis=1).astype(BF)
    beside = lax.ppermute(band, ("lat", "mem"), beside_pairs())
    across = shift_lat(band_half, 2)
    last_out = relayout_last(place, by_round, padded)
    last = over_all(last_out)
    held = jnp.stack([beside[:, :n_half], beside[:, n_half:], across])
    weights = arrange(place, band, held, swap(held))
    own = pair[:, 2 * padded :, :]
    other = swap(own)

    tables = bases(cols, blocks, padded, lat_total)
    dims = (cols, blocks, bands, padded, coefs, lat_total)
    (summed,) = member(place, pair, own, other, weights, tables, None, False, dims)
    mine, theirs = member(place, last, own, other, weights, tables, summed, True, dims)
    merged = (mine.astype(F32) + swap(theirs).astype(F32)).astype(BF).reshape(bands * blocks, half, lat_rows)
    pieces = over_all(merged)
    out = finish(place, pieces, swap(pieces), levels, cols, half, 1.0 / (ensemble - 1))
    return jnp.transpose(out, (1, 0, 2))


def solution(mesh):
    in_specs = (
        P("mem", None, "lon", "lat"),
        P("lon", "lat", None),
        P("lat", "lon"),
        P("lat", "lon"),
        P("lat", "lon"),
        P("lat", "lon"),
    )
    out_specs = P(None, "lon", "lat")

    return jax.shard_map(local, mesh=mesh, in_specs=in_specs, out_specs=out_specs, check_vma=False)
```
